128 devices in a mesh: grp: 4 (over z), seq: 32 (over x, y, core).
Axes of the slice: x: 4, y: 4, z: 4, core: 2. Of those that a mesh axis runs over, the one named last changes fastest.
Arguments:
- hidden_in: bfloat16 [96, 4096], P(None, ('grp', 'seq')), may hold values from -6 to 6
- norm_gain: float32 [4096], replicated, may hold values from 0.5 to 1.5
- w_ssm_in: bfloat16 [4096, 8192], P(None, ('grp', 'seq')), may hold values from -0.09375 to 0.09375
- w_ssm_gate: bfloat16 [4096, 8192], P(None, ('grp', 'seq')), may hold values from -0.09375 to 0.09375
- conv_weight: float32 [4, 8192], P(None, ('grp', 'seq')), may hold values from -3 to 3
- conv_bias: float32 [8192], P(('grp', 'seq')), may hold values from -0.5 to 0.5
- conv_state: bfloat16 [96, 3, 8192], P(None, None, ('grp', 'seq')), may hold values from -6 to 6
- w_state_proj: bfloat16 [8192, 288], P(('grp', 'seq')), may hold values from -0.0625 to 0.0625
- w_step: bfloat16 [256, 8192], P(None, ('grp', 'seq')), may hold values from -0.375 to 0.375
- step_bias: float32 [8192], P(('grp', 'seq')), may hold values from -4 to -1
- log_decay: float32 [16, 8192], P(None, ('grp', 'seq')), may hold values from 0 to 2.7
- skip_gain: float32 [8192], P(('grp', 'seq')), may hold values from 0.5 to 1.5
- ssm_state: float32 [96, 16, 8192], P(None, None, ('grp', 'seq')), may hold values from -6 to 6
- w_ssm_out: bfloat16 [8192, 4096], P(('grp', 'seq')), may hold values from -0.25 to 0.25
- w_query: bfloat16 [4096, 2048], P(None, 'grp'), may hold values from -6 to 6
- key_projection: bfloat16 [4096, 1024], P(None, 'grp'), may hold values from -0.09375 to 0.09375
- value_projection: bfloat16 [4096, 1024], P(None, 'grp'), may hold values from -0.09375 to 0.09375
- w_attn_out: bfloat16 [2048, 4096], P('grp', 'seq'), may hold values from -0.125 to 0.125
- w_mlp_gate: bfloat16 [4096, 14336], P(None, ('grp', 'seq')), may hold values from -0.09375 to 0.09375
- w_mlp_up: bfloat16 [4096, 14336], P(None, ('grp', 'seq')), may hold values from -0.09375 to 0.09375
- w_mlp_down: bfloat16 [14336, 4096], P(('grp', 'seq')), may hold values from -0.1875 to 0.1875
- cached_inputs: bfloat16 [96, 512, 4096], P('seq'), may hold values from -6 to 6
- window_lengths: int32 [96], replicated, may hold values from 1 to 512, as said below
Outputs:
- hidden_out: bfloat16 [96, 4096], P(None, ('grp', 'seq'))
- state_out: float32 [96, 16, 8192], P(None, None, ('grp', 'seq'))
The draws below stay inside these ranges and needn't reach their ends.
Inputs may be any that keep to these rules, and one draw needn't show every extreme that they name: `window_lengths`: every sequence has at least one valid cached position, and some sequence fills the whole window of 512.
All inputs are finite; a program needn't handle non-finite values.
Results may differ from the reference program's by a relative error of at most 0.012.
The reference program's roundings to bfloat16 on the way count: a program that leaves them out, or rounds other values in their place, can miss the bound.
Values may be sent and summed in bfloat16 or wider, within the bound.
No kernel may reach another device: no remote copies, remote signals or barrier semaphores. Data moves between devices by JAX's collectives and lax.ppermute only.
A program may use at most 128 MiB of HBM per device.

```python
import jax
import jax.numpy as jnp
from jax import lax

MODEL_DIM = 4096
E = 8192
NS = 16
KC = 4
DTR = 256
QUERY_HEADS = 16
KEY_VALUE_HEADS = 8
HEAD_SIZE = 128
FF = 14336
WINDOW_SPAN = 512
BATCH_SEQUENCES = 96


def draw_window_lengths(key, part):
    drawn_lengths = jax.random.randint(jax.random.fold_in(key, 7), (BATCH_SEQUENCES,), 1, WINDOW_SPAN + 1, dtype=jnp.int32)
    chosen = jax.random.randint(jax.random.fold_in(key, 11), (), 0, BATCH_SEQUENCES, dtype=jnp.int32)
    return jnp.where(jnp.arange(BATCH_SEQUENCES, dtype=jnp.int32) == chosen, WINDOW_SPAN, drawn_lengths).astype(jnp.int32)


def draw_w_query(key, part):
    columns = QUERY_HEADS * HEAD_SIZE
    chosen_heads = jax.random.permutation(jax.random.fold_in(key, 3), QUERY_HEADS)
    entries = jax.random.normal(jax.random.fold_in(key, 5), (MODEL_DIM, columns), jnp.float32)
    levels = jnp.array([24.0, 48.0, 96.0], jnp.float32)
    head_scale = jnp.ones((QUERY_HEADS,), jnp.float32).at[chosen_heads[:3]].set(levels)
    column_scale = jnp.repeat(head_scale, HEAD_SIZE)
    scaled = entries * column_scale[None, :] * float(MODEL_DIM) ** (-0.5)
    return jnp.clip(scaled, -6.0, 6.0).astype(jnp.bfloat16)


def spiked(values, key, source, target, blocks, factor):
    def block_of(axis_at):
        return (jnp.arange(values.shape[axis_at]) // (values.shape[axis_at] // blocks)).reshape((-1,) + (1,) * (values.ndim - 1 - axis_at))

    one_side = jax.random.permutation(key, blocks)[block_of(target)]
    far = (block_of(target) + blocks // 2) % blocks
    return jnp.where((block_of(source) == one_side) | (block_of(source) == far), factor * values, values)


def level_of(stream_key, dims, shards, least, high):
    loudness, own = 1.0, jax.random.fold_in(stream_key, 6)
    for dim, shards_of in shards:
        draws = jnp.exp(jax.random.uniform(jax.random.fold_in(own, dim), (shards_of,), jnp.float32, least / len(shards), high / len(shards)))
        loudness = loudness * jnp.repeat(draws, dims[dim] // shards_of).reshape([-1 if axis == dim else 1 for axis in range(len(dims))])
    return loudness


def bell_draw(stream_key, dims, scale, reach, pieces=(), held_as=jnp.bfloat16):
    level = level_of(stream_key, dims, pieces, -0.22, 0.18) if pieces else 1.0
    values = jax.random.normal(stream_key, dims, jnp.float32) * scale * level
    return jnp.minimum(jnp.maximum(values, -reach), reach).astype(held_as)


def noise_with(rng, extent, deviation, limit, shards, heavy, kind=jnp.bfloat16):
    drawn = deviation * jax.random.normal(rng, extent, jnp.float32)
    if shards:
        drawn = drawn * level_of(rng, extent, shards, -0.22, 0.18)
    return jnp.clip(spiked(drawn, jax.random.fold_in(rng, 3), *heavy), -limit, limit).astype(kind)


def setup_inputs(seed: int = 0) -> dict:
    key_list = jax.random.split(jax.random.key(seed), 24)
    return {
        "hidden_in": bell_draw(key_list[0], (BATCH_SEQUENCES, MODEL_DIM), 1.0, 6.0, ((1, 128),)),
        "norm_gain": jnp.clip(1.0 + 0.1 * jax.random.normal(key_list[1], (MODEL_DIM,), jnp.float32), 0.5, 1.5),
        "w_ssm_in": bell_draw(key_list[2], (MODEL_DIM, E), MODEL_DIM ** -0.5, 0.09375, ((1, 128),)),
        "w_ssm_gate": bell_draw(key_list[3], (MODEL_DIM, E), MODEL_DIM ** -0.5, 0.09375, ((1, 128),)),
        "conv_weight": bell_draw(key_list[4], (KC, E), KC ** -0.5, 3.0, ((1, 128),), jnp.float32),
        "conv_bias": jnp.clip(jax.random.uniform(key_list[5], (E,), jnp.float32, -0.5, 0.5) * level_of(key_list[5], (E,), ((0, 128),), -0.4, 0.0), -0.5, 0.5),
        "conv_state": bell_draw(key_list[6], (BATCH_SEQUENCES, KC - 1, E), 1.0, 6.0, ((2, 128),)),
        "w_state_proj": bell_draw(key_list[7], (E, DTR + 2 * NS), E ** -0.5, 0.0625, ((0, 128),)),
        "w_step": bell_draw(key_list[8], (DTR, E), DTR ** -0.5, 0.375, ((1, 128),)),
        "step_bias": jnp.clip(-4.0 + 3.0 * jax.random.uniform(key_list[9], (E,), jnp.float32) ** level_of(key_list[9], (E,), ((0, 128),), -0.2, 0.2), -4.0, -1.0),
        "log_decay": jnp.clip(2.7 * jax.random.uniform(key_list[10], (NS, E), jnp.float32) ** level_of(key_list[10], (NS, E), ((1, 128),), -0.2, 0.2), 0.0, 2.7),
        "skip_gain": jnp.clip(0.5 + 1.0 * jax.random.uniform(key_list[11], (E,), jnp.float32) ** level_of(key_list[11], (E,), ((0, 128),), -0.2, 0.2), 0.5, 1.5),
        "ssm_state": bell_draw(key_list[12], (BATCH_SEQUENCES, NS, E), 1.0, 6.0, ((2, 128),), jnp.float32),
        "w_ssm_out": noise_with(key_list[13], (E, MODEL_DIM), E ** -0.5, 0.25, ((0, 128),), (0, 1, 128, 5.5)),
        "w_query": draw_w_query(jax.random.fold_in(key_list[23], 71), 0),
        "key_projection": bell_draw(key_list[15], (MODEL_DIM, KEY_VALUE_HEADS * HEAD_SIZE), MODEL_DIM ** -0.5, 0.09375, ((1, 4),)),
        "value_projection": bell_draw(key_list[16], (MODEL_DIM, KEY_VALUE_HEADS * HEAD_SIZE), MODEL_DIM ** -0.5, 0.09375, ((1, 4),)),
        "w_attn_out": bell_draw(key_list[17], (QUERY_HEADS * HEAD_SIZE, MODEL_DIM), (QUERY_HEADS * HEAD_SIZE) ** -0.5, 0.125, ((0, 4), (1, 32))),
        "w_mlp_gate": bell_draw(key_list[18], (MODEL_DIM, FF), MODEL_DIM ** -0.5, 0.09375, ((1, 128),)),
        "w_mlp_up": bell_draw(key_list[19], (MODEL_DIM, FF), MODEL_DIM ** -0.5, 0.09375, ((1, 128),)),
        "w_mlp_down": noise_with(key_list[20], (FF, MODEL_DIM), FF ** -0.5, 0.1875, ((0, 128),), (0, 1, 128, 5.5)),
        "cached_inputs": bell_draw(key_list[21], (BATCH_SEQUENCES, WINDOW_SPAN, MODEL_DIM), 1.0, 6.0, ((0, 32),)),
        "window_lengths": draw_window_lengths(jax.random.fold_in(key_list[23], 71), 0),
    }


epsilon = 1e-05
rope_base = 10000.0

def apply_rotary(head_values, positions):
    half_dim = head_values.shape[-1] // 2
    frequency = rope_base ** (-(jnp.arange(half_dim, dtype=jnp.float32) * 2.0) / head_values.shape[-1])
    angles = positions[..., None, None] * frequency
    cosine = jnp.cos(angles)
    sine_part = jnp.sin(angles)
    front_half = head_values[..., :half_dim]
    back_half = head_values[..., half_dim:]
    return jnp.concatenate([front_half * cosine - back_half * sine_part, back_half * cosine + front_half * sine_part], axis=-1)

def reference(hidden_in, norm_gain, w_ssm_in, w_ssm_gate, conv_weight, conv_bias, conv_state, w_state_proj, w_step, step_bias, log_decay, skip_gain, ssm_state, w_ssm_out, w_query, key_projection, value_projection, w_attn_out, w_mlp_gate, w_mlp_up, w_mlp_down, cached_inputs, window_lengths):
    hidden_f = hidden_in.astype(jnp.float32)
    row_scale = lax.rsqrt(lax.optimization_barrier(jnp.mean(hidden_f * hidden_f, axis=1, keepdims=True)) + epsilon)
    normed_input = (hidden_f * row_scale * norm_gain).astype(jnp.bfloat16)
    ssm_input = jnp.dot(normed_input, w_ssm_in, preferred_element_type=jnp.float32).astype(jnp.bfloat16)
    gate_input = jnp.dot(normed_input, w_ssm_gate, preferred_element_type=jnp.float32)
    past_inputs = conv_state.astype(jnp.float32)
    conv_sum = conv_bias + lax.optimization_barrier(jnp.sum(past_inputs * conv_weight[:-1][None], axis=1)) + conv_weight[-1] * lax.optimization_barrier(ssm_input).astype(jnp.float32)
    conv_out = jax.nn.silu(conv_sum)
    low_rank = jnp.dot(conv_out.astype(jnp.bfloat16), w_state_proj, preferred_element_type=jnp.float32)
    step_low = low_rank[:, :DTR].astype(jnp.bfloat16)
    input_map = low_rank[:, DTR:DTR + NS]
    output_map = low_rank[:, DTR + NS:]
    step_size = jax.nn.softplus(jnp.dot(step_low, w_step, preferred_element_type=jnp.float32) + step_bias)
    decay_rate = jnp.exp(log_decay)
    state_out = jnp.exp(-step_size[:, None, :] * decay_rate[None]) * ssm_state + step_size[:, None, :] * input_map[:, :, None] * conv_out[:, None, :]
    ssm_mixed = lax.optimization_barrier(jnp.sum(state_out * output_map[:, :, None], axis=1)) + skip_gain * conv_out
    ssm_gated = (ssm_mixed * jax.nn.silu(gate_input)).astype(jnp.bfloat16)
    ssm_term = jnp.dot(ssm_gated, w_ssm_out, preferred_element_type=jnp.float32)
    gate_act = jnp.dot(normed_input, w_mlp_gate, preferred_element_type=jnp.float32)
    up_act = jnp.dot(normed_input, w_mlp_up, preferred_element_type=jnp.float32)
    mlp_hidden = (jax.nn.silu(gate_act) * up_act).astype(jnp.bfloat16)
    mlp_term = jnp.dot(mlp_hidden, w_mlp_down, preferred_element_type=jnp.float32)
    fresh_position = window_lengths.astype(jnp.float32)
    query = apply_rotary(jnp.dot(normed_input, w_query, preferred_element_type=jnp.float32).reshape(BATCH_SEQUENCES, QUERY_HEADS, HEAD_SIZE), fresh_position).astype(jnp.bfloat16)
    fresh_key = apply_rotary(jnp.dot(normed_input, key_projection, preferred_element_type=jnp.float32).reshape(BATCH_SEQUENCES, KEY_VALUE_HEADS, HEAD_SIZE), fresh_position).astype(jnp.bfloat16)
    fresh_value = jnp.dot(normed_input, value_projection, preferred_element_type=jnp.float32).astype(jnp.bfloat16).reshape(BATCH_SEQUENCES, KEY_VALUE_HEADS, HEAD_SIZE)
    heads_per_group = QUERY_HEADS // KEY_VALUE_HEADS
    attention_scale = HEAD_SIZE ** (-0.5)

    def one_row(row_args):
        window_row_inputs, query_for_row, row_key, row_value, row_length = row_args
        slot_ids = jnp.arange(WINDOW_SPAN, dtype=jnp.int32)
        window_key_rows = jnp.dot(window_row_inputs, key_projection, preferred_element_type=jnp.float32).reshape(WINDOW_SPAN, KEY_VALUE_HEADS, HEAD_SIZE)
        window_key_rows = apply_rotary(window_key_rows, slot_ids.astype(jnp.float32)).astype(jnp.bfloat16)
        window_value_rows = jnp.dot(window_row_inputs, value_projection, preferred_element_type=jnp.float32).astype(jnp.bfloat16).reshape(WINDOW_SPAN, KEY_VALUE_HEADS, HEAD_SIZE)
        grouped_query = query_for_row.astype(jnp.float32).reshape(KEY_VALUE_HEADS, heads_per_group, HEAD_SIZE)
        scores = jnp.einsum('kgd,wkd->kgw', grouped_query, window_key_rows.astype(jnp.float32)) * attention_scale
        fresh_score = jnp.einsum('kgd,kd->kg', grouped_query, row_key.astype(jnp.float32)) * attention_scale
        is_valid = slot_ids < row_length
        scores = jnp.where(is_valid[None, None, :], scores, -1e+30)
        row_max = jnp.maximum(lax.optimization_barrier(jnp.max(scores, axis=-1)), fresh_score)
        weights = jnp.where(is_valid[None, None, :], jnp.exp(scores - row_max[..., None]), 0.0)
        weight_new = jnp.exp(fresh_score - row_max)
        row_total = lax.optimization_barrier(jnp.sum(weights, axis=-1)) + weight_new
        weighted = jnp.einsum('kgw,wkd->kgd', weights, window_value_rows.astype(jnp.float32)) + weight_new[..., None] * row_value.astype(jnp.float32)[:, None, :]
        return (weighted / row_total[..., None]).reshape(QUERY_HEADS * HEAD_SIZE).astype(jnp.bfloat16)
    attended = lax.map(one_row, (cached_inputs, query, fresh_key, fresh_value, window_lengths))
    attn_term = jnp.dot(attended, w_attn_out, preferred_element_type=jnp.float32)
    hidden_out = (hidden_f + (ssm_term + mlp_term + attn_term)).astype(jnp.bfloat16)
    return (hidden_out, state_out)
```

```python
import jax
import jax.numpy as jnp
import numpy as np
from jax import lax
from jax.experimental import pallas as pl
from jax.experimental.pallas import tpu as pltpu
from jax.sharding import Mesh
from jax.sharding import PartitionSpec as P

HEAD_SIZE = 128
GRP_SEQ = ("grp", "seq_0", "seq_1", "seq_2")
SEQ = ("seq_0", "seq_1", "seq_2")
EPSILON = 1e-05
ROPE_BASE = 10000.0
F32 = jnp.float32
BF16 = jnp.bfloat16
NT = (((1,), (1,)), ((), ()))
TN = (((0,), (0,)), ((), ()))
RING = 4
ROWS = 144
SLOT = 16


def rotary_tables(count):
    half = HEAD_SIZE // 2
    frequency = np.float32(ROPE_BASE) ** (
        -(np.arange(half, dtype=np.float32) * np.float32(2.0)) / np.float32(HEAD_SIZE)
    )
    angles = np.arange(count, dtype=np.float32)[:, None] * frequency.astype(np.float32)
    cosine = np.cos(angles.astype(np.float64)).astype(np.float32)
    sine = np.sin(angles.astype(np.float64)).astype(np.float32)
    return (
        np.concatenate([cosine, cosine], axis=1),
        np.concatenate([-sine, sine], axis=1),
    )


def shifted(value, axis, step):
    size = lax.axis_size(axis)
    return lax.ppermute(value, axis, [(i, (i + step) % size) for i in range(size)])


def from_ring(value, axis):
    ahead = shifted(value, axis, 1)
    behind = shifted(value, axis, 3)
    across = shifted(value, axis, 2)
    return [value, ahead, across, behind]


def dot(a, b):
    return jnp.dot(a, b, preferred_element_type=F32)


def vmem_call(kernel, out_shapes, smem_count, operands, scratch=()):
    smem = pl.BlockSpec(memory_space=pltpu.SMEM)
    vmem = pl.BlockSpec(memory_space=pltpu.VMEM)
    return pl.pallas_call(
        kernel,
        out_shape=out_shapes,
        in_specs=[smem] * smem_count + [vmem] * (len(operands) - smem_count),
        out_specs=jax.tree.map(lambda _: vmem, out_shapes),
        scratch_shapes=list(scratch),
    )(*operands)


def window_kernel(place, rows, w_key, w_value, cosines, sines, key_out, value_out, *, chunk):
    step = pl.program_id(0)
    per_seq = 512 // chunk
    start = (step % per_seq) * chunk
    length = place[4 + step // per_seq]

    @pl.when(start < length)
    def _():
        block = rows[0]
        keys = dot(block, w_key[...])
        begin = pl.multiple_of(start, chunk)
        cos = cosines[pl.ds(begin, chunk), :]
        sin = sines[pl.ds(begin, chunk), :]
        for head in range(keys.shape[1] // HEAD_SIZE):
            part = keys[:, head * HEAD_SIZE : (head + 1) * HEAD_SIZE]
            turned = part * cos + pltpu.roll(part, HEAD_SIZE // 2, 1) * sin
            key_out[0, :, head * HEAD_SIZE : (head + 1) * HEAD_SIZE] = turned.astype(BF16)
        value_out[0] = dot(block, w_value[...]).astype(BF16)

    @pl.when(start >= length)
    def _():
        key_out[...] = jnp.zeros_like(key_out)
        value_out[...] = jnp.zeros_like(value_out)


def window_rows(place, cached, w_key, w_value, cosines, sines):
    seqs, window, width = cached.shape
    chunk = 256
    per_seq = window // chunk
    columns = w_key.shape[1]
    whole = pl.BlockSpec(memory_space=pltpu.VMEM)
    out = jax.ShapeDtypeStruct((seqs, window, columns), BF16)

    def rows_at(i, place):
        inside = (i % per_seq) * chunk < place[4 + i // per_seq]
        return (i // per_seq, jnp.where(inside, i % per_seq, 0), 0)

    def out_at(i, place):
        return (i // per_seq, i % per_seq, 0)

    import functools

    return pl.pallas_call(
        functools.partial(window_kernel, chunk=chunk),
        out_shape=(out, out),
        grid_spec=pltpu.PrefetchScalarGridSpec(
            num_scalar_prefetch=1,
            grid=(seqs * per_seq,),
            in_specs=[pl.BlockSpec((1, chunk, width), rows_at), whole, whole, whole, whole],
            out_specs=[
                pl.BlockSpec((1, chunk, columns), out_at),
                pl.BlockSpec((1, chunk, columns), out_at),
            ],
        ),
    )(place, cached, w_key, w_value, cosines, sines)


def chunk_at(j):
    return j // 32, (j // 8) % 4, (j // 2) % 4, j % 2


def inner_kernel(place, near, far, gain, w_in, w_proj, past, params, normed_out, conv_out, low_out):
    z, x, y, c = place[0], place[1], place[2], place[3]
    total = jnp.zeros(near.shape[1:], F32)
    for slot in range(near.shape[0]):
        a = near[slot].astype(F32)
        b = far[slot].astype(F32)
        total = total + a * a + b * b
    width = gain.shape[0] * gain.shape[1]
    mean = jnp.sum(total, axis=0, keepdims=True) * (1.0 / width)
    scale = lax.rsqrt(mean + EPSILON)
    rows = near.shape[1]
    for j in range(gain.shape[0]):
        jz, jx, jy, jc = chunk_at(j)
        slot = (
            lax.rem(y - jy + RING, RING) * 16
            + lax.rem(x - jx + RING, RING) * 4
            + lax.rem(z - jz + RING, RING)
        )
        raw = jnp.where(c == jc, near[slot].astype(F32), far[slot].astype(F32))
        normed_out[j * rows : (j + 1) * rows, :] = (raw * scale * gain[j]).astype(BF16)
    fresh = dot(w_in[...], normed_out[...]).astype(BF16).astype(F32)
    mixed = params[:, 20:21] + params[:, 19:20] * fresh
    for k in range(past.shape[0]):
        mixed = mixed + past[k].astype(F32) * params[:, 16 + k : 17 + k]
    conv = jax.nn.silu(mixed)
    conv_out[...] = conv
    low = lax.dot_general(w_proj[...], conv.astype(BF16), TN, preferred_element_type=F32)
    low_out[c, :, 0:96] = low[0:ROWS, :]
    low_out[1 - c, :, 0:96] = low[ROWS:, :]


def gate_kernel(normed, w_gate, w_mlp_gate, w_mlp_up, w_mlp_down, gate_out, term_out):
    gate_out[...] = jax.nn.silu(dot(w_gate[...], normed[...]))
    act = jax.nn.silu(dot(w_mlp_gate[...], normed[...])) * dot(w_mlp_up[...], normed[...])
    term_out[...] = lax.dot_general(
        act.astype(BF16), w_mlp_down[...], TN, preferred_element_type=F32
    )


def attention_kernel(
    place, normed, w_query, w_key, w_value, keys, values, cosines, sines, s0, s1, s2, s3, out
):
    seqs, window = keys.shape[0], keys.shape[1]
    kv_heads = keys.shape[2] // HEAD_SIZE
    group = w_query.shape[1] // keys.shape[2]
    batch = normed.shape[1]
    first = place[7] * seqs
    row = lax.broadcasted_iota(jnp.int32, (8, batch), 0)
    column = lax.broadcasted_iota(jnp.int32, (8, batch), 1)
    pick = jnp.where((column == first + row) & (row < seqs), 1.0, 0.0).astype(BF16)
    own = lax.dot_general(pick, normed[...], NT, preferred_element_type=F32).astype(BF16)
    query = dot(own, w_query[...])
    fresh_key = dot(own, w_key[...])
    fresh_value = dot(own, w_value[...]).astype(BF16).astype(F32)
    scale = HEAD_SIZE ** (-0.5)
    slot_ids = lax.broadcasted_iota(jnp.int32, (1, window), 1)
    out[0:ROWS, :] = s0[...] + s1[...] + (s2[...] + s3[...])
    out[ROWS:, :] = jnp.zeros((SLOT, HEAD_SIZE), F32)

    def turned(part, cos, sin):
        return (part * cos + pltpu.roll(part, HEAD_SIZE // 2, 1) * sin).astype(BF16)

    for b in range(seqs):
        length = place[4 + b]
        cos = cosines[pl.ds(length, 1), :]
        sin = sines[pl.ds(length, 1), :]
        valid = slot_ids < length
        for g in range(kv_heads):
            lanes = slice(g * HEAD_SIZE, (g + 1) * HEAD_SIZE)
            heads = [
                query[b : b + 1, (g * group + i) * HEAD_SIZE : (g * group + i + 1) * HEAD_SIZE]
                for i in range(group)
            ]
            stacked = jnp.concatenate(heads + [jnp.zeros((8 - group, HEAD_SIZE), F32)], axis=0)
            q = turned(stacked, cos, sin)
            k_new = turned(jnp.broadcast_to(fresh_key[b : b + 1, lanes], (8, HEAD_SIZE)), cos, sin)
            scores = (
                lax.dot_general(q, keys[b, :, lanes], NT, preferred_element_type=F32) * scale
            )
            fresh = (
                jnp.sum(q.astype(F32) * k_new.astype(F32), axis=1, keepdims=True) * scale
            )
            scores = jnp.where(valid, scores, -1e30)
            top = jnp.maximum(jnp.max(scores, axis=1, keepdims=True), fresh)
            weights = jnp.where(valid, jnp.exp(scores - top), 0.0)
            weight_new = jnp.exp(fresh - top)
            denominator = jnp.sum(weights, axis=1, keepdims=True) + weight_new
            summed = dot(weights.astype(BF16), values[b, :, lanes])
            summed = summed + weight_new * fresh_value[b : b + 1, lanes]
            result = (summed / denominator).astype(BF16).astype(F32)
            at = ROWS + (b * kv_heads + g) * group
            out[at : at + group, :] = result[0:group, :]


def outer_kernel(
    place, near, far, w_step, params, conv, gate, state, w_out, term, w_attn, state_out,
    keep_out, send_out, total,
):
    z, x, y, c, seq = place[0], place[1], place[2], place[3], place[7]
    batch = conv.shape[1]
    mine = c == 0
    near_low = near[0:ROWS, 0:batch]
    far_low = far[0:ROWS, 0:batch]
    low = jnp.concatenate(
        [jnp.where(mine, near_low, far_low), jnp.where(mine, far_low, near_low)], axis=0
    )
    rank = w_step.shape[1]
    states = state.shape[0]
    step = jax.nn.softplus(dot(w_step[...], low[0:rank].astype(BF16)) + params[:, 21:22])
    conv_value = conv[...]
    driven = step * conv_value
    mixed = params[:, 22:23] * conv_value
    for n in range(states):
        decay = jnp.exp(-step * params[:, n : n + 1])
        fresh = decay * state[n] + driven * low[rank + n : rank + n + 1]
        state_out[n] = fresh
        mixed = mixed + fresh * low[rank + states + n : rank + states + n + 1]
    gated = (mixed * gate[...]).astype(BF16)
    total[...] = term[...] + lax.dot_general(gated, w_out[...], TN, preferred_element_type=F32)

    slots = near.shape[0] - ROWS
    attended = jnp.concatenate([near[ROWS:, :], far[ROWS:, :]], axis=0).astype(BF16)
    seqs = 3
    heads = w_attn.shape[0] // HEAD_SIZE
    token = lax.broadcasted_iota(jnp.int32, (batch, 2 * slots), 0)
    source = lax.broadcasted_iota(jnp.int32, (batch, 2 * slots), 1)
    owner = token // seqs
    kx = lax.rem(x - owner // 8 + RING, RING)
    ky = lax.rem(y - (owner // 2) % 4 + RING, RING)
    kc = jnp.where(owner % 2 == c, 0, 1)
    at = kc * slots + (ky * RING + kx) * SLOT + (token % seqs) * heads
    attn = jnp.zeros((batch, w_attn.shape[1]), F32)
    for h in range(heads):
        pick = jnp.where(source == at + h, 1.0, 0.0).astype(BF16)
        rows = dot(pick, attended).astype(BF16)
        attn = attn + dot(rows, w_attn[h * HEAD_SIZE : (h + 1) * HEAD_SIZE, :])
    start = pl.multiple_of(seq * HEAD_SIZE, HEAD_SIZE)
    total[:, pl.ds(start, HEAD_SIZE)] = total[:, pl.ds(start, HEAD_SIZE)] + attn

    rows = keep_out.shape[1]
    for i in range(total.shape[1] // HEAD_SIZE):
        block = total[:, i * HEAD_SIZE : (i + 1) * HEAD_SIZE].T.astype(BF16)
        for q in range(0, HEAD_SIZE // rows, 2):
            jz, jx, jy, _ = chunk_at(i * (HEAD_SIZE // rows) + q)
            slot = (
                lax.rem(jz - z + RING, RING) * 16
                + lax.rem(jx - x + RING, RING) * 4
                + lax.rem(jy - y + RING, RING)
            )
            even = block[q * rows : (q + 1) * rows, :]
            odd = block[(q + 1) * rows : (q + 2) * rows, :]
            keep_out[slot] = jnp.where(mine, even, odd)
            send_out[slot] = jnp.where(mine, odd, even)


def sum_over_ring(parts, axis):
    ahead = shifted(parts[1], axis, 1)
    behind = shifted(parts[3], axis, 3)
    across = shifted(parts[2], axis, 2)
    arrived = [p.astype(F32) for p in (parts[0], ahead, across, behind)]
    return (arrived[0] + arrived[1]) + (arrived[2] + arrived[3])


def per_device(
    hidden_in,
    norm_gain,
    w_ssm_in,
    w_ssm_gate,
    conv_weight,
    conv_bias,
    conv_state,
    w_state_proj,
    w_step,
    step_bias,
    log_decay,
    skip_gain,
    ssm_state,
    w_ssm_out,
    w_query,
    key_projection,
    value_projection,
    w_attn_out,
    w_mlp_gate,
    w_mlp_up,
    w_mlp_down,
    cached_inputs,
    window_lengths,
):
    batch, features = hidden_in.shape
    width = norm_gain.shape[0]
    channels = w_ssm_in.shape[1]
    seqs, window, _ = cached_inputs.shape
    z, x, y, c = (lax.axis_index(a) for a in GRP_SEQ)
    seq = lax.axis_index(SEQ)
    lengths_own = lax.dynamic_slice_in_dim(window_lengths, seq * seqs, seqs, 0)
    place = jnp.concatenate(
        [jnp.stack([z, x, y, c]).astype(jnp.int32), lengths_own, seq[None].astype(jnp.int32)]
    )
    cosines, sines = (jnp.asarray(t) for t in rotary_tables(window + 8))
    params = jnp.concatenate(
        [
            jnp.exp(log_decay).T,
            conv_weight.T,
            conv_bias[:, None],
            step_bias[:, None],
            skip_gain[:, None],
        ],
        axis=1,
    )
    gain = jnp.broadcast_to(norm_gain[:, None], (width, batch)).reshape(-1, features, batch)

    hidden = hidden_in.T
    held = hidden[None]
    for axis in ("grp", "seq_0", "seq_1"):
        held = jnp.concatenate(from_ring(held, axis), axis=0)
    other = shifted(held, "seq_2", 1)

    keys, values = window_rows(
        place, cached_inputs, key_projection, value_projection, cosines, sines
    )

    normed, conv, low = vmem_call(
        inner_kernel,
        (
            jax.ShapeDtypeStruct((width, batch), BF16),
            jax.ShapeDtypeStruct((channels, batch), F32),
            jax.ShapeDtypeStruct((2, ROWS, 128), F32),
        ),
        1,
        (
            place, held, other, gain, w_ssm_in.T, w_state_proj,
            jnp.transpose(conv_state, (1, 2, 0)), params,
        ),
    )
    half = low[0] + shifted(low[1], "seq_2", 1)
    arrived = from_ring(half, "grp")
    gate, term = vmem_call(
        gate_kernel,
        (
            jax.ShapeDtypeStruct((channels, batch), F32),
            jax.ShapeDtypeStruct((batch, width), F32),
        ),
        0,
        (normed, w_ssm_gate.T, w_mlp_gate.T, w_mlp_up.T, w_mlp_down),
    )
    packed = vmem_call(
        attention_kernel,
        jax.ShapeDtypeStruct((ROWS + SLOT, HEAD_SIZE), F32),
        1,
        (
            place, normed, w_query, key_projection, value_projection, keys, values,
            cosines, sines, *arrived,
        ),
    )
    for axis in ("seq_0", "seq_1"):
        parts = from_ring(packed, axis)
        summed = (parts[0][:ROWS] + parts[1][:ROWS]) + (parts[2][:ROWS] + parts[3][:ROWS])
        packed = jnp.concatenate([summed] + [p[ROWS:] for p in parts], axis=0)
    packed_other = shifted(packed, "seq_2", 1)

    piece = jax.ShapeDtypeStruct((64, features, batch), BF16)
    state_new, keep, send = vmem_call(
        outer_kernel,
        (jax.ShapeDtypeStruct((log_decay.shape[0], channels, batch), F32), piece, piece),
        1,
        (
            place, packed, packed_other, w_step.T, params, conv, gate,
            jnp.transpose(ssm_state, (1, 2, 0)), w_ssm_out, term, w_attn_out,
        ),
        (pltpu.VMEM((batch, width), F32),),
    )
    came = shifted(send, "seq_2", 1)
    parts = [
        (keep[16 * k : 16 * k + 16].astype(F32) + came[16 * k : 16 * k + 16].astype(F32)).astype(BF16)
        for k in range(RING)
    ]
    total = sum_over_ring(parts, "grp")
    parts = [total[4 * k : 4 * k + 4].astype(BF16) for k in range(RING)]
    total = sum_over_ring(parts, "seq_0")
    parts = [total[k].astype(BF16) for k in range(RING)]
    total = sum_over_ring(parts, "seq_1")
    hidden_out = (hidden.astype(F32) + total).astype(BF16).T
    return (hidden_out, jnp.transpose(state_new, (2, 0, 1)))


def solution(mesh):
    torus = Mesh(
        mesh.devices.reshape(mesh.shape["grp"], 4, 4, 2), ("grp", "seq_0", "seq_1", "seq_2")
    )
    placed = (
        P(None, GRP_SEQ),
        P(),
        P(None, GRP_SEQ),
        P(None, GRP_SEQ),
        P(None, GRP_SEQ),
        P(GRP_SEQ),
        P(None, None, GRP_SEQ),
        P(GRP_SEQ, None),
        P(None, GRP_SEQ),
        P(GRP_SEQ),
        P(None, GRP_SEQ),
        P(GRP_SEQ),
        P(None, None, GRP_SEQ),
        P(GRP_SEQ, None),
        P(None, "grp"),
        P(None, "grp"),
        P(None, "grp"),
        P("grp", SEQ),
        P(None, GRP_SEQ),
        P(None, GRP_SEQ),
        P(GRP_SEQ, None),
        P(SEQ, None, None),
        P(),
    )
    return jax.shard_map(
        per_device,
        mesh=torus,
        in_specs=placed,
        out_specs=(P(None, GRP_SEQ), P(None, None, GRP_SEQ)),
        check_vma=False,
    )
```

```python
import functools

import jax
import jax.numpy as jnp
import numpy as np
from jax import lax
from jax.experimental import pallas as pl
from jax.experimental.pallas import tpu as pltpu
from jax.sharding import Mesh
from jax.sharding import PartitionSpec as P


HEAD_SIZE = 128
GRP_SEQ = ("grp", "seq_0", "seq_1", "seq_2")
SEQ = ("seq_0", "seq_1", "seq_2")
CHIPS = ("grp", "seq_0", "seq_1")
EPSILON = 1e-05
ROPE_BASE = 10000.0
F32 = jnp.float32
BF16 = jnp.bfloat16
NT = (((1,), (1,)), ((), ()))
TN = (((0,), (0,)), ((), ()))
RING = 4
ROWS = 144
SLOT = 16


def rotary_tables(count):
    half = HEAD_SIZE // 2
    frequency = np.float32(ROPE_BASE) ** (
        -(np.arange(half, dtype=np.float32) * np.float32(2.0)) / np.float32(HEAD_SIZE)
    )
    angles = np.arange(count, dtype=np.float32)[:, None] * frequency.astype(np.float32)
    cosine = np.cos(angles.astype(np.float64)).astype(np.float32)
    sine = np.sin(angles.astype(np.float64)).astype(np.float32)
    return (
        np.concatenate([cosine, cosine], axis=1),
        np.concatenate([-sine, sine], axis=1),
    )


def shifted(value, axis, step):
    size = lax.axis_size(axis)
    return lax.ppermute(value, axis, [(i, (i + step) % size) for i in range(size)])


def from_ring(value, axis):
    arrived = [value]
    for step in (1, 3, 2):
        arrived.append(shifted(value, axis, step))
    return [arrived[0], arrived[1], arrived[3], arrived[2]]


def dot(a, b):
    return jnp.dot(a, b, preferred_element_type=F32)


def here():
    return tuple(lax.axis_index(a).astype(jnp.int32) for a in GRP_SEQ)


def own_seq():
    _, x, y, c = here()
    return (x * RING + y) * 2 + c


def in_vmem(value):
    return pltpu.with_memory_space_constraint(value, pltpu.VMEM)


def vmem_call(kernel, outs, operands, lengths=None, scratch=(), limit=12 << 20):
    smem = pl.BlockSpec(memory_space=pltpu.SMEM)
    vmem = pl.BlockSpec(memory_space=pltpu.VMEM)
    scalars = () if lengths is None else (lengths,)
    return pl.pallas_call(
        kernel,
        out_shape=tuple(pltpu.VMEM(shape, dtype) if inner else jax.ShapeDtypeStruct(shape, dtype) for shape, dtype, inner in outs),
        in_specs=[smem] * len(scalars) + [vmem] * len(operands),
        out_specs=tuple(vmem for _ in outs),
        scratch_shapes=list(scratch),
        compiler_params=pltpu.CompilerParams(vmem_limit_bytes=limit),
    )(*scalars, *(in_vmem(v) for v in operands))


def window_kernel(lengths, rows, w_key, w_value, cosines, sines, key_out, value_out, *, chunk):
    step = pl.program_id(0)
    per_seq = 512 // chunk
    start = (step % per_seq) * chunk
    length = lengths[own_seq() * 3 + step // per_seq]

    @pl.when(start < length)
    def _():
        block = rows[0]
        keys = dot(block, w_key[...])
        begin = pl.multiple_of(start, chunk)
        cos = cosines[pl.ds(begin, chunk), :]
        sin = sines[pl.ds(begin, chunk), :]
        for head in range(keys.shape[1] // HEAD_SIZE):
            part = keys[:, head * HEAD_SIZE : (head + 1) * HEAD_SIZE]
            turned = part * cos + pltpu.roll(part, HEAD_SIZE // 2, 1) * sin
            key_out[0, :, head * HEAD_SIZE : (head + 1) * HEAD_SIZE] = turned.astype(BF16)
        value_out[0] = dot(block, w_value[...]).astype(BF16)

    @pl.when(start >= length)
    def _():
        key_out[...] = jnp.zeros_like(key_out)
        value_out[...] = jnp.zeros_like(value_out)


def window_rows(lengths, cached, w_key, w_value, cosines, sines, chunk=256):
    seqs, window, width = cached.shape
    per_seq = window // chunk
    columns = w_key.shape[1]
    whole = pl.BlockSpec(memory_space=pltpu.VMEM)
    out = jax.ShapeDtypeStruct((seqs, window, columns), BF16)

    def block_at(i, _):
        return (i // per_seq, i % per_seq, 0)

    return pl.pallas_call(
        functools.partial(window_kernel, chunk=chunk),
        out_shape=(out, out),
        grid_spec=pltpu.PrefetchScalarGridSpec(
            num_scalar_prefetch=1,
            grid=(seqs * per_seq,),
            in_specs=[pl.BlockSpec((1, chunk, width), block_at), whole, whole, whole, whole],
            out_specs=[
                pl.BlockSpec((1, chunk, columns), block_at),
                pl.BlockSpec((1, chunk, columns), block_at),
            ],
        ),
        compiler_params=pltpu.CompilerParams(vmem_limit_bytes=24 << 20),
    )(
        lengths,
        pltpu.with_memory_space_constraint(cached, pltpu.HBM),
        *(in_vmem(v) for v in (w_key, w_value, cosines, sines)),
    )


def inner_kernel(near, far, gain, w_in, w_proj, past, taps, bias, normed_out, conv_out, low_out):
    c = lax.axis_index("seq_2").astype(jnp.int32)
    rows, batch = near.shape[1], near.shape[2]
    total = jnp.zeros((rows, batch), F32)
    for slot in range(near.shape[0]):
        a = near[slot].astype(F32)
        b = far[slot].astype(F32)
        total = total + a * a + b * b
    width = gain.shape[0] * gain.shape[1]
    mean = jnp.sum(total, axis=0, keepdims=True) * (1.0 / width)
    scale = lax.rsqrt(mean + EPSILON)
    gains = gain[...].T
    mine = c == 0
    per_gain = gain.shape[1] // rows
    for slot in range(near.shape[0]):
        a = near[slot].astype(F32)
        b = far[slot].astype(F32)
        pair = (jnp.where(mine, a, b), jnp.where(mine, b, a))
        for k in range(2):
            j = 2 * slot + k
            at = (j % per_gain) * rows
            column = gains[at : at + rows, j // per_gain : j // per_gain + 1]
            normed_out[j * rows : (j + 1) * rows, :] = (pair[k] * scale * column).astype(BF16)
    fresh = dot(w_in[...], normed_out[...]).astype(BF16).astype(F32)
    params = jnp.concatenate([taps[...], bias[...], jnp.zeros((3, taps.shape[1]), F32)], axis=0).T
    mixed = params[:, 4:5] + params[:, 3:4] * fresh
    for k in range(past.shape[0]):
        mixed = mixed + past[k].astype(F32) * params[:, k : k + 1]
    conv = jax.nn.silu(mixed)
    conv_out[...] = conv
    low = lax.dot_general(w_proj[...], conv.astype(BF16), TN, preferred_element_type=F32)
    low = jnp.concatenate([low, jnp.zeros((low.shape[0], 128 - batch), F32)], axis=1)
    low_out[c] = low[0:ROWS]
    low_out[1 - c] = low[ROWS:]


def gate_kernel(normed, w_gate, w_mlp_gate, w_mlp_up, gate_out, act_out):
    gate_out[...] = jax.nn.silu(dot(w_gate[...], normed[...]))
    act = jax.nn.silu(dot(w_mlp_gate[...], normed[...])) * dot(w_mlp_up[...], normed[...])
    act_out[...] = act.astype(BF16)


def down_kernel(act, w_mlp_down, term_out):
    term_out[...] = lax.dot_general(act[...], w_mlp_down[...], TN, preferred_element_type=F32)


def attention_kernel(
    lengths, normed, w_query, w_key, w_value, keys, values, cosines, sines, out
):
    seqs, window = keys.shape[0], keys.shape[1]
    kv_heads = keys.shape[2] // HEAD_SIZE
    group = w_query.shape[1] // keys.shape[2]
    batch = normed.shape[1]
    first = own_seq() * seqs
    row = lax.broadcasted_iota(jnp.int32, (8, batch), 0)
    column = lax.broadcasted_iota(jnp.int32, (8, batch), 1)
    pick = jnp.where((column == first + row) & (row < seqs), 1.0, 0.0).astype(BF16)
    own = lax.dot_general(pick, normed[...], NT, preferred_element_type=F32).astype(BF16)
    query = dot(own, w_query[...])
    fresh_key = dot(own, w_key[...])
    fresh_value = dot(own, w_value[...]).astype(BF16).astype(F32)
    scale = HEAD_SIZE ** (-0.5)
    slot_ids = lax.broadcasted_iota(jnp.int32, (1, window), 1)
    out[...] = jnp.zeros((SLOT, HEAD_SIZE), F32)

    def turned(part, cos, sin):
        return (part * cos + pltpu.roll(part, HEAD_SIZE // 2, 1) * sin).astype(BF16)

    for b in range(seqs):
        length = lengths[first + b]
        cos = cosines[pl.ds(length, 1), :]
        sin = sines[pl.ds(length, 1), :]
        valid = slot_ids < length
        for g in range(kv_heads):
            lanes = slice(g * HEAD_SIZE, (g + 1) * HEAD_SIZE)
            heads = [
                query[b : b + 1, (g * group + i) * HEAD_SIZE : (g * group + i + 1) * HEAD_SIZE]
                for i in range(group)
            ]
            stacked = jnp.concatenate(heads + [jnp.zeros((8 - group, HEAD_SIZE), F32)], axis=0)
            q = turned(stacked, cos, sin)
            k_new = turned(jnp.broadcast_to(fresh_key[b : b + 1, lanes], (8, HEAD_SIZE)), cos, sin)
            scores = (
                lax.dot_general(q, keys[b, :, lanes], NT, preferred_element_type=F32) * scale
            )
            fresh = (
                jnp.sum(q.astype(F32) * k_new.astype(F32), axis=1, keepdims=True) * scale
            )
            scores = jnp.where(valid, scores, -1e30)
            top = jnp.maximum(jnp.max(scores, axis=1, keepdims=True), fresh)
            weights = jnp.where(valid, jnp.exp(scores - top), 0.0)
            weight_new = jnp.exp(fresh - top)
            denominator = jnp.sum(weights, axis=1, keepdims=True) + weight_new
            summed = dot(weights.astype(BF16), values[b, :, lanes])
            summed = summed + weight_new * fresh_value[b : b + 1, lanes]
            result = (summed / denominator).astype(BF16).astype(F32)
            at = (b * kv_heads + g) * group
            out[at : at + group, :] = result[0:group, :]


def pack_kernel(s0, s1, s2, s3, attended, out):
    out[0:ROWS, :] = (s0[...] + s1[...]) + (s2[...] + s3[...])
    out[ROWS:, :] = attended[...]


def combine_kernel(p0, p1, p2, p3, out):
    out[0:ROWS, :] = (p0[0:ROWS] + p1[0:ROWS]) + (p2[0:ROWS] + p3[0:ROWS])
    size = p0.shape[0] - ROWS
    for k, part in enumerate((p0, p1, p2, p3)):
        out[ROWS + k * size : ROWS + (k + 1) * size, :] = part[ROWS:, :]


def outer_kernel(
    near, far, w_step, log_decay, step_bias, skip, conv, gate, state, w_out, term, w_attn,
    state_out, keep_out, send_out, total,
):
    _, x, y, c = here()
    seq = own_seq()
    batch = conv.shape[1]
    mine = c == 0
    near_low = near[0:ROWS, 0:batch]
    far_low = far[0:ROWS, 0:batch]
    low = jnp.concatenate(
        [jnp.where(mine, near_low, far_low), jnp.where(mine, far_low, near_low)], axis=0
    )
    rank = w_step.shape[1]
    states = state.shape[0]
    params = jnp.concatenate(
        [jnp.exp(log_decay[...]), step_bias[...], skip[...], jnp.zeros((6, conv.shape[0]), F32)],
        axis=0,
    ).T
    step = jax.nn.softplus(
        dot(w_step[...], low[0:rank].astype(BF16)) + params[:, states : states + 1]
    )
    conv_value = conv[...]
    driven = step * conv_value
    mixed = params[:, states + 1 : states + 2] * conv_value
    for n in range(states):
        decay = jnp.exp(-step * params[:, n : n + 1])
        fresh = decay * state[n] + driven * low[rank + n : rank + n + 1]
        state_out[n] = fresh
        mixed = mixed + fresh * low[rank + states + n : rank + states + n + 1]
    gated = (mixed * gate[...]).astype(BF16)
    total[...] = term[...] + lax.dot_general(gated, w_out[...], TN, preferred_element_type=F32)

    slots = near.shape[0] - ROWS
    attended = jnp.concatenate([near[ROWS:, :], far[ROWS:, :]], axis=0).astype(BF16)
    seqs = 3
    heads = w_attn.shape[0] // HEAD_SIZE
    token = lax.broadcasted_iota(jnp.int32, (batch, 2 * slots), 0)
    source = lax.broadcasted_iota(jnp.int32, (batch, 2 * slots), 1)
    owner = token // seqs
    kx = lax.rem(x - owner // 8 + RING, RING)
    ky = lax.rem(y - (owner // 2) % 4 + RING, RING)
    kc = jnp.where(owner % 2 == c, 0, 1)
    at = kc * slots + (ky * RING + kx) * SLOT + (token % seqs) * heads
    attn = jnp.zeros((batch, w_attn.shape[1]), F32)
    for h in range(heads):
        pick = jnp.where(source == at + h, 1.0, 0.0).astype(BF16)
        rows = dot(pick, attended).astype(BF16)
        attn = attn + dot(rows, w_attn[h * HEAD_SIZE : (h + 1) * HEAD_SIZE, :])
    start = pl.multiple_of(seq * HEAD_SIZE, HEAD_SIZE)
    total[:, pl.ds(start, HEAD_SIZE)] = total[:, pl.ds(start, HEAD_SIZE)] + attn

    rows = keep_out.shape[1]
    for i in range(total.shape[1] // HEAD_SIZE):
        block = total[:, i * HEAD_SIZE : (i + 1) * HEAD_SIZE].T.astype(BF16)
        for q in range(0, HEAD_SIZE // rows, 2):
            slot = (i * (HEAD_SIZE // rows) + q) // 2
            even = block[q * rows : (q + 1) * rows, :]
            odd = block[(q + 1) * rows : (q + 2) * rows, :]
            keep_out[slot] = jnp.where(mine, even, odd)
            send_out[slot] = jnp.where(mine, odd, even)


def block(
    hidden_in,
    norm_gain,
    w_ssm_in,
    w_ssm_gate,
    conv_weight,
    conv_bias,
    conv_state,
    w_state_proj,
    w_step,
    step_bias,
    log_decay,
    skip_gain,
    ssm_state,
    w_ssm_out,
    w_query,
    key_projection,
    value_projection,
    w_attn_out,
    w_mlp_gate,
    w_mlp_up,
    w_mlp_down,
    cached_inputs,
    window_lengths,
):
    batch, features = hidden_in.shape
    width = norm_gain.shape[0]
    channels = w_ssm_in.shape[1]
    window = cached_inputs.shape[1]
    states = log_decay.shape[0]
    cosines, sines = (jnp.asarray(t) for t in rotary_tables(window + 8))

    hidden = hidden_in.T
    copies = jnp.broadcast_to(hidden[None], (64, features, batch))
    held = lax.all_to_all(copies, CHIPS, 0, 0, tiled=True)
    other = shifted(held, "seq_2", 1)

    keys, values = window_rows(
        window_lengths, cached_inputs, key_projection, value_projection, cosines, sines
    )

    normed, conv, low = vmem_call(
        inner_kernel,
        (
            ((width, batch), BF16, True),
            ((channels, batch), F32, True),
            ((2, ROWS, 128), F32, True),
        ),
        (
            held, other, norm_gain.reshape(-1, 128), w_ssm_in.T, w_state_proj,
            jnp.transpose(conv_state, (1, 2, 0)), conv_weight, conv_bias[None],
        ),
    )
    half = low[0] + shifted(low[1], "seq_2", 1)
    arrived = from_ring(half, "grp")
    (attended,) = vmem_call(
        attention_kernel,
        (((SLOT, HEAD_SIZE), F32, True),),
        (normed, w_query, key_projection, value_projection, keys, values, cosines, sines),
        lengths=window_lengths,
    )
    gate, act = vmem_call(
        gate_kernel,
        (((channels, batch), F32, True), ((w_mlp_up.shape[1], batch), BF16, True)),
        (normed, w_ssm_gate.T, w_mlp_gate.T, w_mlp_up.T),
    )
    (term,) = vmem_call(down_kernel, (((batch, width), F32, True),), (act, w_mlp_down))
    (packed,) = vmem_call(
        pack_kernel, (((ROWS + SLOT, HEAD_SIZE), F32, True),), (*arrived, attended)
    )
    for axis in ("seq_0", "seq_1"):
        parts = from_ring(packed, axis)
        size = ROWS + RING * (packed.shape[0] - ROWS)
        (packed,) = vmem_call(combine_kernel, (((size, HEAD_SIZE), F32, True),), parts)
    packed_other = shifted(packed, "seq_2", 1)

    piece = ((64, features, batch), BF16, True)
    state_new, keep, send = vmem_call(
        outer_kernel,
        (((states, channels, batch), F32, False), piece, piece),
        (
            packed, packed_other, w_step.T, log_decay, step_bias[None], skip_gain[None], conv, gate,
            jnp.transpose(ssm_state, (1, 2, 0)), w_ssm_out, term, w_attn_out,
        ),
        scratch=(pltpu.VMEM((batch, width), F32),),
    )
    came = shifted(send, "seq_2", 1)
    summed = (keep.astype(F32) + came.astype(F32)).astype(BF16)
    arrived = lax.all_to_all(summed, CHIPS, 0, 0, tiled=True)
    total = jnp.sum(arrived.astype(F32), axis=0)
    hidden_out = (hidden.astype(F32) + total).astype(BF16).T
    return (hidden_out, jnp.transpose(state_new, (2, 0, 1)))


def solution(mesh):
    torus = Mesh(
        mesh.devices.reshape(mesh.shape["grp"], 4, 4, 2), ("grp", "seq_0", "seq_1", "seq_2")
    )
    placed = (
        P(None, GRP_SEQ),
        P(),
        P(None, GRP_SEQ),
        P(None, GRP_SEQ),
        P(None, GRP_SEQ),
        P(GRP_SEQ),
        P(None, None, GRP_SEQ),
        P(GRP_SEQ, None),
        P(None, GRP_SEQ),
        P(GRP_SEQ),
        P(None, GRP_SEQ),
        P(GRP_SEQ),
        P(None, None, GRP_SEQ),
        P(GRP_SEQ, None),
        P(None, "grp"),
        P(None, "grp"),
        P(None, "grp"),
        P("grp", SEQ),
        P(None, GRP_SEQ),
        P(None, GRP_SEQ),
        P(GRP_SEQ, None),
        P(SEQ, None, None),
        P(),
    )
    return jax.shard_map(
        block,
        mesh=torus,
        in_specs=placed,
        out_specs=(P(None, GRP_SEQ), P(None, None, GRP_SEQ)),
        check_vma=False,
    )
```

```python
import jax
import jax.numpy as jnp
import numpy as np
from jax import lax
from jax.experimental import pallas as pl
from jax.experimental.pallas import tpu as pltpu
from jax.sharding import Mesh
from jax.sharding import PartitionSpec as P


HEAD_SIZE = 128
GRP_SEQ = ("grp", "seq_0", "seq_1", "seq_2")
SEQ = ("seq_0", "seq_1", "seq_2")
CHIPS = ("grp", "seq_0", "seq_1")
EPSILON = 1e-05
ROPE_BASE = 10000.0
F32 = jnp.float32
BF16 = jnp.bfloat16
NT = (((1,), (1,)), ((), ()))
TN = (((0,), (0,)), ((), ()))
RING = 4
ROWS = 144
SLOT = 16
WEIGHT_PIECES = 4


def rotary_tables(count):
    half = HEAD_SIZE // 2
    frequency = np.float32(ROPE_BASE) ** (
        -(np.arange(half, dtype=np.float32) * np.float32(2.0)) / np.float32(HEAD_SIZE)
    )
    angles = np.arange(count, dtype=np.float32)[:, None] * frequency.astype(np.float32)
    cosine = np.cos(angles.astype(np.float64)).astype(np.float32)
    sine = np.sin(angles.astype(np.float64)).astype(np.float32)
    return (
        np.concatenate([cosine, cosine], axis=1),
        np.concatenate([-sine, sine], axis=1),
    )


def shifted(value, axis, step):
    size = lax.axis_size(axis)
    return lax.ppermute(value, axis, [(i, (i + step) % size) for i in range(size)])


def from_ring(value, axis):
    arrived = [value]
    for step in (1, 3, 2):
        arrived.append(shifted(value, axis, step))
    return [arrived[0], arrived[1], arrived[3], arrived[2]]


def dot(a, b):
    return jnp.dot(a, b, preferred_element_type=F32)


def here():
    return tuple(lax.axis_index(a).astype(jnp.int32) for a in GRP_SEQ)


def own_seq():
    _, x, y, c = here()
    return (x * RING + y) * 2 + c


def in_hbm(value):
    return pltpu.with_memory_space_constraint(value, pltpu.HBM)


def in_vmem(value):
    return pltpu.with_memory_space_constraint(value, pltpu.VMEM)


def vmem_call(kernel, outs, operands, fetched=(), scratch=(), limit=12 << 20):
    vmem = pl.BlockSpec(memory_space=pltpu.VMEM)
    anywhere = pl.BlockSpec(memory_space=pl.ANY)
    return pl.pallas_call(
        kernel,
        out_shape=tuple(pltpu.VMEM(shape, dtype) if inner else jax.ShapeDtypeStruct(shape, dtype) for shape, dtype, inner in outs),
        in_specs=[anywhere if k in fetched else vmem for k in range(len(operands))],
        out_specs=tuple(vmem for _ in outs),
        scratch_shapes=list(scratch),
        compiler_params=pltpu.CompilerParams(vmem_limit_bytes=limit),
    )(*((in_hbm if k in fetched else in_vmem)(v) for k, v in enumerate(operands)))


def window_kernel(
    lengths, cached, w_key, w_value, cosines, sines, key_out, value_out,
    rows, weights, cos, sin, turned, plain, row_sem, first_sem, key_sem, value_sem, table_sem, out_sem,
):
    seqs, window, width = cached.shape
    columns = w_key.shape[1]
    first = own_seq() * seqs
    pieces = WEIGHT_PIECES
    step = width // pieces

    def piece_copies(p):
        span = pl.ds(p * step, step)
        return (
            pltpu.make_async_copy(
                w_key.at[span], weights.at[span, pl.ds(0, columns)], key_sem.at[p]
            ),
            pltpu.make_async_copy(
                w_value.at[span], weights.at[span, pl.ds(columns, columns)], value_sem.at[p]
            ),
            pltpu.make_async_copy(cached.at[0, :, span], rows.at[0, :, span], first_sem.at[p]),
        )

    tables = (
        pltpu.make_async_copy(cosines.at[pl.ds(0, window)], cos, table_sem.at[0]),
        pltpu.make_async_copy(sines.at[pl.ds(0, window)], sin, table_sem.at[1]),
    )
    later = [
        pltpu.make_async_copy(cached.at[b], rows.at[b], row_sem.at[b]) for b in range(1, seqs)
    ]
    for p in range(pieces):
        for copy in piece_copies(p):
            copy.start()
    for copy in tables:
        copy.start()
    for copy in later:
        copy.start()

    def finish(b, both):
        for head in range(columns // HEAD_SIZE):
            lanes = slice(head * HEAD_SIZE, (head + 1) * HEAD_SIZE)
            part = both[:, lanes]
            turned[b, :, lanes] = (
                part * cos[...] + pltpu.roll(part, HEAD_SIZE // 2, 1) * sin[...]
            ).astype(BF16)
        plain[b] = both[:, columns:].astype(BF16)

    def out_copies(b):
        return (
            pltpu.make_async_copy(turned.at[b], key_out.at[b], out_sem.at[0, b]),
            pltpu.make_async_copy(plain.at[b], value_out.at[b], out_sem.at[1, b]),
        )

    total = None
    for p in range(pieces):
        for copy in piece_copies(p):
            copy.wait()
        span = slice(p * step, (p + 1) * step)
        part = dot(rows[0, :, span], weights[span, :])
        total = part if total is None else total + part
    for copy in tables:
        copy.wait()
    finish(0, total)
    for copy in out_copies(0):
        copy.start()
    for b in range(1, seqs):
        later[b - 1].wait()
        finish(b, dot(rows[b], weights[...]))
        for copy in out_copies(b):
            copy.start()
    for b in range(seqs):
        for copy in out_copies(b):
            copy.wait()


def window_rows(lengths, cached, w_key, w_value, cosines, sines):
    seqs, window, width = cached.shape
    columns = w_key.shape[1]
    anywhere = pl.BlockSpec(memory_space=pl.ANY)
    out = pltpu.HBM((seqs, window, columns), BF16)
    dma = pltpu.SemaphoreType.DMA
    return pl.pallas_call(
        window_kernel,
        out_shape=(out, out),
        in_specs=[pl.BlockSpec(memory_space=pltpu.SMEM)] + [anywhere] * 5,
        out_specs=(anywhere, anywhere),
        scratch_shapes=[
            pltpu.VMEM((seqs, window, width), BF16),
            pltpu.VMEM((width, 2 * columns), BF16),
            pltpu.VMEM((window, HEAD_SIZE), F32),
            pltpu.VMEM((window, HEAD_SIZE), F32),
            pltpu.VMEM((seqs, window, columns), BF16),
            pltpu.VMEM((seqs, window, columns), BF16),
            dma((seqs,)),
            dma((WEIGHT_PIECES,)),
            dma((WEIGHT_PIECES,)),
            dma((WEIGHT_PIECES,)),
            dma((2,)),
            dma((2, seqs)),
        ],
        compiler_params=pltpu.CompilerParams(vmem_limit_bytes=40 << 20),
    )(lengths, *(in_hbm(v) for v in (cached, w_key, w_value, cosines, sines)))


def inner_kernel(
    near, far, gain, w_in_hbm, w_proj, past, taps, bias, normed_out, conv_out, low_out, w_in, w_sem,
):
    fetch = pltpu.make_async_copy(w_in_hbm, w_in, w_sem)
    fetch.start()
    c = lax.axis_index("seq_2").astype(jnp.int32)
    rows, batch = near.shape[1], near.shape[2]
    total = jnp.zeros((rows, batch), F32)
    for slot in range(near.shape[0]):
        a = near[slot].astype(F32)
        b = far[slot].astype(F32)
        total = total + a * a + b * b
    width = gain.shape[0] * gain.shape[1]
    mean = jnp.sum(total, axis=0, keepdims=True) * (1.0 / width)
    scale = lax.rsqrt(mean + EPSILON)
    gains = gain[...].T
    mine = c == 0
    per_gain = gain.shape[1] // rows
    for slot in range(near.shape[0]):
        a = near[slot].astype(F32)
        b = far[slot].astype(F32)
        pair = (jnp.where(mine, a, b), jnp.where(mine, b, a))
        for k in range(2):
            j = 2 * slot + k
            at = (j % per_gain) * rows
            column = gains[at : at + rows, j // per_gain : j // per_gain + 1]
            normed_out[j * rows : (j + 1) * rows, :] = (pair[k] * scale * column).astype(BF16)
    fetch.wait()
    fresh = dot(w_in[...], normed_out[...]).astype(BF16).astype(F32)
    params = jnp.concatenate([taps[...], bias[...], jnp.zeros((3, taps.shape[1]), F32)], axis=0).T
    mixed = params[:, 4:5] + params[:, 3:4] * fresh
    for k in range(past.shape[0]):
        mixed = mixed + past[k].astype(F32) * params[:, k : k + 1]
    conv = jax.nn.silu(mixed)
    conv_out[...] = conv
    low = lax.dot_general(w_proj[...], conv.astype(BF16), TN, preferred_element_type=F32)
    low = jnp.concatenate([low, jnp.zeros((low.shape[0], 128 - batch), F32)], axis=1)
    low_out[c] = low[0:ROWS]
    low_out[1 - c] = low[ROWS:]


def gate_kernel(normed, w_gate, w_mlp_gate, w_mlp_up, gate_out, act_out):
    gate_out[...] = jax.nn.silu(dot(w_gate[...], normed[...]))
    act = jax.nn.silu(dot(w_mlp_gate[...], normed[...])) * dot(w_mlp_up[...], normed[...])
    act_out[...] = act.astype(BF16)


def down_kernel(act, w_mlp_down, term_out):
    term_out[...] = lax.dot_general(act[...], w_mlp_down[...], TN, preferred_element_type=F32)


def attention_kernel(
    lengths, normed, w_query, w_key, w_value, key_rows, value_rows, cosines, sines, out,
    weights, keys, values, cos_rows, sin_rows, weight_sem, row_sem, table_sem,
):
    seqs, window = keys.shape[0], keys.shape[1]
    columns = keys.shape[2]
    queries = w_query.shape[1]
    kv_heads = columns // HEAD_SIZE
    group = queries // columns
    width, batch = normed.shape
    first = own_seq() * seqs
    pieces = WEIGHT_PIECES
    step = width // pieces

    def piece_copies(p):
        span = pl.ds(p * step, step)
        return (
            pltpu.make_async_copy(
                w_query.at[span], weights.at[span, pl.ds(0, queries)], weight_sem.at[0, p]
            ),
            pltpu.make_async_copy(
                w_key.at[span], weights.at[span, pl.ds(queries, columns)], weight_sem.at[1, p]
            ),
            pltpu.make_async_copy(
                w_value.at[span],
                weights.at[span, pl.ds(queries + columns, columns)],
                weight_sem.at[2, p],
            ),
        )

    row_copies = (
        pltpu.make_async_copy(key_rows, keys, row_sem.at[0]),
        pltpu.make_async_copy(value_rows, values, row_sem.at[1]),
    )
    table_copies = []
    for b in range(seqs):
        at = pl.ds(lengths[first + b], 1)
        table_copies.append(
            pltpu.make_async_copy(cosines.at[at], cos_rows.at[pl.ds(b, 1)], table_sem.at[0, b])
        )
        table_copies.append(
            pltpu.make_async_copy(sines.at[at], sin_rows.at[pl.ds(b, 1)], table_sem.at[1, b])
        )
    for p in range(pieces):
        for copy in piece_copies(p):
            copy.start()
    for copy in (*table_copies, *row_copies):
        copy.start()
    row = lax.broadcasted_iota(jnp.int32, (8, batch), 0)
    column = lax.broadcasted_iota(jnp.int32, (8, batch), 1)
    pick = jnp.where((column == first + row) & (row < seqs), 1.0, 0.0).astype(BF16)
    own = lax.dot_general(pick, normed[...], NT, preferred_element_type=F32).astype(BF16)
    projected = None
    for p in range(pieces):
        for copy in piece_copies(p):
            copy.wait()
        span = slice(p * step, (p + 1) * step)
        part = dot(own[:, span], weights[span, :])
        projected = part if projected is None else projected + part
    query = projected[:, 0:queries]
    fresh_key = projected[:, queries : queries + columns]
    fresh_value = projected[:, queries + columns :].astype(BF16).astype(F32)
    for copy in (*table_copies, *row_copies):
        copy.wait()
    scale = HEAD_SIZE ** (-0.5)
    slot_ids = lax.broadcasted_iota(jnp.int32, (1, window), 1)
    out[...] = jnp.zeros((SLOT, HEAD_SIZE), F32)

    def turned(part, cos, sin):
        return (part * cos + pltpu.roll(part, HEAD_SIZE // 2, 1) * sin).astype(BF16)

    for b in range(seqs):
        length = lengths[first + b]
        cos = cos_rows[b : b + 1, :]
        sin = sin_rows[b : b + 1, :]
        valid = slot_ids < length
        for g in range(kv_heads):
            lanes = slice(g * HEAD_SIZE, (g + 1) * HEAD_SIZE)
            heads = [
                query[b : b + 1, (g * group + i) * HEAD_SIZE : (g * group + i + 1) * HEAD_SIZE]
                for i in range(group)
            ]
            stacked = jnp.concatenate(heads + [jnp.zeros((8 - group, HEAD_SIZE), F32)], axis=0)
            q = turned(stacked, cos, sin)
            k_new = turned(jnp.broadcast_to(fresh_key[b : b + 1, lanes], (8, HEAD_SIZE)), cos, sin)
            scores = (
                lax.dot_general(q, keys[b, :, lanes], NT, preferred_element_type=F32) * scale
            )
            fresh = (
                jnp.sum(q.astype(F32) * k_new.astype(F32), axis=1, keepdims=True) * scale
            )
            scores = jnp.where(valid, scores, -1e30)
            top = jnp.maximum(jnp.max(scores, axis=1, keepdims=True), fresh)
            weights = jnp.where(valid, jnp.exp(scores - top), 0.0)
            weight_new = jnp.exp(fresh - top)
            denominator = jnp.sum(weights, axis=1, keepdims=True) + weight_new
            summed = dot(weights.astype(BF16), values[b, :, lanes])
            summed = summed + weight_new * fresh_value[b : b + 1, lanes]
            result = (summed / denominator).astype(BF16).astype(F32)
            at = (b * kv_heads + g) * group
            out[at : at + group, :] = result[0:group, :]


def attended_rows(lengths, normed, w_query, w_key, w_value, keys, values, cosines, sines):
    anywhere = pl.BlockSpec(memory_space=pl.ANY)
    vmem = pl.BlockSpec(memory_space=pltpu.VMEM)
    dma = pltpu.SemaphoreType.DMA
    width = normed.shape[0]
    return pl.pallas_call(
        attention_kernel,
        out_shape=pltpu.VMEM((SLOT, HEAD_SIZE), F32),
        in_specs=[pl.BlockSpec(memory_space=pltpu.SMEM), vmem] + [anywhere] * 7,
        out_specs=vmem,
        scratch_shapes=[
            pltpu.VMEM((width, w_query.shape[1] + 2 * w_key.shape[1]), BF16),
            pltpu.VMEM(keys.shape, BF16),
            pltpu.VMEM(values.shape, BF16),
            pltpu.VMEM((8, HEAD_SIZE), F32),
            pltpu.VMEM((8, HEAD_SIZE), F32),
            dma((3, WEIGHT_PIECES)),
            dma((2,)),
            dma((2, keys.shape[0])),
        ],
        compiler_params=pltpu.CompilerParams(vmem_limit_bytes=20 << 20),
    )(
        lengths,
        in_vmem(normed),
        *(in_hbm(v) for v in (w_query, w_key, w_value, keys, values, cosines, sines)),
    )


def pack_kernel(s0, s1, s2, s3, attended, out):
    out[0:ROWS, :] = (s0[...] + s1[...]) + (s2[...] + s3[...])
    out[ROWS:, :] = attended[...]


def combine_kernel(p0, p1, p2, p3, out):
    out[0:ROWS, :] = (p0[0:ROWS] + p1[0:ROWS]) + (p2[0:ROWS] + p3[0:ROWS])
    size = p0.shape[0] - ROWS
    for k, part in enumerate((p0, p1, p2, p3)):
        out[ROWS + k * size : ROWS + (k + 1) * size, :] = part[ROWS:, :]


def outer_kernel(
    near, far, w_step, log_decay, step_bias, skip, conv, gate, state, w_out, term, w_attn,
    state_out, keep_out, send_out, total,
):
    _, x, y, c = here()
    seq = own_seq()
    batch = conv.shape[1]
    mine = c == 0
    near_low = near[0:ROWS, 0:batch]
    far_low = far[0:ROWS, 0:batch]
    low = jnp.concatenate(
        [jnp.where(mine, near_low, far_low), jnp.where(mine, far_low, near_low)], axis=0
    )
    rank = w_step.shape[1]
    states = state.shape[0]
    params = jnp.concatenate(
        [jnp.exp(log_decay[...]), step_bias[...], skip[...], jnp.zeros((6, conv.shape[0]), F32)],
        axis=0,
    ).T
    step = jax.nn.softplus(
        dot(w_step[...], low[0:rank].astype(BF16)) + params[:, states : states + 1]
    )
    conv_value = conv[...]
    driven = step * conv_value
    mixed = params[:, states + 1 : states + 2] * conv_value
    for n in range(states):
        decay = jnp.exp(-step * params[:, n : n + 1])
        fresh = decay * state[n] + driven * low[rank + n : rank + n + 1]
        state_out[n] = fresh
        mixed = mixed + fresh * low[rank + states + n : rank + states + n + 1]
    gated = (mixed * gate[...]).astype(BF16)
    total[...] = term[...] + lax.dot_general(gated, w_out[...], TN, preferred_element_type=F32)

    slots = near.shape[0] - ROWS
    attended = jnp.concatenate([near[ROWS:, :], far[ROWS:, :]], axis=0).astype(BF16)
    seqs = 3
    heads = w_attn.shape[0] // HEAD_SIZE
    token = lax.broadcasted_iota(jnp.int32, (batch, 2 * slots), 0)
    source = lax.broadcasted_iota(jnp.int32, (batch, 2 * slots), 1)
    owner = token // seqs
    kx = lax.rem(x - owner // 8 + RING, RING)
    ky = lax.rem(y - (owner // 2) % 4 + RING, RING)
    kc = jnp.where(owner % 2 == c, 0, 1)
    at = kc * slots + (ky * RING + kx) * SLOT + (token % seqs) * heads
    attn = jnp.zeros((batch, w_attn.shape[1]), F32)
    for h in range(heads):
        pick = jnp.where(source == at + h, 1.0, 0.0).astype(BF16)
        rows = dot(pick, attended).astype(BF16)
        attn = attn + dot(rows, w_attn[h * HEAD_SIZE : (h + 1) * HEAD_SIZE, :])
    start = pl.multiple_of(seq * HEAD_SIZE, HEAD_SIZE)
    total[:, pl.ds(start, HEAD_SIZE)] = total[:, pl.ds(start, HEAD_SIZE)] + attn

    rows = keep_out.shape[1]
    for i in range(total.shape[1] // HEAD_SIZE):
        block = total[:, i * HEAD_SIZE : (i + 1) * HEAD_SIZE].T.astype(BF16)
        for q in range(0, HEAD_SIZE // rows, 2):
            slot = (i * (HEAD_SIZE // rows) + q) // 2
            even = block[q * rows : (q + 1) * rows, :]
            odd = block[(q + 1) * rows : (q + 2) * rows, :]
            keep_out[slot] = jnp.where(mine, even, odd)
            send_out[slot] = jnp.where(mine, odd, even)


def block(
    hidden_in,
    norm_gain,
    w_ssm_in,
    w_ssm_gate,
    conv_weight,
    conv_bias,
    conv_state,
    w_state_proj,
    w_step,
    step_bias,
    log_decay,
    skip_gain,
    ssm_state,
    w_ssm_out,
    w_query,
    key_projection,
    value_projection,
    w_attn_out,
    w_mlp_gate,
    w_mlp_up,
    w_mlp_down,
    cached_inputs,
    window_lengths,
):
    batch, features = hidden_in.shape
    width = norm_gain.shape[0]
    channels = w_ssm_in.shape[1]
    window = cached_inputs.shape[1]
    states = log_decay.shape[0]
    cosines, sines = (jnp.asarray(t) for t in rotary_tables(window + 8))

    hidden = hidden_in.T
    copies = jnp.broadcast_to(hidden[None], (64, features, batch))
    held = lax.all_to_all(copies, CHIPS, 0, 0, tiled=True)
    other = shifted(held, "seq_2", 1)

    keys, values = window_rows(
        window_lengths, cached_inputs, key_projection, value_projection, cosines, sines
    )

    normed, conv, low = vmem_call(
        inner_kernel,
        (
            ((width, batch), BF16, True),
            ((channels, batch), F32, True),
            ((2, ROWS, 128), F32, True),
        ),
        (
            held, other, norm_gain.reshape(-1, 128), w_ssm_in.T, w_state_proj,
            jnp.transpose(conv_state, (1, 2, 0)), conv_weight, conv_bias[None],
        ),
        fetched=(3,),
        scratch=(pltpu.VMEM((channels, width), BF16), pltpu.SemaphoreType.DMA),
    )
    half = low[0] + shifted(low[1], "seq_2", 1)
    arrived = from_ring(half, "grp")
    attended = attended_rows(
        window_lengths, normed, w_query, key_projection, value_projection, keys, values,
        cosines, sines,
    )
    gate, act = vmem_call(
        gate_kernel,
        (((channels, batch), F32, True), ((w_mlp_up.shape[1], batch), BF16, True)),
        (normed, w_ssm_gate.T, w_mlp_gate.T, w_mlp_up.T),
    )
    (term,) = vmem_call(down_kernel, (((batch, width), F32, True),), (act, w_mlp_down))
    (packed,) = vmem_call(
        pack_kernel, (((ROWS + SLOT, HEAD_SIZE), F32, True),), (*arrived, attended)
    )
    for axis in ("seq_0", "seq_1"):
        parts = from_ring(packed, axis)
        size = ROWS + RING * (packed.shape[0] - ROWS)
        (packed,) = vmem_call(combine_kernel, (((size, HEAD_SIZE), F32, True),), parts)
    packed_other = shifted(packed, "seq_2", 1)

    piece = ((64, features, batch), BF16, True)
    state_new, keep, send = vmem_call(
        outer_kernel,
        (((states, channels, batch), F32, False), piece, piece),
        (
            packed, packed_other, w_step.T, log_decay, step_bias[None], skip_gain[None], conv, gate,
            jnp.transpose(ssm_state, (1, 2, 0)), w_ssm_out, term, w_attn_out,
        ),
        scratch=(pltpu.VMEM((batch, width), F32),),
    )
    came = shifted(send, "seq_2", 1)
    summed = (keep.astype(F32) + came.astype(F32)).astype(BF16)
    arrived = lax.all_to_all(summed, CHIPS, 0, 0, tiled=True)
    total = jnp.sum(arrived.astype(F32), axis=0)
    hidden_out = (hidden.astype(F32) + total).astype(BF16).T
    return (hidden_out, jnp.transpose(state_new, (2, 0, 1)))


def solution(mesh):
    torus = Mesh(
        mesh.devices.reshape(mesh.shape["grp"], 4, 4, 2), ("grp", "seq_0", "seq_1", "seq_2")
    )
    placed = (
        P(None, GRP_SEQ),
        P(),
        P(None, GRP_SEQ),
        P(None, GRP_SEQ),
        P(None, GRP_SEQ),
        P(GRP_SEQ),
        P(None, None, GRP_SEQ),
        P(GRP_SEQ, None),
        P(None, GRP_SEQ),
        P(GRP_SEQ),
        P(None, GRP_SEQ),
        P(GRP_SEQ),
        P(None, None, GRP_SEQ),
        P(GRP_SEQ, None),
        P(None, "grp"),
        P(None, "grp"),
        P(None, "grp"),
        P("grp", SEQ),
        P(None, GRP_SEQ),
        P(None, GRP_SEQ),
        P(GRP_SEQ, None),
        P(SEQ, None, None),
        P(),
    )
    return jax.shard_map(
        block,
        mesh=torus,
        in_specs=placed,
        out_specs=(P(None, GRP_SEQ), P(None, None, GRP_SEQ)),
        check_vma=False,
    )
```

```python
import jax
import jax.numpy as jnp
import numpy as np
from jax import lax
from jax.experimental import pallas as pl
from jax.experimental.pallas import tpu as pltpu
from jax.sharding import Mesh
from jax.sharding import PartitionSpec as P


HEAD_SIZE = 128
GRP_SEQ = ("grp", "seq_0", "seq_1", "seq_2")
SEQ = ("seq_0", "seq_1", "seq_2")
CHIPS = ("grp", "seq_0", "seq_1")
PLANE = ("seq_0", "seq_1")
EPSILON = 1e-05
ROPE_BASE = 10000.0
F32 = jnp.float32
BF16 = jnp.bfloat16
NT = (((1,), (1,)), ((), ()))
TN = (((0,), (0,)), ((), ()))
RING = 4
ROWS = 144
SLOT = 16
WEIGHT_PIECES = 4


def rotary_tables(count):
    half = HEAD_SIZE // 2
    frequency = np.float32(ROPE_BASE) ** (
        -(np.arange(half, dtype=np.float32) * np.float32(2.0)) / np.float32(HEAD_SIZE)
    )
    angles = np.arange(count, dtype=np.float32)[:, None] * frequency.astype(np.float32)
    cosine = np.cos(angles.astype(np.float64)).astype(np.float32)
    sine = np.sin(angles.astype(np.float64)).astype(np.float32)
    return (
        np.concatenate([cosine, cosine], axis=1),
        np.concatenate([-sine, sine], axis=1),
    )


def shifted(value, axis, step):
    size = lax.axis_size(axis)
    return lax.ppermute(value, axis, [(i, (i + step) % size) for i in range(size)])


def from_ring(value, axis):
    arrived = [value]
    for step in (1, 3, 2):
        arrived.append(shifted(value, axis, step))
    return [arrived[0], arrived[1], arrived[3], arrived[2]]


def dot(a, b):
    return jnp.dot(a, b, preferred_element_type=F32)


def here():
    return tuple(lax.axis_index(a).astype(jnp.int32) for a in GRP_SEQ)


def own_seq():
    _, x, y, c = here()
    return (x * RING + y) * 2 + c


def in_hbm(value):
    return pltpu.with_memory_space_constraint(value, pltpu.HBM)


def in_vmem(value):
    return pltpu.with_memory_space_constraint(value, pltpu.VMEM)


def vmem_call(kernel, outs, operands, fetched=(), scratch=(), limit=12 << 20):
    vmem = pl.BlockSpec(memory_space=pltpu.VMEM)
    anywhere = pl.BlockSpec(memory_space=pl.ANY)
    return pl.pallas_call(
        kernel,
        out_shape=tuple(pltpu.VMEM(shape, dtype) if inner else jax.ShapeDtypeStruct(shape, dtype) for shape, dtype, inner in outs),
        in_specs=[anywhere if k in fetched else vmem for k in range(len(operands))],
        out_specs=tuple(vmem for _ in outs),
        scratch_shapes=list(scratch),
        compiler_params=pltpu.CompilerParams(vmem_limit_bytes=limit),
    )(*((in_hbm if k in fetched else in_vmem)(v) for k, v in enumerate(operands)))


def window_kernel(
    lengths, cached, w_key, w_value, cosines, sines, key_out, value_out,
    rows, weights, cos, sin, turned, plain, row_sem, first_sem, key_sem, value_sem, table_sem, out_sem,
):
    seqs, window, width = cached.shape
    columns = w_key.shape[1]
    first = own_seq() * seqs
    pieces = WEIGHT_PIECES
    step = width // pieces

    def piece_copies(p):
        span = pl.ds(p * step, step)
        return (
            pltpu.make_async_copy(
                w_key.at[span], weights.at[span, pl.ds(0, columns)], key_sem.at[p]
            ),
            pltpu.make_async_copy(
                w_value.at[span], weights.at[span, pl.ds(columns, columns)], value_sem.at[p]
            ),
            pltpu.make_async_copy(cached.at[0, :, span], rows.at[0, :, span], first_sem.at[p]),
        )

    tables = (
        pltpu.make_async_copy(cosines.at[pl.ds(0, window)], cos, table_sem.at[0]),
        pltpu.make_async_copy(sines.at[pl.ds(0, window)], sin, table_sem.at[1]),
    )
    later = [
        pltpu.make_async_copy(cached.at[b], rows.at[b], row_sem.at[b]) for b in range(1, seqs)
    ]
    for p in range(pieces):
        for copy in piece_copies(p):
            copy.start()
    for copy in tables:
        copy.start()
    for copy in later:
        copy.start()

    def finish(b, both):
        for head in range(columns // HEAD_SIZE):
            lanes = slice(head * HEAD_SIZE, (head + 1) * HEAD_SIZE)
            part = both[:, lanes]
            turned[b, :, lanes] = (
                part * cos[...] + pltpu.roll(part, HEAD_SIZE // 2, 1) * sin[...]
            ).astype(BF16)
        plain[b] = both[:, columns:].astype(BF16)

    def out_copies(b):
        return (
            pltpu.make_async_copy(turned.at[b], key_out.at[b], out_sem.at[0, b]),
            pltpu.make_async_copy(plain.at[b], value_out.at[b], out_sem.at[1, b]),
        )

    total = None
    for p in range(pieces):
        for copy in piece_copies(p):
            copy.wait()
        span = slice(p * step, (p + 1) * step)
        part = dot(rows[0, :, span], weights[span, :])
        total = part if total is None else total + part
    for copy in tables:
        copy.wait()
    finish(0, total)
    for copy in out_copies(0):
        copy.start()
    for b in range(1, seqs):
        later[b - 1].wait()
        finish(b, dot(rows[b], weights[...]))
        for copy in out_copies(b):
            copy.start()
    for b in range(seqs):
        for copy in out_copies(b):
            copy.wait()


def window_rows(lengths, cached, w_key, w_value, cosines, sines):
    seqs, window, width = cached.shape
    columns = w_key.shape[1]
    anywhere = pl.BlockSpec(memory_space=pl.ANY)
    out = pltpu.HBM((seqs, window, columns), BF16)
    dma = pltpu.SemaphoreType.DMA
    return pl.pallas_call(
        window_kernel,
        out_shape=(out, out),
        in_specs=[pl.BlockSpec(memory_space=pltpu.SMEM)] + [anywhere] * 5,
        out_specs=(anywhere, anywhere),
        scratch_shapes=[
            pltpu.VMEM((seqs, window, width), BF16),
            pltpu.VMEM((width, 2 * columns), BF16),
            pltpu.VMEM((window, HEAD_SIZE), F32),
            pltpu.VMEM((window, HEAD_SIZE), F32),
            pltpu.VMEM((seqs, window, columns), BF16),
            pltpu.VMEM((seqs, window, columns), BF16),
            dma((seqs,)),
            dma((WEIGHT_PIECES,)),
            dma((WEIGHT_PIECES,)),
            dma((WEIGHT_PIECES,)),
            dma((2,)),
            dma((2, seqs)),
        ],
        compiler_params=pltpu.CompilerParams(vmem_limit_bytes=40 << 20),
    )(lengths, *(in_hbm(v) for v in (cached, w_key, w_value, cosines, sines)))


def inner_kernel(
    near, far, gain, w_in_hbm, w_proj, past, taps, bias, normed_out, conv_out, low_out, w_in, w_sem,
):
    fetch = pltpu.make_async_copy(w_in_hbm, w_in, w_sem)
    fetch.start()
    c = lax.axis_index("seq_2").astype(jnp.int32)
    rows, batch = near.shape[1], near.shape[2]
    total = jnp.zeros((rows, batch), F32)
    for slot in range(near.shape[0]):
        a = near[slot].astype(F32)
        b = far[slot].astype(F32)
        total = total + a * a + b * b
    width = gain.shape[0] * gain.shape[1]
    mean = jnp.sum(total, axis=0, keepdims=True) * (1.0 / width)
    scale = lax.rsqrt(mean + EPSILON)
    gains = gain[...].T
    mine = c == 0
    per_gain = gain.shape[1] // rows
    for slot in range(near.shape[0]):
        a = near[slot].astype(F32)
        b = far[slot].astype(F32)
        pair = (jnp.where(mine, a, b), jnp.where(mine, b, a))
        for k in range(2):
            j = 2 * slot + k
            at = (j % per_gain) * rows
            column = gains[at : at + rows, j // per_gain : j // per_gain + 1]
            normed_out[j * rows : (j + 1) * rows, :] = (pair[k] * scale * column).astype(BF16)
    fetch.wait()
    fresh = dot(w_in[...], normed_out[...]).astype(BF16).astype(F32)
    params = jnp.concatenate([taps[...], bias[...], jnp.zeros((3, taps.shape[1]), F32)], axis=0).T
    mixed = params[:, 4:5] + params[:, 3:4] * fresh
    for k in range(past.shape[0]):
        mixed = mixed + past[k].astype(F32) * params[:, k : k + 1]
    conv = jax.nn.silu(mixed)
    conv_out[...] = conv
    low = lax.dot_general(w_proj[...], conv.astype(BF16), TN, preferred_element_type=F32)
    low = jnp.concatenate([low, jnp.zeros((low.shape[0], 128 - batch), F32)], axis=1)
    low_out[c] = low[0:ROWS]
    low_out[1 - c] = low[ROWS:]


def gate_kernel(normed, w_gate, w_mlp_gate, w_mlp_up, gate_out, act_out):
    gate_out[...] = jax.nn.silu(dot(w_gate[...], normed[...]))
    act = jax.nn.silu(dot(w_mlp_gate[...], normed[...])) * dot(w_mlp_up[...], normed[...])
    act_out[...] = act.astype(BF16)


def down_kernel(act, w_mlp_down, term_out):
    term_out[...] = lax.dot_general(act[...], w_mlp_down[...], TN, preferred_element_type=F32)


def attention_kernel(
    lengths, normed, w_query, w_key, w_value, key_rows, value_rows, cosines, sines, out,
    weights, keys, values, cos_rows, sin_rows, weight_sem, row_sem, table_sem,
):
    seqs, window = keys.shape[0], keys.shape[1]
    columns = keys.shape[2]
    queries = w_query.shape[1]
    kv_heads = columns // HEAD_SIZE
    group = queries // columns
    width, batch = normed.shape
    first = own_seq() * seqs
    pieces = WEIGHT_PIECES
    step = width // pieces

    def piece_copies(p):
        span = pl.ds(p * step, step)
        return (
            pltpu.make_async_copy(
                w_query.at[span], weights.at[span, pl.ds(0, queries)], weight_sem.at[0, p]
            ),
            pltpu.make_async_copy(
                w_key.at[span], weights.at[span, pl.ds(queries, columns)], weight_sem.at[1, p]
            ),
            pltpu.make_async_copy(
                w_value.at[span],
                weights.at[span, pl.ds(queries + columns, columns)],
                weight_sem.at[2, p],
            ),
        )

    row_copies = (
        pltpu.make_async_copy(key_rows, keys, row_sem.at[0]),
        pltpu.make_async_copy(value_rows, values, row_sem.at[1]),
    )
    table_copies = []
    for b in range(seqs):
        at = pl.ds(lengths[first + b], 1)
        table_copies.append(
            pltpu.make_async_copy(cosines.at[at], cos_rows.at[pl.ds(b, 1)], table_sem.at[0, b])
        )
        table_copies.append(
            pltpu.make_async_copy(sines.at[at], sin_rows.at[pl.ds(b, 1)], table_sem.at[1, b])
        )
    for p in range(pieces):
        for copy in piece_copies(p):
            copy.start()
    for copy in (*table_copies, *row_copies):
        copy.start()
    row = lax.broadcasted_iota(jnp.int32, (8, batch), 0)
    column = lax.broadcasted_iota(jnp.int32, (8, batch), 1)
    pick = jnp.where((column == first + row) & (row < seqs), 1.0, 0.0).astype(BF16)
    own = lax.dot_general(pick, normed[...], NT, preferred_element_type=F32).astype(BF16)
    projected = None
    for p in range(pieces):
        for copy in piece_copies(p):
            copy.wait()
        span = slice(p * step, (p + 1) * step)
        part = dot(own[:, span], weights[span, :])
        projected = part if projected is None else projected + part
    query = projected[:, 0:queries]
    fresh_key = projected[:, queries : queries + columns]
    fresh_value = projected[:, queries + columns :].astype(BF16).astype(F32)
    for copy in (*table_copies, *row_copies):
        copy.wait()
    scale = HEAD_SIZE ** (-0.5)
    blocks = [(b, g) for b in range(seqs) for g in range(kv_heads)]
    height = len(blocks) * 8
    spare = jnp.zeros((8 - group, HEAD_SIZE), F32)
    stacked, cos, sin, new_key, new_value = [], [], [], [], []
    for b, g in blocks:
        lanes = slice(g * HEAD_SIZE, (g + 1) * HEAD_SIZE)
        for i in range(group):
            head = g * group + i
            stacked.append(query[b : b + 1, head * HEAD_SIZE : (head + 1) * HEAD_SIZE])
        stacked.append(spare)
        cos.append(jnp.broadcast_to(cos_rows[b : b + 1, :], (8, HEAD_SIZE)))
        sin.append(jnp.broadcast_to(sin_rows[b : b + 1, :], (8, HEAD_SIZE)))
        new_key.append(jnp.broadcast_to(fresh_key[b : b + 1, lanes], (8, HEAD_SIZE)))
        new_value.append(jnp.broadcast_to(fresh_value[b : b + 1, lanes], (8, HEAD_SIZE)))
    cos = jnp.concatenate(cos, axis=0)
    sin = jnp.concatenate(sin, axis=0)

    def turned(part):
        return (part * cos + pltpu.roll(part, HEAD_SIZE // 2, 1) * sin).astype(BF16)

    q = turned(jnp.concatenate(stacked, axis=0))
    k_new = turned(jnp.concatenate(new_key, axis=0))
    scores = jnp.concatenate(
        [
            lax.dot_general(
                q[n * 8 : n * 8 + 8],
                keys[b, :, g * HEAD_SIZE : (g + 1) * HEAD_SIZE],
                NT,
                preferred_element_type=F32,
            )
            for n, (b, g) in enumerate(blocks)
        ],
        axis=0,
    ) * scale
    fresh = jnp.sum(q.astype(F32) * k_new.astype(F32), axis=1, keepdims=True) * scale
    slot_ids = lax.broadcasted_iota(jnp.int32, (height, window), 1)
    owner = lax.broadcasted_iota(jnp.int32, (height, window), 0) // (8 * kv_heads)
    length = jnp.where(
        owner == 0,
        lengths[first],
        jnp.where(owner == 1, lengths[first + 1], lengths[first + 2]),
    )
    valid = slot_ids < length
    scores = jnp.where(valid, scores, -1e30)
    top = jnp.maximum(jnp.max(scores, axis=1, keepdims=True), fresh)
    shares = jnp.where(valid, jnp.exp(scores - top), 0.0)
    share_new = jnp.exp(fresh - top)
    denominator = jnp.sum(shares, axis=1, keepdims=True) + share_new
    rounded = shares.astype(BF16)
    summed = jnp.concatenate(
        [
            dot(rounded[n * 8 : n * 8 + 8], values[b, :, g * HEAD_SIZE : (g + 1) * HEAD_SIZE])
            for n, (b, g) in enumerate(blocks)
        ],
        axis=0,
    )
    result = (summed + share_new * jnp.concatenate(new_value, axis=0)) / denominator
    result = result.astype(BF16).astype(F32)
    out[...] = jnp.zeros((SLOT, HEAD_SIZE), F32)
    for n in range(len(blocks)):
        out[n * group : (n + 1) * group, :] = result[n * 8 : n * 8 + group, :]


def attended_rows(lengths, normed, w_query, w_key, w_value, keys, values, cosines, sines):
    anywhere = pl.BlockSpec(memory_space=pl.ANY)
    vmem = pl.BlockSpec(memory_space=pltpu.VMEM)
    dma = pltpu.SemaphoreType.DMA
    width = normed.shape[0]
    return pl.pallas_call(
        attention_kernel,
        out_shape=pltpu.VMEM((SLOT, HEAD_SIZE), F32),
        in_specs=[pl.BlockSpec(memory_space=pltpu.SMEM), vmem] + [anywhere] * 7,
        out_specs=vmem,
        scratch_shapes=[
            pltpu.VMEM((width, w_query.shape[1] + 2 * w_key.shape[1]), BF16),
            pltpu.VMEM(keys.shape, BF16),
            pltpu.VMEM(values.shape, BF16),
            pltpu.VMEM((8, HEAD_SIZE), F32),
            pltpu.VMEM((8, HEAD_SIZE), F32),
            dma((3, WEIGHT_PIECES)),
            dma((2,)),
            dma((2, keys.shape[0])),
        ],
        compiler_params=pltpu.CompilerParams(vmem_limit_bytes=20 << 20),
    )(
        lengths,
        in_vmem(normed),
        *(in_hbm(v) for v in (w_query, w_key, w_value, keys, values, cosines, sines)),
    )


def pack_kernel(s0, s1, s2, s3, attended, out):
    low = ((s0[...] + s1[...]) + (s2[...] + s3[...])).astype(BF16)
    rows = attended[...].astype(BF16)
    for k in range(out.shape[0]):
        out[k, 0:ROWS, :] = low
        out[k, ROWS:, :] = rows


def combine_kernel(arrived, low_out, rows_out):
    total = arrived[0, 0:ROWS, :].astype(F32)
    rows_out[0:SLOT, :] = arrived[0, ROWS:, :]
    for k in range(1, arrived.shape[0]):
        total = total + arrived[k, 0:ROWS, :].astype(F32)
        rows_out[k * SLOT : (k + 1) * SLOT, :] = arrived[k, ROWS:, :]
    low_out[...] = total


def outer_kernel(
    near, far, near_rows, far_rows, w_step, log_decay, step_bias, skip, conv, gate, state, w_out, term, w_attn,
    state_out, keep_out, send_out, total,
):
    c = lax.axis_index("seq_2").astype(jnp.int32)
    seq = own_seq()
    batch = conv.shape[1]
    mine = c == 0
    near_low = near[:, 0:batch]
    far_low = far[:, 0:batch]
    low = jnp.concatenate(
        [jnp.where(mine, near_low, far_low), jnp.where(mine, far_low, near_low)], axis=0
    )
    rank = w_step.shape[1]
    states = state.shape[0]
    params = jnp.concatenate(
        [jnp.exp(log_decay[...]), step_bias[...], skip[...], jnp.zeros((6, conv.shape[0]), F32)],
        axis=0,
    ).T
    step = jax.nn.softplus(
        dot(w_step[...], low[0:rank].astype(BF16)) + params[:, states : states + 1]
    )
    conv_value = conv[...]
    driven = step * conv_value
    mixed = params[:, states + 1 : states + 2] * conv_value
    for n in range(states):
        decay = jnp.exp(-step * params[:, n : n + 1])
        fresh = decay * state[n] + driven * low[rank + n : rank + n + 1]
        state_out[n] = fresh
        mixed = mixed + fresh * low[rank + states + n : rank + states + n + 1]
    gated = (mixed * gate[...]).astype(BF16)
    total[...] = term[...] + lax.dot_general(gated, w_out[...], TN, preferred_element_type=F32)

    slots = near_rows.shape[0]
    attended = jnp.concatenate([near_rows[...], far_rows[...]], axis=0)
    seqs = 3
    heads = w_attn.shape[0] // HEAD_SIZE
    token = lax.broadcasted_iota(jnp.int32, (batch, 2 * slots), 0)
    source = lax.broadcasted_iota(jnp.int32, (batch, 2 * slots), 1)
    owner = token // seqs
    other_core = jnp.where(owner % 2 == c, 0, 1)
    at = other_core * slots + (owner // 2) * SLOT + (token % seqs) * heads
    attn = jnp.zeros((batch, w_attn.shape[1]), F32)
    for h in range(heads):
        pick = jnp.where(source == at + h, 1.0, 0.0).astype(BF16)
        rows = dot(pick, attended).astype(BF16)
        attn = attn + dot(rows, w_attn[h * HEAD_SIZE : (h + 1) * HEAD_SIZE, :])
    start = pl.multiple_of(seq * HEAD_SIZE, HEAD_SIZE)
    total[:, pl.ds(start, HEAD_SIZE)] = total[:, pl.ds(start, HEAD_SIZE)] + attn

    rows = keep_out.shape[1]
    for i in range(total.shape[1] // HEAD_SIZE):
        block = total[:, i * HEAD_SIZE : (i + 1) * HEAD_SIZE].T.astype(BF16)
        for q in range(0, HEAD_SIZE // rows, 2):
            slot = (i * (HEAD_SIZE // rows) + q) // 2
            even = block[q * rows : (q + 1) * rows, :]
            odd = block[(q + 1) * rows : (q + 2) * rows, :]
            keep_out[slot] = jnp.where(mine, even, odd)
            send_out[slot] = jnp.where(mine, odd, even)


def block(
    hidden_in,
    norm_gain,
    w_ssm_in,
    w_ssm_gate,
    conv_weight,
    conv_bias,
    conv_state,
    w_state_proj,
    w_step,
    step_bias,
    log_decay,
    skip_gain,
    ssm_state,
    w_ssm_out,
    w_query,
    key_projection,
    value_projection,
    w_attn_out,
    w_mlp_gate,
    w_mlp_up,
    w_mlp_down,
    cached_inputs,
    window_lengths,
):
    batch, features = hidden_in.shape
    width = norm_gain.shape[0]
    channels = w_ssm_in.shape[1]
    window = cached_inputs.shape[1]
    states = log_decay.shape[0]
    cosines, sines = (jnp.asarray(t) for t in rotary_tables(window + 8))

    hidden = hidden_in.T
    copies = jnp.broadcast_to(hidden[None], (64, features, batch))
    held = lax.all_to_all(copies, CHIPS, 0, 0, tiled=True)
    other = shifted(held, "seq_2", 1)

    keys, values = window_rows(
        window_lengths, cached_inputs, key_projection, value_projection, cosines, sines
    )

    normed, conv, low = vmem_call(
        inner_kernel,
        (
            ((width, batch), BF16, True),
            ((channels, batch), F32, True),
            ((2, ROWS, 128), F32, True),
        ),
        (
            held, other, norm_gain.reshape(-1, 128), w_ssm_in.T, w_state_proj,
            jnp.transpose(conv_state, (1, 2, 0)), conv_weight, conv_bias[None],
        ),
        fetched=(3,),
        scratch=(pltpu.VMEM((channels, width), BF16), pltpu.SemaphoreType.DMA),
    )
    paired = shifted(low[1], "seq_2", 1)
    half = low[0] + paired
    arrived = from_ring(half, "grp")
    attended = attended_rows(
        window_lengths, normed, w_query, key_projection, value_projection, keys, values,
        cosines, sines,
    )
    gate, act = vmem_call(
        gate_kernel,
        (((channels, batch), F32, True), ((w_mlp_up.shape[1], batch), BF16, True)),
        (normed, w_ssm_gate.T, w_mlp_gate.T, w_mlp_up.T),
    )
    (term,) = vmem_call(down_kernel, (((batch, width), F32, True),), (act, w_mlp_down))
    (packed,) = vmem_call(
        pack_kernel, (((16, ROWS + SLOT, HEAD_SIZE), BF16, True),), (*arrived, attended)
    )
    packed = lax.all_to_all(packed, PLANE, 0, 0, tiled=True)
    near_low, near_rows = vmem_call(
        combine_kernel,
        (((ROWS, HEAD_SIZE), F32, True), ((16 * SLOT, HEAD_SIZE), BF16, True)),
        (packed,),
    )
    far_low = shifted(near_low, "seq_2", 1)
    far_rows = shifted(near_rows, "seq_2", 1)

    piece = ((64, features, batch), BF16, True)
    state_new, keep, send = vmem_call(
        outer_kernel,
        (((states, channels, batch), F32, False), piece, piece),
        (
            near_low, far_low, near_rows, far_rows, w_step.T, log_decay, step_bias[None], skip_gain[None], conv, gate,
            jnp.transpose(ssm_state, (1, 2, 0)), w_ssm_out, term, w_attn_out,
        ),
        scratch=(pltpu.VMEM((batch, width), F32),),
    )
    came = shifted(send, "seq_2", 1)
    summed = (keep.astype(F32) + came.astype(F32)).astype(BF16)
    arrived = lax.all_to_all(summed, CHIPS, 0, 0, tiled=True)
    total = jnp.sum(arrived.astype(F32), axis=0)
    hidden_out = (hidden.astype(F32) + total).astype(BF16).T
    return (hidden_out, jnp.transpose(state_new, (2, 0, 1)))


def solution(mesh):
    torus = Mesh(
        mesh.devices.reshape(mesh.shape["grp"], 4, 4, 2), ("grp", "seq_0", "seq_1", "seq_2")
    )
    placed = (
        P(None, GRP_SEQ),
        P(),
        P(None, GRP_SEQ),
        P(None, GRP_SEQ),
        P(None, GRP_SEQ),
        P(GRP_SEQ),
        P(None, None, GRP_SEQ),
        P(GRP_SEQ, None),
        P(None, GRP_SEQ),
        P(GRP_SEQ),
        P(None, GRP_SEQ),
        P(GRP_SEQ),
        P(None, None, GRP_SEQ),
        P(GRP_SEQ, None),
        P(None, "grp"),
        P(None, "grp"),
        P(None, "grp"),
        P("grp", SEQ),
        P(None, GRP_SEQ),
        P(None, GRP_SEQ),
        P(GRP_SEQ, None),
        P(SEQ, None, None),
        P(),
    )
    return jax.shard_map(
        block,
        mesh=torus,
        in_specs=placed,
        out_specs=(P(None, GRP_SEQ), P(None, None, GRP_SEQ)),
        check_vma=False,
    )
```

```python
import functools

import jax
import jax.numpy as jnp
import numpy as np
from jax import lax
from jax.experimental import pallas as pl
from jax.experimental.pallas import tpu as pltpu
from jax.sharding import Mesh
from jax.sharding import PartitionSpec as P


HEAD_SIZE = 128
GRP_SEQ = ("grp", "seq_0", "seq_1", "seq_2")
SEQ = ("seq_0", "seq_1", "seq_2")
CHIPS = ("grp", "seq_0", "seq_1")
EPSILON = 1e-05
ROPE_BASE = 10000.0
F32 = jnp.float32
BF16 = jnp.bfloat16
NT = (((1,), (1,)), ((), ()))
TN = (((0,), (0,)), ((), ()))
RING = 4
SLOT = 16
PIECE = 4
WEIGHT_PIECES = 4


def rotary_tables(count):
    half = HEAD_SIZE // 2
    frequency = np.float32(ROPE_BASE) ** (
        -(np.arange(half, dtype=np.float32) * np.float32(2.0)) / np.float32(HEAD_SIZE)
    )
    angles = np.arange(count, dtype=np.float32)[:, None] * frequency.astype(np.float32)
    cosine = np.cos(angles.astype(np.float64)).astype(np.float32)
    sine = np.sin(angles.astype(np.float64)).astype(np.float32)
    return (
        np.concatenate([cosine, cosine], axis=1),
        np.concatenate([-sine, sine], axis=1),
    )


def shifted(value, axis, step):
    size = lax.axis_size(axis)
    return lax.ppermute(value, axis, [(i, (i + step) % size) for i in range(size)])


def dot(a, b):
    return jnp.dot(a, b, preferred_element_type=F32)


def own_seq():
    x, y, c = (lax.axis_index(a).astype(jnp.int32) for a in SEQ)
    return (x * RING + y) * 2 + c


def in_hbm(value):
    return pltpu.with_memory_space_constraint(value, pltpu.HBM)


def in_vmem(value):
    return pltpu.with_memory_space_constraint(value, pltpu.VMEM)


def vmem_call(kernel, outs, operands, fetched=(), stored=(), scratch=(), limit=12 << 20):
    vmem = pl.BlockSpec(memory_space=pltpu.VMEM)
    anywhere = pl.BlockSpec(memory_space=pl.ANY)
    return pl.pallas_call(
        kernel,
        out_shape=tuple((pltpu.VMEM if inner else pltpu.HBM)(shape, dtype) for shape, dtype, inner in outs),
        in_specs=[anywhere if k in fetched else vmem for k in range(len(operands))],
        out_specs=tuple(anywhere if k in stored else vmem for k in range(len(outs))),
        scratch_shapes=list(scratch),
        compiler_params=pltpu.CompilerParams(vmem_limit_bytes=limit),
    )(*((in_hbm if k in fetched else in_vmem)(v) for k, v in enumerate(operands)))


def window_kernel(
    cached, w_key, w_value, cosines, sines, key_out, value_out,
    rows, weights, cos, sin, turned, plain, row_sem, first_sem, key_sem, value_sem, table_sem, out_sem,
    *, begin,
):
    seqs, window = key_out.shape[0], key_out.shape[1]
    width, columns = w_key.shape
    pieces = WEIGHT_PIECES
    step = width // pieces

    def piece_copies(p):
        span = pl.ds(p * step, step)
        return (
            pltpu.make_async_copy(
                w_key.at[span], weights.at[span, pl.ds(0, columns)], key_sem.at[p]
            ),
            pltpu.make_async_copy(
                w_value.at[span], weights.at[span, pl.ds(columns, columns)], value_sem.at[p]
            ),
            pltpu.make_async_copy(cached.at[begin, :, span], rows.at[0, :, span], first_sem.at[p]),
        )

    tables = (
        pltpu.make_async_copy(cosines.at[pl.ds(0, window)], cos, table_sem.at[0]),
        pltpu.make_async_copy(sines.at[pl.ds(0, window)], sin, table_sem.at[1]),
    )
    later = [
        pltpu.make_async_copy(cached.at[begin + b], rows.at[b], row_sem.at[b]) for b in range(1, seqs)
    ]
    for p in range(pieces):
        for copy in piece_copies(p):
            copy.start()
    for copy in tables:
        copy.start()
    for copy in later:
        copy.start()

    def finish(b, both):
        for head in range(columns // HEAD_SIZE):
            lanes = slice(head * HEAD_SIZE, (head + 1) * HEAD_SIZE)
            part = both[:, lanes]
            turned[b, :, lanes] = (
                part * cos[...] + pltpu.roll(part, HEAD_SIZE // 2, 1) * sin[...]
            ).astype(BF16)
        plain[b] = both[:, columns:].astype(BF16)

    def out_copies(b):
        return (
            pltpu.make_async_copy(turned.at[b], key_out.at[b], out_sem.at[0, b]),
            pltpu.make_async_copy(plain.at[b], value_out.at[b], out_sem.at[1, b]),
        )

    total = None
    for p in range(pieces):
        for copy in piece_copies(p):
            copy.wait()
        span = slice(p * step, (p + 1) * step)
        part = dot(rows[0, :, span], weights[span, :])
        total = part if total is None else total + part
    for copy in tables:
        copy.wait()
    finish(0, total)
    for copy in out_copies(0):
        copy.start()
    for b in range(1, seqs):
        later[b - 1].wait()
        finish(b, dot(rows[b], weights[...]))
        for copy in out_copies(b):
            copy.start()
    for b in range(seqs):
        for copy in out_copies(b):
            copy.wait()


def window_rows(begin, seqs, cached, w_key, w_value, cosines, sines):
    _, window, width = cached.shape
    columns = w_key.shape[1]
    anywhere = pl.BlockSpec(memory_space=pl.ANY)
    out = pltpu.HBM((seqs, window, columns), BF16)
    dma = pltpu.SemaphoreType.DMA
    return pl.pallas_call(
        functools.partial(window_kernel, begin=begin),
        out_shape=(out, out),
        in_specs=[anywhere] * 5,
        out_specs=(anywhere, anywhere),
        scratch_shapes=[
            pltpu.VMEM((seqs, window, width), BF16),
            pltpu.VMEM((width, 2 * columns), BF16),
            pltpu.VMEM((window, HEAD_SIZE), F32),
            pltpu.VMEM((window, HEAD_SIZE), F32),
            pltpu.VMEM((seqs, window, columns), BF16),
            pltpu.VMEM((seqs, window, columns), BF16),
            dma((seqs,)),
            dma((WEIGHT_PIECES,)),
            dma((WEIGHT_PIECES,)),
            dma((WEIGHT_PIECES,)),
            dma((2,)),
            dma((2, seqs)),
        ],
        compiler_params=pltpu.CompilerParams(vmem_limit_bytes=40 << 20),
    )(*(in_hbm(v) for v in (cached, w_key, w_value, cosines, sines)))


def inner_kernel(
    near, far, gain, w_in_hbm, w_proj, past, taps, bias, normed_hbm, conv_out, low_out,
    normed_out, w_in, w_sem, normed_sem,
):
    fetch = pltpu.make_async_copy(w_in_hbm, w_in, w_sem)
    fetch.start()
    c = lax.axis_index("seq_2").astype(jnp.int32)
    rows, batch = near.shape[1], near.shape[2]
    total = jnp.zeros((rows, batch), F32)
    for slot in range(near.shape[0]):
        a = near[slot].astype(F32)
        b = far[slot].astype(F32)
        total = total + a * a + b * b
    width = gain.shape[0] * gain.shape[1]
    mean = jnp.sum(total, axis=0, keepdims=True) * (1.0 / width)
    scale = lax.rsqrt(mean + EPSILON)
    gains = gain[...].T
    mine = c == 0
    per_gain = gain.shape[1] // rows
    for slot in range(near.shape[0]):
        a = near[slot].astype(F32)
        b = far[slot].astype(F32)
        pair = (jnp.where(mine, a, b), jnp.where(mine, b, a))
        for k in range(2):
            j = 2 * slot + k
            at = (j % per_gain) * rows
            column = gains[at : at + rows, j // per_gain : j // per_gain + 1]
            normed_out[j * rows : (j + 1) * rows, :] = (pair[k] * scale * column).astype(BF16)
    keep = pltpu.make_async_copy(normed_out, normed_hbm, normed_sem)
    keep.start()
    fetch.wait()
    fresh = dot(w_in[...], normed_out[...]).astype(BF16).astype(F32)
    params = jnp.concatenate([taps[...], bias[...], jnp.zeros((3, taps.shape[1]), F32)], axis=0).T
    mixed = params[:, 4:5] + params[:, 3:4] * fresh
    for k in range(past.shape[0]):
        mixed = mixed + past[k].astype(F32) * params[:, k : k + 1]
    conv = jax.nn.silu(mixed)
    conv_out[...] = conv
    low = lax.dot_general(w_proj[...], conv.astype(BF16), TN, preferred_element_type=F32)
    low = jnp.concatenate([low, jnp.zeros((low.shape[0], 128 - batch), F32)], axis=1)
    for k in range(low_out.shape[0]):
        if k < low.shape[0] // PIECE:
            low_out[k] = low[k * PIECE : (k + 1) * PIECE]
        else:
            low_out[k] = jnp.zeros((PIECE, 128), F32)
    keep.wait()


def gate_kernel(normed, w_gate, w_mlp_gate, w_mlp_up, gate_out, act_out):
    gate_out[...] = jax.nn.silu(dot(w_gate[...], normed[...]))
    act = jax.nn.silu(dot(w_mlp_gate[...], normed[...])) * dot(w_mlp_up[...], normed[...])
    act_out[...] = act.astype(BF16)


def down_kernel(act, w_mlp_down, term_out):
    term_out[...] = lax.dot_general(act[...], w_mlp_down[...], TN, preferred_element_type=F32)


def attention_kernel(
    lengths, normed_hbm, w_query, w_key, w_value, first_keys, first_values, later_keys,
    later_values, cosines, sines, out, normed, normed_sem, weights, keys, values, cos_rows, sin_rows, weight_sem, row_sem, table_sem,
):
    seqs, window = keys.shape[0], keys.shape[1]
    columns = keys.shape[2]
    queries = w_query.shape[1]
    kv_heads = columns // HEAD_SIZE
    group = queries // columns
    width, batch = normed.shape
    first = own_seq() * seqs
    pieces = WEIGHT_PIECES
    step = width // pieces

    def piece_copies(p):
        span = pl.ds(p * step, step)
        return (
            pltpu.make_async_copy(
                w_query.at[span], weights.at[span, pl.ds(0, queries)], weight_sem.at[0, p]
            ),
            pltpu.make_async_copy(
                w_key.at[span], weights.at[span, pl.ds(queries, columns)], weight_sem.at[1, p]
            ),
            pltpu.make_async_copy(
                w_value.at[span],
                weights.at[span, pl.ds(queries + columns, columns)],
                weight_sem.at[2, p],
            ),
        )

    row_copies = (
        pltpu.make_async_copy(first_keys, keys.at[pl.ds(0, 1)], row_sem.at[0]),
        pltpu.make_async_copy(first_values, values.at[pl.ds(0, 1)], row_sem.at[1]),
        pltpu.make_async_copy(later_keys, keys.at[pl.ds(1, seqs - 1)], row_sem.at[2]),
        pltpu.make_async_copy(later_values, values.at[pl.ds(1, seqs - 1)], row_sem.at[3]),
    )
    fetch = pltpu.make_async_copy(normed_hbm, normed, normed_sem)
    fetch.start()
    table_copies = []
    for b in range(seqs):
        at = pl.ds(lengths[first + b], 1)
        table_copies.append(
            pltpu.make_async_copy(cosines.at[at], cos_rows.at[pl.ds(b, 1)], table_sem.at[0, b])
        )
        table_copies.append(
            pltpu.make_async_copy(sines.at[at], sin_rows.at[pl.ds(b, 1)], table_sem.at[1, b])
        )
    for p in range(pieces):
        for copy in piece_copies(p):
            copy.start()
    for copy in (*table_copies, *row_copies):
        copy.start()
    fetch.wait()
    row = lax.broadcasted_iota(jnp.int32, (8, batch), 0)
    column = lax.broadcasted_iota(jnp.int32, (8, batch), 1)
    pick = jnp.where((column == first + row) & (row < seqs), 1.0, 0.0).astype(BF16)
    own = lax.dot_general(pick, normed[...], NT, preferred_element_type=F32).astype(BF16)
    projected = None
    for p in range(pieces):
        for copy in piece_copies(p):
            copy.wait()
        span = slice(p * step, (p + 1) * step)
        part = dot(own[:, span], weights[span, :])
        projected = part if projected is None else projected + part
    query = projected[:, 0:queries]
    fresh_key = projected[:, queries : queries + columns]
    fresh_value = projected[:, queries + columns :].astype(BF16).astype(F32)
    for copy in (*table_copies, *row_copies):
        copy.wait()
    scale = HEAD_SIZE ** (-0.5)
    blocks = [(b, g) for b in range(seqs) for g in range(kv_heads)]
    height = len(blocks) * 8
    spare = jnp.zeros((8 - group, HEAD_SIZE), F32)
    stacked, cos, sin, new_key, new_value = [], [], [], [], []
    for b, g in blocks:
        lanes = slice(g * HEAD_SIZE, (g + 1) * HEAD_SIZE)
        for i in range(group):
            head = g * group + i
            stacked.append(query[b : b + 1, head * HEAD_SIZE : (head + 1) * HEAD_SIZE])
        stacked.append(spare)
        cos.append(jnp.broadcast_to(cos_rows[b : b + 1, :], (8, HEAD_SIZE)))
        sin.append(jnp.broadcast_to(sin_rows[b : b + 1, :], (8, HEAD_SIZE)))
        new_key.append(jnp.broadcast_to(fresh_key[b : b + 1, lanes], (8, HEAD_SIZE)))
        new_value.append(jnp.broadcast_to(fresh_value[b : b + 1, lanes], (8, HEAD_SIZE)))
    cos = jnp.concatenate(cos, axis=0)
    sin = jnp.concatenate(sin, axis=0)

    def turned(part):
        return (part * cos + pltpu.roll(part, HEAD_SIZE // 2, 1) * sin).astype(BF16)

    q = turned(jnp.concatenate(stacked, axis=0))
    k_new = turned(jnp.concatenate(new_key, axis=0))
    scores = jnp.concatenate(
        [
            lax.dot_general(
                q[n * 8 : n * 8 + 8],
                keys[b, :, g * HEAD_SIZE : (g + 1) * HEAD_SIZE],
                NT,
                preferred_element_type=F32,
            )
            for n, (b, g) in enumerate(blocks)
        ],
        axis=0,
    ) * scale
    fresh = jnp.sum(q.astype(F32) * k_new.astype(F32), axis=1, keepdims=True) * scale
    slot_ids = lax.broadcasted_iota(jnp.int32, (height, window), 1)
    owner = lax.broadcasted_iota(jnp.int32, (height, window), 0) // (8 * kv_heads)
    length = jnp.where(
        owner == 0,
        lengths[first],
        jnp.where(owner == 1, lengths[first + 1], lengths[first + 2]),
    )
    valid = slot_ids < length
    scores = jnp.where(valid, scores, -1e30)
    top = jnp.maximum(jnp.max(scores, axis=1, keepdims=True), fresh)
    shares = jnp.where(valid, jnp.exp(scores - top), 0.0)
    share_new = jnp.exp(fresh - top)
    denominator = jnp.sum(shares, axis=1, keepdims=True) + share_new
    rounded = shares.astype(BF16)
    summed = jnp.concatenate(
        [
            dot(rounded[n * 8 : n * 8 + 8], values[b, :, g * HEAD_SIZE : (g + 1) * HEAD_SIZE])
            for n, (b, g) in enumerate(blocks)
        ],
        axis=0,
    )
    result = (summed + share_new * jnp.concatenate(new_value, axis=0)) / denominator
    result = result.astype(BF16).astype(F32)
    out[...] = jnp.zeros((SLOT, HEAD_SIZE), F32)
    for n in range(len(blocks)):
        out[n * group : (n + 1) * group, :] = result[n * 8 : n * 8 + group, :]


def attended_rows(lengths, *operands):
    normed, w_query, w_key, _, first_keys, _, later_keys = operands[:7]
    anywhere = pl.BlockSpec(memory_space=pl.ANY)
    dma = pltpu.SemaphoreType.DMA
    seqs = first_keys.shape[0] + later_keys.shape[0]
    held = pltpu.VMEM((seqs, *first_keys.shape[1:]), BF16)
    return pl.pallas_call(
        attention_kernel,
        out_shape=pltpu.VMEM((SLOT, HEAD_SIZE), F32),
        in_specs=[pl.BlockSpec(memory_space=pltpu.SMEM)] + [anywhere] * len(operands),
        out_specs=pl.BlockSpec(memory_space=pltpu.VMEM),
        scratch_shapes=[
            pltpu.VMEM(normed.shape, BF16),
            dma,
            pltpu.VMEM((normed.shape[0], w_query.shape[1] + 2 * w_key.shape[1]), BF16),
            held,
            held,
            pltpu.VMEM((8, HEAD_SIZE), F32),
            pltpu.VMEM((8, HEAD_SIZE), F32),
            dma((3, WEIGHT_PIECES)),
            dma((4,)),
            dma((2, seqs)),
        ],
        compiler_params=pltpu.CompilerParams(vmem_limit_bytes=24 << 20),
    )(lengths, *(in_hbm(v) for v in operands))


def pack_kernel(arrived, attended, out):
    total = arrived[0]
    for k in range(1, arrived.shape[0]):
        total = total + arrived[k]
    block = jnp.concatenate([attended[0 : SLOT - PIECE, :], total], axis=0).astype(BF16)
    for k in range(out.shape[0]):
        out[k] = block


def outer_kernel(
    packed, w_step_hbm, log_decay, step_bias, skip, conv_hbm, gate_hbm, state, w_out_hbm, term,
    w_attn_hbm, state_out, keep_out, send_out, total, w_step, conv, gate, w_out, w_attn, sems,
):
    fetches = [
        pltpu.make_async_copy(source, target, sems.at[k])
        for k, (source, target) in enumerate(
            (
                (w_step_hbm, w_step),
                (conv_hbm, conv),
                (gate_hbm, gate),
                (w_out_hbm, w_out),
                (w_attn_hbm, w_attn),
            )
        )
    ]
    for fetch in fetches:
        fetch.start()
    c = lax.axis_index("seq_2").astype(jnp.int32)
    seq = own_seq()
    batch = conv.shape[1]
    mine = c == 0
    states = state.shape[0]
    pieces = (w_step.shape[1] + 2 * states) // PIECE
    low = jnp.concatenate(
        [packed[k].astype(F32)[SLOT - PIECE :, 0:batch] for k in range(pieces)], axis=0
    )
    rank = w_step.shape[1]
    params = jnp.concatenate(
        [jnp.exp(log_decay[...]), step_bias[...], skip[...], jnp.zeros((6, conv.shape[0]), F32)],
        axis=0,
    ).T
    for fetch in fetches:
        fetch.wait()
    step = jax.nn.softplus(
        dot(w_step[...], low[0:rank].astype(BF16)) + params[:, states : states + 1]
    )
    conv_value = conv[...]
    driven = step * conv_value
    mixed = params[:, states + 1 : states + 2] * conv_value
    for n in range(states):
        decay = jnp.exp(-step * params[:, n : n + 1])
        fresh = decay * state[n] + driven * low[rank + n : rank + n + 1]
        state_out[n] = fresh
        mixed = mixed + fresh * low[rank + states + n : rank + states + n + 1]
    gated = (mixed * gate[...]).astype(BF16)
    total[...] = term[...] + lax.dot_general(gated, w_out[...], TN, preferred_element_type=F32)

    group = lax.axis_index("grp").astype(jnp.int32)
    members = packed.shape[0] // RING
    attended = packed[pl.ds(group * members, members)].reshape(members * SLOT, HEAD_SIZE)
    seqs = batch // members
    heads = w_attn.shape[0] // HEAD_SIZE
    token = lax.broadcasted_iota(jnp.int32, (batch, members * SLOT), 0)
    source = lax.broadcasted_iota(jnp.int32, (batch, members * SLOT), 1)
    at = (token // seqs) * SLOT + (token % seqs) * heads
    attn = jnp.zeros((batch, w_attn.shape[1]), F32)
    for h in range(heads):
        pick = jnp.where(source == at + h, 1.0, 0.0).astype(BF16)
        rows = dot(pick, attended).astype(BF16)
        attn = attn + dot(rows, w_attn[h * HEAD_SIZE : (h + 1) * HEAD_SIZE, :])
    start = pl.multiple_of(seq * HEAD_SIZE, HEAD_SIZE)
    total[:, pl.ds(start, HEAD_SIZE)] = total[:, pl.ds(start, HEAD_SIZE)] + attn

    rows = keep_out.shape[1]
    for i in range(total.shape[1] // HEAD_SIZE):
        block = total[:, i * HEAD_SIZE : (i + 1) * HEAD_SIZE].T.astype(BF16)
        for q in range(0, HEAD_SIZE // rows, 2):
            slot = (i * (HEAD_SIZE // rows) + q) // 2
            even = block[q * rows : (q + 1) * rows, :]
            odd = block[(q + 1) * rows : (q + 2) * rows, :]
            keep_out[slot] = jnp.where(mine, even, odd)
            send_out[slot] = jnp.where(mine, odd, even)


def block(
    hidden_in,
    norm_gain,
    w_ssm_in,
    w_ssm_gate,
    conv_weight,
    conv_bias,
    conv_state,
    w_state_proj,
    w_step,
    step_bias,
    log_decay,
    skip_gain,
    ssm_state,
    w_ssm_out,
    w_query,
    key_projection,
    value_projection,
    w_attn_out,
    w_mlp_gate,
    w_mlp_up,
    w_mlp_down,
    cached_inputs,
    window_lengths,
):
    batch, features = hidden_in.shape
    width = norm_gain.shape[0]
    channels = w_ssm_in.shape[1]
    window = cached_inputs.shape[1]
    states = log_decay.shape[0]
    cosines, sines = (jnp.asarray(t) for t in rotary_tables(window + 8))

    hidden = hidden_in.T
    copies = jnp.broadcast_to(hidden[None], (64, features, batch))
    held = lax.all_to_all(copies, CHIPS, 0, 0, tiled=True)
    other = shifted(held, "seq_2", 1)

    tables = (key_projection, value_projection, cosines, sines)
    first_rows = window_rows(0, 1, cached_inputs, *tables)

    devices = 64 * 2
    normed, conv, low = vmem_call(
        inner_kernel,
        (
            ((width, batch), BF16, False),
            ((channels, batch), F32, False),
            ((devices, PIECE, 128), F32, False),
        ),
        (
            held, other, norm_gain.reshape(-1, 128), w_ssm_in.T, w_state_proj,
            jnp.transpose(conv_state, (1, 2, 0)), conv_weight, conv_bias[None],
        ),
        fetched=(3,),
        stored=(0,),
        scratch=(
            pltpu.VMEM((width, batch), BF16),
            pltpu.VMEM((channels, width), BF16),
            pltpu.SemaphoreType.DMA,
            pltpu.SemaphoreType.DMA,
        ),
    )
    low = lax.all_to_all(low, GRP_SEQ, 0, 0, tiled=True)
    later_rows = window_rows(1, cached_inputs.shape[0] - 1, cached_inputs, *tables)
    gate, act = vmem_call(
        gate_kernel,
        (((channels, batch), F32, False), ((w_mlp_up.shape[1], batch), BF16, False)),
        (normed, w_ssm_gate.T, w_mlp_gate.T, w_mlp_up.T),
    )
    attended = attended_rows(
        window_lengths, normed, w_query, key_projection, value_projection, *first_rows,
        *later_rows, cosines, sines,
    )
    (packed,) = vmem_call(
        pack_kernel, (((devices, SLOT, HEAD_SIZE), BF16, True),), (low, attended)
    )
    packed = lax.all_to_all(packed, GRP_SEQ, 0, 0, tiled=True)
    (term,) = vmem_call(down_kernel, (((batch, width), F32, True),), (act, w_mlp_down))

    piece = ((64, features, batch), BF16, True)
    state_new, keep, send = vmem_call(
        outer_kernel,
        (((states, channels, batch), F32, False), piece, piece),
        (
            packed, w_step.T, log_decay, step_bias[None], skip_gain[None], conv, gate,
            jnp.transpose(ssm_state, (1, 2, 0)), w_ssm_out, term, w_attn_out,
        ),
        fetched=(1, 5, 6, 8, 10),
        scratch=(
            pltpu.VMEM((batch, width), F32),
            pltpu.VMEM((channels, w_step.shape[0]), BF16),
            pltpu.VMEM((channels, batch), F32),
            pltpu.VMEM((channels, batch), F32),
            pltpu.VMEM(w_ssm_out.shape, BF16),
            pltpu.VMEM(w_attn_out.shape, BF16),
            pltpu.SemaphoreType.DMA((5,)),
        ),
    )
    came = shifted(send, "seq_2", 1)
    summed = (keep.astype(F32) + came.astype(F32)).astype(BF16)
    arrived = lax.all_to_all(summed, CHIPS, 0, 0, tiled=True)
    total = jnp.sum(arrived.astype(F32), axis=0)
    hidden_out = (hidden.astype(F32) + total).astype(BF16).T
    return (hidden_out, jnp.transpose(state_new, (2, 0, 1)))


def solution(mesh):
    torus = Mesh(
        mesh.devices.reshape(mesh.shape["grp"], 4, 4, 2), ("grp", "seq_0", "seq_1", "seq_2")
    )
    placed = (
        P(None, GRP_SEQ),
        P(),
        P(None, GRP_SEQ),
        P(None, GRP_SEQ),
        P(None, GRP_SEQ),
        P(GRP_SEQ),
        P(None, None, GRP_SEQ),
        P(GRP_SEQ, None),
        P(None, GRP_SEQ),
        P(GRP_SEQ),
        P(None, GRP_SEQ),
        P(GRP_SEQ),
        P(None, None, GRP_SEQ),
        P(GRP_SEQ, None),
        P(None, "grp"),
        P(None, "grp"),
        P(None, "grp"),
        P("grp", SEQ),
        P(None, GRP_SEQ),
        P(None, GRP_SEQ),
        P(GRP_SEQ, None),
        P(SEQ, None, None),
        P(),
    )
    return jax.shard_map(
        block,
        mesh=torus,
        in_specs=placed,
        out_specs=(P(None, GRP_SEQ), P(None, None, GRP_SEQ)),
        check_vma=False,
    )
```

```python
import functools

import jax
import jax.numpy as jnp
import numpy as np
from jax import lax
from jax.experimental import pallas as pl
from jax.experimental.pallas import tpu as pltpu
from jax.sharding import Mesh
from jax.sharding import PartitionSpec as P


HEAD_SIZE = 128
GRP_SEQ = ("grp", "seq_0", "seq_1", "seq_2")
SEQ = ("seq_0", "seq_1", "seq_2")
CHIPS = ("grp", "seq_0", "seq_1")
PLANE = ("seq_0", "seq_1")
EPSILON = 1e-05
ROPE_BASE = 10000.0
F32 = jnp.float32
BF16 = jnp.bfloat16
NT = (((1,), (1,)), ((), ()))
TN = (((0,), (0,)), ((), ()))
RING = 4
ROWS = 144
SLOT = 16
WEIGHT_PIECES = 4
WINDOW_SIZES = (256, 384, 512)
MAIN = 112
TAIL = 32


def rotary_tables(count):
    half = HEAD_SIZE // 2
    frequency = np.float32(ROPE_BASE) ** (
        -(np.arange(half, dtype=np.float32) * np.float32(2.0)) / np.float32(HEAD_SIZE)
    )
    angles = np.arange(count, dtype=np.float32)[:, None] * frequency.astype(np.float32)
    cosine = np.cos(angles.astype(np.float64)).astype(np.float32)
    sine = np.sin(angles.astype(np.float64)).astype(np.float32)
    return (
        np.concatenate([cosine, cosine], axis=1),
        np.concatenate([-sine, sine], axis=1),
    )


def shifted(value, axis, step):
    size = lax.axis_size(axis)
    return lax.ppermute(value, axis, [(i, (i + step) % size) for i in range(size)])


def from_ring(value, axis):
    arrived = [value]
    for step in (1, 3, 2):
        arrived.append(shifted(value, axis, step))
    return [arrived[0], arrived[1], arrived[3], arrived[2]]


def dot(a, b):
    return jnp.dot(a, b, preferred_element_type=F32)


def here():
    return tuple(lax.axis_index(a).astype(jnp.int32) for a in GRP_SEQ)


def own_seq():
    _, x, y, c = here()
    return (x * RING + y) * 2 + c


def in_hbm(value):
    return pltpu.with_memory_space_constraint(value, pltpu.HBM)


def in_vmem(value):
    return pltpu.with_memory_space_constraint(value, pltpu.VMEM)


def vmem_call(kernel, outs, operands, fetched=(), scratch=(), limit=12 << 20):
    vmem = pl.BlockSpec(memory_space=pltpu.VMEM)
    anywhere = pl.BlockSpec(memory_space=pl.ANY)
    return pl.pallas_call(
        kernel,
        out_shape=tuple(pltpu.VMEM(shape, dtype) if inner else jax.ShapeDtypeStruct(shape, dtype) for shape, dtype, inner in outs),
        in_specs=[anywhere if k in fetched else vmem for k in range(len(operands))],
        out_specs=tuple(vmem for _ in outs),
        scratch_shapes=list(scratch),
        compiler_params=pltpu.CompilerParams(vmem_limit_bytes=limit),
    )(*((in_hbm if k in fetched else in_vmem)(v) for k, v in enumerate(operands)))


def window_kernel(
    lengths_hbm, cached, w_key, w_value, cosines, sines, key_out, value_out,
    rows, weights, cos, sin, turned, plain, lengths,
    row_sem, first_sem, key_sem, value_sem, table_sem, out_sem, length_sem,
):
    seqs, window, width = cached.shape
    columns = w_key.shape[1]
    first = own_seq() * seqs
    pieces = WEIGHT_PIECES
    step = width // pieces

    def piece_copies(p):
        span = pl.ds(p * step, step)
        return (
            pltpu.make_async_copy(
                w_key.at[span], weights.at[span, pl.ds(0, columns)], key_sem.at[p]
            ),
            pltpu.make_async_copy(
                w_value.at[span], weights.at[span, pl.ds(columns, columns)], value_sem.at[p]
            ),
            pltpu.make_async_copy(cached.at[0, :, span], rows.at[0, :, span], first_sem.at[p]),
        )

    tables = (
        pltpu.make_async_copy(cosines.at[pl.ds(0, window)], cos, table_sem.at[0]),
        pltpu.make_async_copy(sines.at[pl.ds(0, window)], sin, table_sem.at[1]),
    )
    later = [
        pltpu.make_async_copy(cached.at[b], rows.at[b], row_sem.at[b]) for b in range(1, seqs)
    ]
    fetch = pltpu.make_async_copy(lengths_hbm, lengths, length_sem)
    fetch.start()
    for p in range(pieces):
        for copy in piece_copies(p):
            copy.start()
    for copy in tables:
        copy.start()
    for copy in later:
        copy.start()
    fetch.wait()

    def finish(b, both):
        live = both.shape[0]
        for head in range(columns // HEAD_SIZE):
            lanes = slice(head * HEAD_SIZE, (head + 1) * HEAD_SIZE)
            part = both[:, lanes]
            turned[b, 0:live, lanes] = (
                part * cos[0:live, :] + pltpu.roll(part, HEAD_SIZE // 2, 1) * sin[0:live, :]
            ).astype(BF16)
        plain[b, 0:live, :] = both[:, columns:].astype(BF16)
        if live < window:
            turned[b, live:, :] = jnp.zeros((window - live, columns), BF16)
            plain[b, live:, :] = jnp.zeros((window - live, columns), BF16)

    def by_length(b, work):
        length = lengths[first + b]
        low = 0
        for size in WINDOW_SIZES:
            if size == WINDOW_SIZES[0]:
                chosen = length <= size
            elif size == WINDOW_SIZES[-1]:
                chosen = length > low
            else:
                chosen = (length > low) & (length <= size)
            pl.when(chosen)(functools.partial(work, size))
            low = size

    def out_copies(b):
        return (
            pltpu.make_async_copy(turned.at[b], key_out.at[b], out_sem.at[0, b]),
            pltpu.make_async_copy(plain.at[b], value_out.at[b], out_sem.at[1, b]),
        )

    for copy in tables:
        copy.wait()

    def first_rows(size):
        total = None
        for p in range(pieces):
            for copy in piece_copies(p):
                copy.wait()
            span = slice(p * step, (p + 1) * step)
            part = dot(rows[0, 0:size, span], weights[span, :])
            total = part if total is None else total + part
        finish(0, total)

    by_length(0, first_rows)
    for copy in out_copies(0):
        copy.start()
    for copy in later:
        copy.wait()

    def later_rows(b, carry):
        by_length(b, lambda size: finish(b, dot(rows[b, 0:size, :], weights[...])))
        return carry

    lax.fori_loop(1, seqs, later_rows, 0)
    for b in range(1, seqs):
        for copy in out_copies(b):
            copy.start()
    for b in range(seqs):
        for copy in out_copies(b):
            copy.wait()


def window_rows(lengths, cached, w_key, w_value, cosines, sines):
    seqs, window, width = cached.shape
    columns = w_key.shape[1]
    anywhere = pl.BlockSpec(memory_space=pl.ANY)
    out = pltpu.HBM((seqs, window, columns), BF16)
    dma = pltpu.SemaphoreType.DMA
    return pl.pallas_call(
        window_kernel,
        out_shape=(out, out),
        in_specs=[anywhere] * 6,
        out_specs=(anywhere, anywhere),
        scratch_shapes=[
            pltpu.VMEM((seqs, window, width), BF16),
            pltpu.VMEM((width, 2 * columns), BF16),
            pltpu.VMEM((window, HEAD_SIZE), F32),
            pltpu.VMEM((window, HEAD_SIZE), F32),
            pltpu.VMEM((seqs, window, columns), BF16),
            pltpu.VMEM((seqs, window, columns), BF16),
            pltpu.SMEM(lengths.shape, jnp.int32),
            dma((seqs,)),
            dma((WEIGHT_PIECES,)),
            dma((WEIGHT_PIECES,)),
            dma((WEIGHT_PIECES,)),
            dma((2,)),
            dma((2, seqs)),
            dma,
        ],
        compiler_params=pltpu.CompilerParams(vmem_limit_bytes=40 << 20),
    )(*(in_hbm(v) for v in (lengths, cached, w_key, w_value, cosines, sines)))


def inner_kernel(
    near, far, gain, w_in_hbm, w_proj, past, taps, bias, normed_out, conv_out, low_out, w_in, w_sem,
):
    fetch = pltpu.make_async_copy(w_in_hbm, w_in, w_sem)
    fetch.start()
    c = lax.axis_index("seq_2").astype(jnp.int32)
    rows, batch = near.shape[1], near.shape[2]
    total = jnp.zeros((rows, batch), F32)
    for slot in range(near.shape[0]):
        a = near[slot].astype(F32)
        b = far[slot].astype(F32)
        total = total + a * a + b * b
    width = gain.shape[0] * gain.shape[1]
    mean = jnp.sum(total, axis=0, keepdims=True) * (1.0 / width)
    scale = lax.rsqrt(mean + EPSILON)
    gains = gain[...].T
    mine = c == 0
    per_gain = gain.shape[1] // rows
    for slot in range(near.shape[0]):
        a = near[slot].astype(F32)
        b = far[slot].astype(F32)
        pair = (jnp.where(mine, a, b), jnp.where(mine, b, a))
        for k in range(2):
            j = 2 * slot + k
            at = (j % per_gain) * rows
            column = gains[at : at + rows, j // per_gain : j // per_gain + 1]
            normed_out[j * rows : (j + 1) * rows, :] = (pair[k] * scale * column).astype(BF16)
    fetch.wait()
    fresh = dot(w_in[...], normed_out[...]).astype(BF16).astype(F32)
    params = jnp.concatenate([taps[...], bias[...], jnp.zeros((3, taps.shape[1]), F32)], axis=0).T
    mixed = params[:, 4:5] + params[:, 3:4] * fresh
    for k in range(past.shape[0]):
        mixed = mixed + past[k].astype(F32) * params[:, k : k + 1]
    conv = jax.nn.silu(mixed)
    conv_out[...] = conv
    low = lax.dot_general(w_proj[...], conv.astype(BF16), TN, preferred_element_type=F32)
    low = jnp.concatenate([low, jnp.zeros((low.shape[0], 128 - batch), F32)], axis=1)
    low_out[c] = low[0:ROWS]
    low_out[1 - c] = low[ROWS:]


def gate_kernel(normed, w_gate, w_mlp_gate, w_mlp_up, gate_out, act_out):
    gate_out[...] = jax.nn.silu(dot(w_gate[...], normed[...]))
    act = jax.nn.silu(dot(w_mlp_gate[...], normed[...])) * dot(w_mlp_up[...], normed[...])
    act_out[...] = act.astype(BF16)


def down_kernel(act, w_mlp_down, term_out):
    term_out[...] = lax.dot_general(act[...], w_mlp_down[...], TN, preferred_element_type=F32)


def attention_kernel(
    lengths_hbm, normed, w_query, w_key, w_value, key_rows, value_rows, cosines, sines, out,
    weights, keys, values, cos_rows, sin_rows, lengths, weight_sem, row_sem, table_sem, length_sem,
):
    fetch = pltpu.make_async_copy(lengths_hbm, lengths, length_sem)
    fetch.start()
    seqs, window = keys.shape[0], keys.shape[1]
    columns = keys.shape[2]
    queries = w_query.shape[1]
    kv_heads = columns // HEAD_SIZE
    group = queries // columns
    width, batch = normed.shape
    first = own_seq() * seqs
    pieces = WEIGHT_PIECES
    step = width // pieces

    def piece_copies(p):
        span = pl.ds(p * step, step)
        return (
            pltpu.make_async_copy(
                w_query.at[span], weights.at[span, pl.ds(0, queries)], weight_sem.at[0, p]
            ),
            pltpu.make_async_copy(
                w_key.at[span], weights.at[span, pl.ds(queries, columns)], weight_sem.at[1, p]
            ),
            pltpu.make_async_copy(
                w_value.at[span],
                weights.at[span, pl.ds(queries + columns, columns)],
                weight_sem.at[2, p],
            ),
        )

    row_copies = (
        pltpu.make_async_copy(key_rows, keys, row_sem.at[0]),
        pltpu.make_async_copy(value_rows, values, row_sem.at[1]),
    )
    for p in range(pieces):
        for copy in piece_copies(p):
            copy.start()
    for copy in row_copies:
        copy.start()
    fetch.wait()
    table_copies = []
    for b in range(seqs):
        at = pl.ds(lengths[first + b], 1)
        table_copies.append(
            pltpu.make_async_copy(cosines.at[at], cos_rows.at[pl.ds(b, 1)], table_sem.at[0, b])
        )
        table_copies.append(
            pltpu.make_async_copy(sines.at[at], sin_rows.at[pl.ds(b, 1)], table_sem.at[1, b])
        )
    for copy in table_copies:
        copy.start()
    row = lax.broadcasted_iota(jnp.int32, (8, batch), 0)
    column = lax.broadcasted_iota(jnp.int32, (8, batch), 1)
    pick = jnp.where((column == first + row) & (row < seqs), 1.0, 0.0).astype(BF16)
    own = lax.dot_general(pick, normed[...], NT, preferred_element_type=F32).astype(BF16)
    projected = None
    for p in range(pieces):
        for copy in piece_copies(p):
            copy.wait()
        span = slice(p * step, (p + 1) * step)
        part = dot(own[:, span], weights[span, :])
        projected = part if projected is None else projected + part
    query = projected[:, 0:queries]
    fresh_key = projected[:, queries : queries + columns]
    fresh_value = projected[:, queries + columns :].astype(BF16).astype(F32)
    for copy in (*table_copies, *row_copies):
        copy.wait()
    scale = HEAD_SIZE ** (-0.5)
    blocks = [(b, g) for b in range(seqs) for g in range(kv_heads)]
    height = len(blocks) * 8
    spare = jnp.zeros((8 - group, HEAD_SIZE), F32)
    stacked, cos, sin, new_key, new_value = [], [], [], [], []
    for b, g in blocks:
        lanes = slice(g * HEAD_SIZE, (g + 1) * HEAD_SIZE)
        for i in range(group):
            head = g * group + i
            stacked.append(query[b : b + 1, head * HEAD_SIZE : (head + 1) * HEAD_SIZE])
        stacked.append(spare)
        cos.append(jnp.broadcast_to(cos_rows[b : b + 1, :], (8, HEAD_SIZE)))
        sin.append(jnp.broadcast_to(sin_rows[b : b + 1, :], (8, HEAD_SIZE)))
        new_key.append(jnp.broadcast_to(fresh_key[b : b + 1, lanes], (8, HEAD_SIZE)))
        new_value.append(jnp.broadcast_to(fresh_value[b : b + 1, lanes], (8, HEAD_SIZE)))
    cos = jnp.concatenate(cos, axis=0)
    sin = jnp.concatenate(sin, axis=0)

    def turned(part):
        return (part * cos + pltpu.roll(part, HEAD_SIZE // 2, 1) * sin).astype(BF16)

    q = turned(jnp.concatenate(stacked, axis=0))
    k_new = turned(jnp.concatenate(new_key, axis=0))
    scores = jnp.concatenate(
        [
            lax.dot_general(
                q[n * 8 : n * 8 + 8],
                keys[b, :, g * HEAD_SIZE : (g + 1) * HEAD_SIZE],
                NT,
                preferred_element_type=F32,
            )
            for n, (b, g) in enumerate(blocks)
        ],
        axis=0,
    ) * scale
    fresh = jnp.sum(q.astype(F32) * k_new.astype(F32), axis=1, keepdims=True) * scale
    slot_ids = lax.broadcasted_iota(jnp.int32, (height, window), 1)
    owner = lax.broadcasted_iota(jnp.int32, (height, window), 0) // (8 * kv_heads)
    length = jnp.where(
        owner == 0,
        lengths[first],
        jnp.where(owner == 1, lengths[first + 1], lengths[first + 2]),
    )
    valid = slot_ids < length
    scores = jnp.where(valid, scores, -1e30)
    top = jnp.maximum(jnp.max(scores, axis=1, keepdims=True), fresh)
    shares = jnp.where(valid, jnp.exp(scores - top), 0.0)
    share_new = jnp.exp(fresh - top)
    denominator = jnp.sum(shares, axis=1, keepdims=True) + share_new
    rounded = shares.astype(BF16)
    summed = jnp.concatenate(
        [
            dot(rounded[n * 8 : n * 8 + 8], values[b, :, g * HEAD_SIZE : (g + 1) * HEAD_SIZE])
            for n, (b, g) in enumerate(blocks)
        ],
        axis=0,
    )
    result = (summed + share_new * jnp.concatenate(new_value, axis=0)) / denominator
    result = result.astype(BF16).astype(F32)
    out[...] = jnp.zeros((SLOT, HEAD_SIZE), F32)
    for n in range(len(blocks)):
        out[n * group : (n + 1) * group, :] = result[n * 8 : n * 8 + group, :]


def attended_rows(lengths, normed, w_query, w_key, w_value, keys, values, cosines, sines):
    anywhere = pl.BlockSpec(memory_space=pl.ANY)
    vmem = pl.BlockSpec(memory_space=pltpu.VMEM)
    dma = pltpu.SemaphoreType.DMA
    width = normed.shape[0]
    return pl.pallas_call(
        attention_kernel,
        out_shape=pltpu.VMEM((SLOT, HEAD_SIZE), F32),
        in_specs=[anywhere, vmem] + [anywhere] * 7,
        out_specs=vmem,
        scratch_shapes=[
            pltpu.VMEM((width, w_query.shape[1] + 2 * w_key.shape[1]), BF16),
            pltpu.VMEM(keys.shape, BF16),
            pltpu.VMEM(values.shape, BF16),
            pltpu.VMEM((8, HEAD_SIZE), F32),
            pltpu.VMEM((8, HEAD_SIZE), F32),
            pltpu.SMEM(lengths.shape, jnp.int32),
            dma((3, WEIGHT_PIECES)),
            dma((2,)),
            dma((2, keys.shape[0])),
            dma,
        ],
        compiler_params=pltpu.CompilerParams(vmem_limit_bytes=20 << 20),
    )(
        in_hbm(lengths),
        in_vmem(normed),
        *(in_hbm(v) for v in (w_query, w_key, w_value, keys, values, cosines, sines)),
    )


def pack_kernel(s0, s1, s2, s3, attended, out):
    low = (s0[...] + s1[...]) + (s2[...] + s3[...])
    tail = low[MAIN:, :]
    moved = [pltpu.roll(tail, 96 - TAIL * p, 1) for p in range(3)]
    moved.append(jnp.zeros((MAIN - 3 * TAIL, HEAD_SIZE), F32))
    lane = lax.broadcasted_iota(jnp.int32, (MAIN, HEAD_SIZE), 1)
    low = jnp.where(lane < 96, low[0:MAIN, :], jnp.concatenate(moved, axis=0)).astype(BF16)
    rows = attended[...].astype(BF16)
    for k in range(out.shape[0]):
        out[k, 0:MAIN, :] = low
        out[k, MAIN:, :] = rows


def combine_kernel(arrived, low_out, rows_out):
    total = arrived[0, 0:MAIN, :].astype(F32)
    rows_out[0:SLOT, :] = arrived[0, MAIN:, :]
    for k in range(1, arrived.shape[0]):
        total = total + arrived[k, 0:MAIN, :].astype(F32)
        rows_out[k * SLOT : (k + 1) * SLOT, :] = arrived[k, MAIN:, :]
    low_out[0:MAIN, :] = total
    lane = lax.broadcasted_iota(jnp.int32, (TAIL, HEAD_SIZE), 1)
    tail = jnp.zeros((TAIL, HEAD_SIZE), F32)
    for p in range(3):
        back = pltpu.roll(total[TAIL * p : TAIL * (p + 1), :], HEAD_SIZE - 96 + TAIL * p, 1)
        tail = jnp.where(lane // TAIL == p, back, tail)
    low_out[MAIN:, :] = tail


def outer_kernel(
    near, far, near_rows, far_rows, w_step, log_decay, step_bias, skip, conv, gate, state, w_out, term, w_attn,
    state_out, keep_out, send_out, total,
):
    c = lax.axis_index("seq_2").astype(jnp.int32)
    seq = own_seq()
    batch = conv.shape[1]
    mine = c == 0
    near_low = near[:, 0:batch]
    far_low = far[:, 0:batch]
    low = jnp.concatenate(
        [jnp.where(mine, near_low, far_low), jnp.where(mine, far_low, near_low)], axis=0
    )
    rank = w_step.shape[1]
    states = state.shape[0]
    params = jnp.concatenate(
        [jnp.exp(log_decay[...]), step_bias[...], skip[...], jnp.zeros((6, conv.shape[0]), F32)],
        axis=0,
    ).T
    step = jax.nn.softplus(
        dot(w_step[...], low[0:rank].astype(BF16)) + params[:, states : states + 1]
    )
    conv_value = conv[...]
    driven = step * conv_value
    mixed = params[:, states + 1 : states + 2] * conv_value
    for n in range(states):
        decay = jnp.exp(-step * params[:, n : n + 1])
        fresh = decay * state[n] + driven * low[rank + n : rank + n + 1]
        state_out[n] = fresh
        mixed = mixed + fresh * low[rank + states + n : rank + states + n + 1]
    gated = (mixed * gate[...]).astype(BF16)
    total[...] = term[...] + lax.dot_general(gated, w_out[...], TN, preferred_element_type=F32)

    slots = near_rows.shape[0]
    attended = jnp.concatenate([near_rows[...], far_rows[...]], axis=0)
    seqs = 3
    heads = w_attn.shape[0] // HEAD_SIZE
    token = lax.broadcasted_iota(jnp.int32, (batch, 2 * slots), 0)
    source = lax.broadcasted_iota(jnp.int32, (batch, 2 * slots), 1)
    owner = token // seqs
    other_core = jnp.where(owner % 2 == c, 0, 1)
    at = other_core * slots + (owner // 2) * SLOT + (token % seqs) * heads
    attn = jnp.zeros((batch, w_attn.shape[1]), F32)
    for h in range(heads):
        pick = jnp.where(source == at + h, 1.0, 0.0).astype(BF16)
        rows = dot(pick, attended).astype(BF16)
        attn = attn + dot(rows, w_attn[h * HEAD_SIZE : (h + 1) * HEAD_SIZE, :])
    start = pl.multiple_of(seq * HEAD_SIZE, HEAD_SIZE)
    total[:, pl.ds(start, HEAD_SIZE)] = total[:, pl.ds(start, HEAD_SIZE)] + attn

    rows = keep_out.shape[1]
    for i in range(total.shape[1] // HEAD_SIZE):
        block = total[:, i * HEAD_SIZE : (i + 1) * HEAD_SIZE].T.astype(BF16)
        for q in range(0, HEAD_SIZE // rows, 2):
            slot = (i * (HEAD_SIZE // rows) + q) // 2
            even = block[q * rows : (q + 1) * rows, :]
            odd = block[(q + 1) * rows : (q + 2) * rows, :]
            keep_out[slot] = jnp.where(mine, even, odd)
            send_out[slot] = jnp.where(mine, odd, even)


def block(
    hidden_in,
    norm_gain,
    w_ssm_in,
    w_ssm_gate,
    conv_weight,
    conv_bias,
    conv_state,
    w_state_proj,
    w_step,
    step_bias,
    log_decay,
    skip_gain,
    ssm_state,
    w_ssm_out,
    w_query,
    key_projection,
    value_projection,
    w_attn_out,
    w_mlp_gate,
    w_mlp_up,
    w_mlp_down,
    cached_inputs,
    window_lengths,
):
    batch, features = hidden_in.shape
    width = norm_gain.shape[0]
    channels = w_ssm_in.shape[1]
    window = cached_inputs.shape[1]
    states = log_decay.shape[0]
    cosines, sines = (jnp.asarray(t) for t in rotary_tables(window + 8))

    hidden = hidden_in.T
    copies = jnp.broadcast_to(hidden[None], (64, features, batch))
    held = lax.all_to_all(copies, CHIPS, 0, 0, tiled=True)
    other = shifted(held, "seq_2", 1)

    keys, values = window_rows(
        window_lengths, cached_inputs, key_projection, value_projection, cosines, sines
    )

    normed, conv, low = vmem_call(
        inner_kernel,
        (
            ((width, batch), BF16, True),
            ((channels, batch), F32, True),
            ((2, ROWS, 128), F32, True),
        ),
        (
            held, other, norm_gain.reshape(-1, 128), w_ssm_in.T, w_state_proj,
            jnp.transpose(conv_state, (1, 2, 0)), conv_weight, conv_bias[None],
        ),
        fetched=(3,),
        scratch=(pltpu.VMEM((channels, width), BF16), pltpu.SemaphoreType.DMA),
    )
    paired = shifted(low[1], "seq_2", 1)
    half = low[0] + paired
    arrived = from_ring(half, "grp")
    attended = attended_rows(
        window_lengths, normed, w_query, key_projection, value_projection, keys, values,
        cosines, sines,
    )
    gate, act = vmem_call(
        gate_kernel,
        (((channels, batch), F32, True), ((w_mlp_up.shape[1], batch), BF16, True)),
        (normed, w_ssm_gate.T, w_mlp_gate.T, w_mlp_up.T),
    )
    (term,) = vmem_call(down_kernel, (((batch, width), F32, True),), (act, w_mlp_down))
    (packed,) = vmem_call(
        pack_kernel, (((16, MAIN + SLOT, HEAD_SIZE), BF16, True),), (*arrived, attended)
    )
    packed = lax.all_to_all(packed, PLANE, 0, 0, tiled=True)
    near_low, near_rows = vmem_call(
        combine_kernel,
        (((ROWS, HEAD_SIZE), F32, True), ((16 * SLOT, HEAD_SIZE), BF16, True)),
        (packed,),
    )
    far_low = shifted(near_low, "seq_2", 1)
    far_rows = shifted(near_rows, "seq_2", 1)

    piece = ((64, features, batch), BF16, True)
    state_new, keep, send = vmem_call(
        outer_kernel,
        (((states, channels, batch), F32, False), piece, piece),
        (
            near_low, far_low, near_rows, far_rows, w_step.T, log_decay, step_bias[None], skip_gain[None], conv, gate,
            jnp.transpose(ssm_state, (1, 2, 0)), w_ssm_out, term, w_attn_out,
        ),
        scratch=(pltpu.VMEM((batch, width), F32),),
    )
    came = shifted(send, "seq_2", 1)
    summed = (keep.astype(F32) + came.astype(F32)).astype(BF16)
    arrived = lax.all_to_all(summed, CHIPS, 0, 0, tiled=True)
    total = jnp.sum(arrived.astype(F32), axis=0)
    hidden_out = (hidden.astype(F32) + total).astype(BF16).T
    return (hidden_out, jnp.transpose(state_new, (2, 0, 1)))


def solution(mesh):
    torus = Mesh(
        mesh.devices.reshape(mesh.shape["grp"], 4, 4, 2), ("grp", "seq_0", "seq_1", "seq_2")
    )
    placed = (
        P(None, GRP_SEQ),
        P(),
        P(None, GRP_SEQ),
        P(None, GRP_SEQ),
        P(None, GRP_SEQ),
        P(GRP_SEQ),
        P(None, None, GRP_SEQ),
        P(GRP_SEQ, None),
        P(None, GRP_SEQ),
        P(GRP_SEQ),
        P(None, GRP_SEQ),
        P(GRP_SEQ),
        P(None, None, GRP_SEQ),
        P(GRP_SEQ, None),
        P(None, "grp"),
        P(None, "grp"),
        P(None, "grp"),
        P("grp", SEQ),
        P(None, GRP_SEQ),
        P(None, GRP_SEQ),
        P(GRP_SEQ, None),
        P(SEQ, None, None),
        P(),
    )
    return jax.shard_map(
        block,
        mesh=torus,
        in_specs=placed,
        out_specs=(P(None, GRP_SEQ), P(None, None, GRP_SEQ)),
        check_vma=False,
    )
```

```python
import functools

import jax
import jax.numpy as jnp
import numpy as np
from jax import lax
from jax.experimental import pallas as pl
from jax.experimental.pallas import tpu as pltpu
from jax.sharding import Mesh
from jax.sharding import PartitionSpec as P


HEAD_SIZE = 128
GRP_SEQ = ("grp", "seq_0", "seq_1", "seq_2")
SEQ = ("seq_0", "seq_1", "seq_2")
CHIPS = ("grp", "seq_0", "seq_1")
PLANE = ("seq_0", "seq_1")
EPSILON = 1e-05
ROPE_BASE = 10000.0
F32 = jnp.float32
BF16 = jnp.bfloat16
NT = (((1,), (1,)), ((), ()))
TN = (((0,), (0,)), ((), ()))
RING = 4
ROWS = 144
SLOT = 16
WEIGHT_PIECES = 4
WINDOW_SIZES = (256, 384, 512)
MAIN = 112
COST = 8_000_000_000
TAIL = 32


def rotary_tables(count):
    half = HEAD_SIZE // 2
    frequency = np.float32(ROPE_BASE) ** (
        -(np.arange(half, dtype=np.float32) * np.float32(2.0)) / np.float32(HEAD_SIZE)
    )
    angles = np.arange(count, dtype=np.float32)[:, None] * frequency.astype(np.float32)
    cosine = np.cos(angles.astype(np.float64)).astype(np.float32)
    sine = np.sin(angles.astype(np.float64)).astype(np.float32)
    return (
        np.concatenate([cosine, cosine], axis=1),
        np.concatenate([-sine, sine], axis=1),
    )


def shifted(value, axis, step):
    size = lax.axis_size(axis)
    return lax.ppermute(value, axis, [(i, (i + step) % size) for i in range(size)])


def from_ring(value, axis):
    arrived = [value]
    for step in (1, 3, 2):
        arrived.append(shifted(value, axis, step))
    return [arrived[0], arrived[1], arrived[3], arrived[2]]


def dot(a, b):
    return jnp.dot(a, b, preferred_element_type=F32)


def here():
    return tuple(lax.axis_index(a).astype(jnp.int32) for a in GRP_SEQ)


def own_seq():
    _, x, y, c = here()
    return (x * RING + y) * 2 + c


def in_hbm(value):
    return pltpu.with_memory_space_constraint(value, pltpu.HBM)


def in_vmem(value):
    return pltpu.with_memory_space_constraint(value, pltpu.VMEM)


def vmem_call(kernel, outs, operands, fetched=(), scratch=(), limit=12 << 20, cost=None):
    vmem = pl.BlockSpec(memory_space=pltpu.VMEM)
    anywhere = pl.BlockSpec(memory_space=pl.ANY)
    return pl.pallas_call(
        kernel,
        out_shape=tuple(pltpu.VMEM(shape, dtype) if inner else jax.ShapeDtypeStruct(shape, dtype) for shape, dtype, inner in outs),
        in_specs=[anywhere if k in fetched else vmem for k in range(len(operands))],
        out_specs=tuple(vmem for _ in outs),
        scratch_shapes=list(scratch),
        compiler_params=pltpu.CompilerParams(vmem_limit_bytes=limit),
        cost_estimate=cost,
    )(*((in_hbm if k in fetched else in_vmem)(v) for k, v in enumerate(operands)))


def window_kernel(
    lengths_hbm, cached, w_key, w_value, cosines, sines, key_out, value_out,
    rows, weights, cos, sin, turned, plain, lengths,
    row_sem, first_sem, key_sem, value_sem, table_sem, out_sem, length_sem,
):
    seqs, window, width = cached.shape
    columns = w_key.shape[1]
    first = own_seq() * seqs
    pieces = WEIGHT_PIECES
    step = width // pieces

    def piece_copies(p):
        span = pl.ds(p * step, step)
        return (
            pltpu.make_async_copy(
                w_key.at[span], weights.at[span, pl.ds(0, columns)], key_sem.at[p]
            ),
            pltpu.make_async_copy(
                w_value.at[span], weights.at[span, pl.ds(columns, columns)], value_sem.at[p]
            ),
            pltpu.make_async_copy(cached.at[0, :, span], rows.at[0, :, span], first_sem.at[p]),
        )

    tables = (
        pltpu.make_async_copy(cosines.at[pl.ds(0, window)], cos, table_sem.at[0]),
        pltpu.make_async_copy(sines.at[pl.ds(0, window)], sin, table_sem.at[1]),
    )
    later = [
        pltpu.make_async_copy(cached.at[b], rows.at[b], row_sem.at[b]) for b in range(1, seqs)
    ]
    fetch = pltpu.make_async_copy(lengths_hbm, lengths, length_sem)
    fetch.start()
    for p in range(pieces):
        for copy in piece_copies(p):
            copy.start()
    for copy in tables:
        copy.start()
    for copy in later:
        copy.start()
    fetch.wait()

    def finish(b, both):
        live = both.shape[0]
        for head in range(columns // HEAD_SIZE):
            lanes = slice(head * HEAD_SIZE, (head + 1) * HEAD_SIZE)
            part = both[:, lanes]
            turned[b, 0:live, lanes] = (
                part * cos[0:live, :] + pltpu.roll(part, HEAD_SIZE // 2, 1) * sin[0:live, :]
            ).astype(BF16)
        plain[b, 0:live, :] = both[:, columns:].astype(BF16)
        if live < window:
            turned[b, live:, :] = jnp.zeros((window - live, columns), BF16)
            plain[b, live:, :] = jnp.zeros((window - live, columns), BF16)

    def by_length(b, work):
        length = lengths[first + b]
        low = 0
        for size in WINDOW_SIZES:
            if size == WINDOW_SIZES[0]:
                chosen = length <= size
            elif size == WINDOW_SIZES[-1]:
                chosen = length > low
            else:
                chosen = (length > low) & (length <= size)
            pl.when(chosen)(functools.partial(work, size))
            low = size

    def out_copies(b):
        return (
            pltpu.make_async_copy(turned.at[b], key_out.at[b], out_sem.at[0, b]),
            pltpu.make_async_copy(plain.at[b], value_out.at[b], out_sem.at[1, b]),
        )

    def first_rows(size):
        total = None
        for p in range(pieces):
            for copy in piece_copies(p):
                copy.wait()
            span = slice(p * step, (p + 1) * step)
            part = dot(rows[0, 0:size, span], weights[span, :])
            total = part if total is None else total + part
        for copy in tables:
            copy.wait()
        finish(0, total)

    by_length(0, first_rows)
    for copy in out_copies(0):
        copy.start()
    for copy in later:
        copy.wait()

    def later_rows(b, carry):
        by_length(b, lambda size: finish(b, dot(rows[b, 0:size, :], weights[...])))
        for copy in out_copies(b):
            copy.start()
        return carry

    lax.fori_loop(1, seqs, later_rows, 0)
    for b in range(seqs):
        for copy in out_copies(b):
            copy.wait()


def window_rows(lengths, cached, w_key, w_value, cosines, sines):
    seqs, window, width = cached.shape
    columns = w_key.shape[1]
    anywhere = pl.BlockSpec(memory_space=pl.ANY)
    out = pltpu.HBM((seqs, window, columns), BF16)
    dma = pltpu.SemaphoreType.DMA
    return pl.pallas_call(
        window_kernel,
        out_shape=(out, out),
        in_specs=[anywhere] * 6,
        out_specs=(anywhere, anywhere),
        scratch_shapes=[
            pltpu.VMEM((seqs, window, width), BF16),
            pltpu.VMEM((width, 2 * columns), BF16),
            pltpu.VMEM((window, HEAD_SIZE), F32),
            pltpu.VMEM((window, HEAD_SIZE), F32),
            pltpu.VMEM((seqs, window, columns), BF16),
            pltpu.VMEM((seqs, window, columns), BF16),
            pltpu.SMEM(lengths.shape, jnp.int32),
            dma((seqs,)),
            dma((WEIGHT_PIECES,)),
            dma((WEIGHT_PIECES,)),
            dma((WEIGHT_PIECES,)),
            dma((2,)),
            dma((2, seqs)),
            dma,
        ],
        compiler_params=pltpu.CompilerParams(vmem_limit_bytes=40 << 20),
    )(*(in_hbm(v) for v in (lengths, cached, w_key, w_value, cosines, sines)))


def inner_kernel(
    near, far, gain, w_in_hbm, w_proj, past, taps, bias, normed_out, conv_out, low_out, w_in, w_sem,
):
    fetch = pltpu.make_async_copy(w_in_hbm, w_in, w_sem)
    fetch.start()
    c = lax.axis_index("seq_2").astype(jnp.int32)
    rows, batch = near.shape[1], near.shape[2]
    total = jnp.zeros((rows, batch), F32)
    for slot in range(near.shape[0]):
        a = near[slot].astype(F32)
        b = far[slot].astype(F32)
        total = total + a * a + b * b
    width = gain.shape[0] * gain.shape[1]
    mean = jnp.sum(total, axis=0, keepdims=True) * (1.0 / width)
    scale = lax.rsqrt(mean + EPSILON)
    gains = gain[...].T
    mine = c == 0
    per_gain = gain.shape[1] // rows
    for slot in range(near.shape[0]):
        a = near[slot].astype(F32)
        b = far[slot].astype(F32)
        pair = (jnp.where(mine, a, b), jnp.where(mine, b, a))
        for k in range(2):
            j = 2 * slot + k
            at = (j % per_gain) * rows
            column = gains[at : at + rows, j // per_gain : j // per_gain + 1]
            normed_out[j * rows : (j + 1) * rows, :] = (pair[k] * scale * column).astype(BF16)
    fetch.wait()
    fresh = dot(w_in[...], normed_out[...]).astype(BF16).astype(F32)
    params = jnp.concatenate([taps[...], bias[...], jnp.zeros((3, taps.shape[1]), F32)], axis=0).T
    mixed = params[:, 4:5] + params[:, 3:4] * fresh
    for k in range(past.shape[0]):
        mixed = mixed + past[k].astype(F32) * params[:, k : k + 1]
    conv = jax.nn.silu(mixed)
    conv_out[...] = conv
    low = lax.dot_general(w_proj[...], conv.astype(BF16), TN, preferred_element_type=F32)
    low = jnp.concatenate([low, jnp.zeros((low.shape[0], 128 - batch), F32)], axis=1)
    low_out[c] = low[0:ROWS]
    low_out[1 - c] = low[ROWS:]


def gate_kernel(normed, w_gate, w_mlp_gate, w_mlp_up, gate_out, act_out):
    gate_out[...] = jax.nn.silu(dot(w_gate[...], normed[...]))
    act = jax.nn.silu(dot(w_mlp_gate[...], normed[...])) * dot(w_mlp_up[...], normed[...])
    act_out[...] = act.astype(BF16)


def down_kernel(act, w_mlp_down, term_out):
    term_out[...] = lax.dot_general(act[...], w_mlp_down[...], TN, preferred_element_type=F32)


def attention_kernel(
    lengths_hbm, normed, w_query, w_key, w_value, key_rows, value_rows, cosines, sines, out,
    keys, values, cos_rows, sin_rows, lengths, row_sem, table_sem, length_sem,
):
    fetch = pltpu.make_async_copy(lengths_hbm, lengths, length_sem)
    fetch.start()
    seqs, window = keys.shape[0], keys.shape[1]
    columns = keys.shape[2]
    queries = w_query.shape[1]
    kv_heads = columns // HEAD_SIZE
    group = queries // columns
    batch = normed.shape[1]
    first = own_seq() * seqs
    row_copies = (
        pltpu.make_async_copy(key_rows, keys, row_sem.at[0]),
        pltpu.make_async_copy(value_rows, values, row_sem.at[1]),
    )
    for copy in row_copies:
        copy.start()
    fetch.wait()
    table_copies = []
    for b in range(seqs):
        at = pl.ds(lengths[first + b], 1)
        table_copies.append(
            pltpu.make_async_copy(cosines.at[at], cos_rows.at[pl.ds(b, 1)], table_sem.at[0, b])
        )
        table_copies.append(
            pltpu.make_async_copy(sines.at[at], sin_rows.at[pl.ds(b, 1)], table_sem.at[1, b])
        )
    for copy in table_copies:
        copy.start()
    row = lax.broadcasted_iota(jnp.int32, (8, batch), 0)
    column = lax.broadcasted_iota(jnp.int32, (8, batch), 1)
    pick = jnp.where((column == first + row) & (row < seqs), 1.0, 0.0).astype(BF16)
    own = lax.dot_general(pick, normed[...], NT, preferred_element_type=F32).astype(BF16)
    query = dot(own, w_query[...])
    fresh_key = dot(own, w_key[...])
    fresh_value = dot(own, w_value[...]).astype(BF16).astype(F32)
    for copy in (*table_copies, *row_copies):
        copy.wait()
    scale = HEAD_SIZE ** (-0.5)
    blocks = [(b, g) for b in range(seqs) for g in range(kv_heads)]
    height = len(blocks) * 8
    spare = jnp.zeros((8 - group, HEAD_SIZE), F32)
    stacked, cos, sin, new_key, new_value = [], [], [], [], []
    for b, g in blocks:
        lanes = slice(g * HEAD_SIZE, (g + 1) * HEAD_SIZE)
        for i in range(group):
            head = g * group + i
            stacked.append(query[b : b + 1, head * HEAD_SIZE : (head + 1) * HEAD_SIZE])
        stacked.append(spare)
        cos.append(jnp.broadcast_to(cos_rows[b : b + 1, :], (8, HEAD_SIZE)))
        sin.append(jnp.broadcast_to(sin_rows[b : b + 1, :], (8, HEAD_SIZE)))
        new_key.append(jnp.broadcast_to(fresh_key[b : b + 1, lanes], (8, HEAD_SIZE)))
        new_value.append(jnp.broadcast_to(fresh_value[b : b + 1, lanes], (8, HEAD_SIZE)))
    cos = jnp.concatenate(cos, axis=0)
    sin = jnp.concatenate(sin, axis=0)

    def turned(part):
        return (part * cos + pltpu.roll(part, HEAD_SIZE // 2, 1) * sin).astype(BF16)

    q = turned(jnp.concatenate(stacked, axis=0))
    k_new = turned(jnp.concatenate(new_key, axis=0))
    scores = jnp.concatenate(
        [
            lax.dot_general(
                q[n * 8 : n * 8 + 8],
                keys[b, :, g * HEAD_SIZE : (g + 1) * HEAD_SIZE],
                NT,
                preferred_element_type=F32,
            )
            for n, (b, g) in enumerate(blocks)
        ],
        axis=0,
    ) * scale
    fresh = jnp.sum(q.astype(F32) * k_new.astype(F32), axis=1, keepdims=True) * scale
    slot_ids = lax.broadcasted_iota(jnp.int32, (height, window), 1)
    owner = lax.broadcasted_iota(jnp.int32, (height, window), 0) // (8 * kv_heads)
    length = jnp.where(
        owner == 0,
        lengths[first],
        jnp.where(owner == 1, lengths[first + 1], lengths[first + 2]),
    )
    valid = slot_ids < length
    scores = jnp.where(valid, scores, -1e30)
    top = jnp.maximum(jnp.max(scores, axis=1, keepdims=True), fresh)
    shares = jnp.where(valid, jnp.exp(scores - top), 0.0)
    share_new = jnp.exp(fresh - top)
    denominator = jnp.sum(shares, axis=1, keepdims=True) + share_new
    rounded = shares.astype(BF16)
    summed = jnp.concatenate(
        [
            dot(rounded[n * 8 : n * 8 + 8], values[b, :, g * HEAD_SIZE : (g + 1) * HEAD_SIZE])
            for n, (b, g) in enumerate(blocks)
        ],
        axis=0,
    )
    result = (summed + share_new * jnp.concatenate(new_value, axis=0)) / denominator
    result = result.astype(BF16).astype(F32)
    out[...] = jnp.zeros((SLOT, HEAD_SIZE), F32)
    for n in range(len(blocks)):
        out[n * group : (n + 1) * group, :] = result[n * 8 : n * 8 + group, :]


def attended_rows(lengths, normed, w_query, w_key, w_value, keys, values, cosines, sines):
    anywhere = pl.BlockSpec(memory_space=pl.ANY)
    vmem = pl.BlockSpec(memory_space=pltpu.VMEM)
    dma = pltpu.SemaphoreType.DMA
    return pl.pallas_call(
        attention_kernel,
        out_shape=pltpu.VMEM((SLOT, HEAD_SIZE), F32),
        in_specs=[anywhere] + [vmem] * 4 + [anywhere] * 4,
        out_specs=vmem,
        scratch_shapes=[
            pltpu.VMEM(keys.shape, BF16),
            pltpu.VMEM(values.shape, BF16),
            pltpu.VMEM((8, HEAD_SIZE), F32),
            pltpu.VMEM((8, HEAD_SIZE), F32),
            pltpu.SMEM(lengths.shape, jnp.int32),
            dma((2,)),
            dma((2, keys.shape[0])),
            dma,
        ],
        compiler_params=pltpu.CompilerParams(vmem_limit_bytes=12 << 20),
    )(
        in_hbm(lengths),
        *(in_vmem(v) for v in (normed, w_query, w_key, w_value)),
        *(in_hbm(v) for v in (keys, values, cosines, sines)),
    )


def pack_kernel(s0, s1, s2, s3, attended, out):
    low = (s0[...] + s1[...]) + (s2[...] + s3[...])
    tail = low[MAIN:, :]
    moved = [pltpu.roll(tail, 96 - TAIL * p, 1) for p in range(3)]
    moved.append(jnp.zeros((MAIN - 3 * TAIL, HEAD_SIZE), F32))
    lane = lax.broadcasted_iota(jnp.int32, (MAIN, HEAD_SIZE), 1)
    low = jnp.where(lane < 96, low[0:MAIN, :], jnp.concatenate(moved, axis=0)).astype(BF16)
    rows = attended[...].astype(BF16)
    for k in range(out.shape[0]):
        out[k, 0:MAIN, :] = low
        out[k, MAIN:, :] = rows


def combine_kernel(arrived, low_out, rows_out):
    total = arrived[0, 0:MAIN, :].astype(F32)
    rows_out[0:SLOT, :] = arrived[0, MAIN:, :]
    for k in range(1, arrived.shape[0]):
        total = total + arrived[k, 0:MAIN, :].astype(F32)
        rows_out[k * SLOT : (k + 1) * SLOT, :] = arrived[k, MAIN:, :]
    low_out[0:MAIN, :] = total
    lane = lax.broadcasted_iota(jnp.int32, (TAIL, HEAD_SIZE), 1)
    tail = jnp.zeros((TAIL, HEAD_SIZE), F32)
    for p in range(3):
        back = pltpu.roll(total[TAIL * p : TAIL * (p + 1), :], HEAD_SIZE - 96 + TAIL * p, 1)
        tail = jnp.where(lane // TAIL == p, back, tail)
    low_out[MAIN:, :] = tail


def outer_kernel(
    near, far, near_rows, far_rows, w_step, log_decay, step_bias, skip, conv, gate, state, w_out, term, w_attn,
    state_out, keep_out, send_out, total,
):
    c = lax.axis_index("seq_2").astype(jnp.int32)
    seq = own_seq()
    batch = conv.shape[1]
    mine = c == 0
    near_low = near[:, 0:batch]
    far_low = far[:, 0:batch]
    low = jnp.concatenate(
        [jnp.where(mine, near_low, far_low), jnp.where(mine, far_low, near_low)], axis=0
    )
    rank = w_step.shape[1]
    states = state.shape[0]
    params = jnp.concatenate(
        [jnp.exp(log_decay[...]), step_bias[...], skip[...], jnp.zeros((6, conv.shape[0]), F32)],
        axis=0,
    ).T
    step = jax.nn.softplus(
        dot(w_step[...], low[0:rank].astype(BF16)) + params[:, states : states + 1]
    )
    conv_value = conv[...]
    driven = step * conv_value
    mixed = params[:, states + 1 : states + 2] * conv_value
    for n in range(states):
        decay = jnp.exp(-step * params[:, n : n + 1])
        fresh = decay * state[n] + driven * low[rank + n : rank + n + 1]
        state_out[n] = fresh
        mixed = mixed + fresh * low[rank + states + n : rank + states + n + 1]
    gated = (mixed * gate[...]).astype(BF16)
    total[...] = term[...] + lax.dot_general(gated, w_out[...], TN, preferred_element_type=F32)

    slots = near_rows.shape[0]
    attended = jnp.concatenate([near_rows[...], far_rows[...]], axis=0)
    seqs = 3
    heads = w_attn.shape[0] // HEAD_SIZE
    token = lax.broadcasted_iota(jnp.int32, (batch, 2 * slots), 0)
    source = lax.broadcasted_iota(jnp.int32, (batch, 2 * slots), 1)
    owner = token // seqs
    other_core = jnp.where(owner % 2 == c, 0, 1)
    at = other_core * slots + (owner // 2) * SLOT + (token % seqs) * heads
    attn = jnp.zeros((batch, w_attn.shape[1]), F32)
    for h in range(heads):
        pick = jnp.where(source == at + h, 1.0, 0.0).astype(BF16)
        rows = dot(pick, attended).astype(BF16)
        attn = attn + dot(rows, w_attn[h * HEAD_SIZE : (h + 1) * HEAD_SIZE, :])
    start = pl.multiple_of(seq * HEAD_SIZE, HEAD_SIZE)
    total[:, pl.ds(start, HEAD_SIZE)] = total[:, pl.ds(start, HEAD_SIZE)] + attn

    rows = keep_out.shape[1]
    for i in range(total.shape[1] // HEAD_SIZE):
        block = total[:, i * HEAD_SIZE : (i + 1) * HEAD_SIZE].T.astype(BF16)
        for q in range(0, HEAD_SIZE // rows, 2):
            slot = (i * (HEAD_SIZE // rows) + q) // 2
            even = block[q * rows : (q + 1) * rows, :]
            odd = block[(q + 1) * rows : (q + 2) * rows, :]
            keep_out[slot] = jnp.where(mine, even, odd)
            send_out[slot] = jnp.where(mine, odd, even)


def block(
    hidden_in,
    norm_gain,
    w_ssm_in,
    w_ssm_gate,
    conv_weight,
    conv_bias,
    conv_state,
    w_state_proj,
    w_step,
    step_bias,
    log_decay,
    skip_gain,
    ssm_state,
    w_ssm_out,
    w_query,
    key_projection,
    value_projection,
    w_attn_out,
    w_mlp_gate,
    w_mlp_up,
    w_mlp_down,
    cached_inputs,
    window_lengths,
):
    batch, features = hidden_in.shape
    width = norm_gain.shape[0]
    channels = w_ssm_in.shape[1]
    window = cached_inputs.shape[1]
    states = log_decay.shape[0]
    cosines, sines = (jnp.asarray(t) for t in rotary_tables(window + 8))

    hidden = hidden_in.T
    copies = jnp.broadcast_to(hidden[None], (64, features, batch))
    held = lax.all_to_all(copies, CHIPS, 0, 0, tiled=True)
    other = shifted(held, "seq_2", 1)

    keys, values = window_rows(
        window_lengths, cached_inputs, key_projection, value_projection, cosines, sines
    )

    normed, conv, low = vmem_call(
        inner_kernel,
        (
            ((width, batch), BF16, True),
            ((channels, batch), F32, True),
            ((2, ROWS, 128), F32, True),
        ),
        (
            held, other, norm_gain.reshape(-1, 128), w_ssm_in.T, w_state_proj,
            jnp.transpose(conv_state, (1, 2, 0)), conv_weight, conv_bias[None],
        ),
        fetched=(3,),
        scratch=(pltpu.VMEM((channels, width), BF16), pltpu.SemaphoreType.DMA),
        cost=pl.CostEstimate(flops=COST, bytes_accessed=0, transcendentals=0),
    )
    paired = shifted(low[1], "seq_2", 1)
    half = low[0] + paired
    arrived = from_ring(half, "grp")
    attended = attended_rows(
        window_lengths, normed, w_query, key_projection, value_projection, keys, values,
        cosines, sines,
    )
    gate, act = vmem_call(
        gate_kernel,
        (((channels, batch), F32, True), ((w_mlp_up.shape[1], batch), BF16, True)),
        (normed, w_ssm_gate.T, w_mlp_gate.T, w_mlp_up.T),
    )
    (term,) = vmem_call(down_kernel, (((batch, width), F32, True),), (act, w_mlp_down))
    (packed,) = vmem_call(
        pack_kernel, (((16, MAIN + SLOT, HEAD_SIZE), BF16, True),), (*arrived, attended)
    )
    packed = lax.all_to_all(packed, PLANE, 0, 0, tiled=True)
    near_low, near_rows = vmem_call(
        combine_kernel,
        (((ROWS, HEAD_SIZE), F32, True), ((16 * SLOT, HEAD_SIZE), BF16, True)),
        (packed,),
    )
    far_low = shifted(near_low, "seq_2", 1)
    far_rows = shifted(near_rows, "seq_2", 1)

    piece = ((64, features, batch), BF16, True)
    state_new, keep, send = vmem_call(
        outer_kernel,
        (((states, channels, batch), F32, False), piece, piece),
        (
            near_low, far_low, near_rows, far_rows, w_step.T, log_decay, step_bias[None], skip_gain[None], conv, gate,
            jnp.transpose(ssm_state, (1, 2, 0)), w_ssm_out, term, w_attn_out,
        ),
        scratch=(pltpu.VMEM((batch, width), F32),),
    )
    came = shifted(send, "seq_2", 1)
    summed = (keep.astype(F32) + came.astype(F32)).astype(BF16)
    arrived = lax.all_to_all(summed, CHIPS, 0, 0, tiled=True)
    total = jnp.sum(arrived.astype(F32), axis=0)
    hidden_out = (hidden.astype(F32) + total).astype(BF16).T
    return (hidden_out, jnp.transpose(state_new, (2, 0, 1)))


def solution(mesh):
    torus = Mesh(
        mesh.devices.reshape(mesh.shape["grp"], 4, 4, 2), ("grp", "seq_0", "seq_1", "seq_2")
    )
    placed = (
        P(None, GRP_SEQ),
        P(),
        P(None, GRP_SEQ),
        P(None, GRP_SEQ),
        P(None, GRP_SEQ),
        P(GRP_SEQ),
        P(None, None, GRP_SEQ),
        P(GRP_SEQ, None),
        P(None, GRP_SEQ),
        P(GRP_SEQ),
        P(None, GRP_SEQ),
        P(GRP_SEQ),
        P(None, None, GRP_SEQ),
        P(GRP_SEQ, None),
        P(None, "grp"),
        P(None, "grp"),
        P(None, "grp"),
        P("grp", SEQ),
        P(None, GRP_SEQ),
        P(None, GRP_SEQ),
        P(GRP_SEQ, None),
        P(SEQ, None, None),
        P(),
    )
    return jax.shard_map(
        block,
        mesh=torus,
        in_specs=placed,
        out_specs=(P(None, GRP_SEQ), P(None, None, GRP_SEQ)),
        check_vma=False,
    )
```

```python
import functools

import jax
import jax.numpy as jnp
import numpy as np
from jax import lax
from jax.experimental import pallas as pl
from jax.experimental.pallas import tpu as pltpu
from jax.sharding import Mesh
from jax.sharding import PartitionSpec as P


HEAD_SIZE = 128
GRP_SEQ = ("grp", "seq_0", "seq_1", "seq_2")
SEQ = ("seq_0", "seq_1", "seq_2")
CHIPS = ("grp", "seq_0", "seq_1")
PLANE = ("seq_0", "seq_1")
EPSILON = 1e-05
ROPE_BASE = 10000.0
F32 = jnp.float32
BF16 = jnp.bfloat16
NT = (((1,), (1,)), ((), ()))
TN = (((0,), (0,)), ((), ()))
RING = 4
ROWS = 144
SLOT = 16
WEIGHT_PIECES = 4
WINDOW_SIZES = (256, 384, 512)
MAIN = 112
COST = 8_000_000_000
TAIL = 32


def rotary_tables(count):
    half = HEAD_SIZE // 2
    frequency = np.float32(ROPE_BASE) ** (
        -(np.arange(half, dtype=np.float32) * np.float32(2.0)) / np.float32(HEAD_SIZE)
    )
    angles = np.arange(count, dtype=np.float32)[:, None] * frequency.astype(np.float32)
    cosine = np.cos(angles.astype(np.float64)).astype(np.float32)
    sine = np.sin(angles.astype(np.float64)).astype(np.float32)
    return (
        np.concatenate([cosine, cosine], axis=1),
        np.concatenate([-sine, sine], axis=1),
    )


def shifted(value, axis, step):
    size = lax.axis_size(axis)
    return lax.ppermute(value, axis, [(i, (i + step) % size) for i in range(size)])


def from_ring(value, axis):
    arrived = [value]
    for step in (1, 3, 2):
        arrived.append(shifted(value, axis, step))
    return [arrived[0], arrived[1], arrived[3], arrived[2]]


def dot(a, b):
    return jnp.dot(a, b, preferred_element_type=F32)


def here():
    return tuple(lax.axis_index(a).astype(jnp.int32) for a in GRP_SEQ)


def own_seq():
    _, x, y, c = here()
    return (x * RING + y) * 2 + c


def in_hbm(value):
    return pltpu.with_memory_space_constraint(value, pltpu.HBM)


def in_vmem(value):
    return pltpu.with_memory_space_constraint(value, pltpu.VMEM)


def vmem_call(kernel, outs, operands, fetched=(), stored=(), scratch=(), limit=12 << 20, cost=None):
    vmem = pl.BlockSpec(memory_space=pltpu.VMEM)
    anywhere = pl.BlockSpec(memory_space=pl.ANY)
    return pl.pallas_call(
        kernel,
        out_shape=tuple(pltpu.VMEM(shape, dtype) if inner else jax.ShapeDtypeStruct(shape, dtype) for shape, dtype, inner in outs),
        in_specs=[anywhere if k in fetched else vmem for k in range(len(operands))],
        out_specs=tuple(anywhere if k in stored else vmem for k in range(len(outs))),
        scratch_shapes=list(scratch),
        compiler_params=pltpu.CompilerParams(vmem_limit_bytes=limit),
        cost_estimate=cost,
    )(*((in_hbm if k in fetched else in_vmem)(v) for k, v in enumerate(operands)))


def window_kernel(
    lengths_hbm, cached, w_key, w_value, cosines, sines, key_out, value_out, last_key, last_value,
    rows, weights, cos, sin, early_key, early_value, lengths,
    row_sem, first_sem, key_sem, value_sem, table_sem, out_sem, length_sem,
):
    seqs, window, width = cached.shape
    columns = w_key.shape[1]
    first = own_seq() * seqs
    pieces = WEIGHT_PIECES
    step = width // pieces

    def piece_copies(p):
        span = pl.ds(p * step, step)
        return (
            pltpu.make_async_copy(
                w_key.at[span], weights.at[span, pl.ds(0, columns)], key_sem.at[p]
            ),
            pltpu.make_async_copy(
                w_value.at[span], weights.at[span, pl.ds(columns, columns)], value_sem.at[p]
            ),
            pltpu.make_async_copy(cached.at[0, :, span], rows.at[0, :, span], first_sem.at[p]),
        )

    tables = (
        pltpu.make_async_copy(cosines.at[pl.ds(0, window)], cos, table_sem.at[0]),
        pltpu.make_async_copy(sines.at[pl.ds(0, window)], sin, table_sem.at[1]),
    )
    later = [
        pltpu.make_async_copy(cached.at[b], rows.at[b], row_sem.at[b]) for b in range(1, seqs)
    ]
    fetch = pltpu.make_async_copy(lengths_hbm, lengths, length_sem)
    fetch.start()
    for p in range(pieces):
        for copy in piece_copies(p):
            copy.start()
    for copy in tables:
        copy.start()
    for copy in later:
        copy.start()
    fetch.wait()

    def finish(b, both):
        live = both.shape[0]
        at = b if b < seqs - 1 else 0
        turned, plain = (early_key, early_value) if b < seqs - 1 else (last_key, last_value)
        for head in range(columns // HEAD_SIZE):
            lanes = slice(head * HEAD_SIZE, (head + 1) * HEAD_SIZE)
            part = both[:, lanes]
            turned[at, 0:live, lanes] = (
                part * cos[0:live, :] + pltpu.roll(part, HEAD_SIZE // 2, 1) * sin[0:live, :]
            ).astype(BF16)
        plain[at, 0:live, :] = both[:, columns:].astype(BF16)
        if live < window:
            turned[at, live:, :] = jnp.zeros((window - live, columns), BF16)
            plain[at, live:, :] = jnp.zeros((window - live, columns), BF16)

    def by_length(b, work):
        length = lengths[first + b]
        low = 0
        for size in WINDOW_SIZES:
            if size == WINDOW_SIZES[0]:
                chosen = length <= size
            elif size == WINDOW_SIZES[-1]:
                chosen = length > low
            else:
                chosen = (length > low) & (length <= size)
            pl.when(chosen)(functools.partial(work, size))
            low = size

    def out_copies(b):
        return (
            pltpu.make_async_copy(early_key.at[b], key_out.at[b], out_sem.at[0, b]),
            pltpu.make_async_copy(early_value.at[b], value_out.at[b], out_sem.at[1, b]),
        )

    def first_rows(size):
        total = None
        for p in range(pieces):
            for copy in piece_copies(p):
                copy.wait()
            span = slice(p * step, (p + 1) * step)
            part = dot(rows[0, 0:size, span], weights[span, :])
            total = part if total is None else total + part
        for copy in tables:
            copy.wait()
        finish(0, total)

    by_length(0, first_rows)
    for copy in out_copies(0):
        copy.start()
    for b in range(1, seqs):
        later[b - 1].wait()
        by_length(b, lambda size, b=b: finish(b, dot(rows[b, 0:size, :], weights[...])))
        if b < seqs - 1:
            for copy in out_copies(b):
                copy.start()
    for b in range(seqs - 1):
        for copy in out_copies(b):
            copy.wait()


def window_rows(lengths, cached, w_key, w_value, cosines, sines):
    seqs, window, width = cached.shape
    columns = w_key.shape[1]
    anywhere = pl.BlockSpec(memory_space=pl.ANY)
    early = (seqs - 1, window, columns)
    last = (1, window, columns)
    vmem = pl.BlockSpec(memory_space=pltpu.VMEM)
    dma = pltpu.SemaphoreType.DMA
    return pl.pallas_call(
        window_kernel,
        out_shape=(
            pltpu.HBM(early, BF16), pltpu.HBM(early, BF16), pltpu.VMEM(last, BF16), pltpu.VMEM(last, BF16)
        ),
        in_specs=[anywhere] * 6,
        out_specs=(anywhere, anywhere, vmem, vmem),
        scratch_shapes=[
            pltpu.VMEM((seqs, window, width), BF16),
            pltpu.VMEM((width, 2 * columns), BF16),
            pltpu.VMEM((window, HEAD_SIZE), F32),
            pltpu.VMEM((window, HEAD_SIZE), F32),
            pltpu.VMEM(early, BF16),
            pltpu.VMEM(early, BF16),
            pltpu.SMEM(lengths.shape, jnp.int32),
            dma((seqs,)),
            dma((WEIGHT_PIECES,)),
            dma((WEIGHT_PIECES,)),
            dma((WEIGHT_PIECES,)),
            dma((2,)),
            dma((2, seqs - 1)),
            dma,
        ],
        compiler_params=pltpu.CompilerParams(vmem_limit_bytes=40 << 20),
    )(*(in_hbm(v) for v in (lengths, cached, w_key, w_value, cosines, sines)))


def inner_kernel(
    near, far, gain, w_in_hbm, w_proj, past, taps, bias, normed_out, conv_out, low_out, w_in, w_sem,
):
    fetch = pltpu.make_async_copy(w_in_hbm, w_in, w_sem)
    fetch.start()
    c = lax.axis_index("seq_2").astype(jnp.int32)
    rows, batch = near.shape[1], near.shape[2]
    total = jnp.zeros((rows, batch), F32)
    for slot in range(near.shape[0]):
        a = near[slot].astype(F32)
        b = far[slot].astype(F32)
        total = total + a * a + b * b
    width = gain.shape[0] * gain.shape[1]
    mean = jnp.sum(total, axis=0, keepdims=True) * (1.0 / width)
    scale = lax.rsqrt(mean + EPSILON)
    gains = gain[...].T
    mine = c == 0
    per_gain = gain.shape[1] // rows
    for slot in range(near.shape[0]):
        a = near[slot].astype(F32)
        b = far[slot].astype(F32)
        pair = (jnp.where(mine, a, b), jnp.where(mine, b, a))
        for k in range(2):
            j = 2 * slot + k
            at = (j % per_gain) * rows
            column = gains[at : at + rows, j // per_gain : j // per_gain + 1]
            normed_out[j * rows : (j + 1) * rows, :] = (pair[k] * scale * column).astype(BF16)
    fetch.wait()
    fresh = dot(w_in[...], normed_out[...]).astype(BF16).astype(F32)
    params = jnp.concatenate([taps[...], bias[...], jnp.zeros((3, taps.shape[1]), F32)], axis=0).T
    mixed = params[:, 4:5] + params[:, 3:4] * fresh
    for k in range(past.shape[0]):
        mixed = mixed + past[k].astype(F32) * params[:, k : k + 1]
    conv = jax.nn.silu(mixed)
    conv_out[...] = conv
    low = lax.dot_general(w_proj[...], conv.astype(BF16), TN, preferred_element_type=F32)
    low = jnp.concatenate([low, jnp.zeros((low.shape[0], 128 - batch), F32)], axis=1)
    low_out[c] = low[0:ROWS]
    low_out[1 - c] = low[ROWS:]


def gate_kernel(normed, w_gate, w_mlp_gate, w_mlp_up, gate_out, act_out):
    gate_out[...] = jax.nn.silu(dot(w_gate[...], normed[...]))
    act = jax.nn.silu(dot(w_mlp_gate[...], normed[...])) * dot(w_mlp_up[...], normed[...])
    act_out[...] = act.astype(BF16)


def down_kernel(act, w_mlp_down, term_out):
    term_out[...] = lax.dot_general(act[...], w_mlp_down[...], TN, preferred_element_type=F32)


def attention_kernel(
    lengths_hbm, normed, w_query, w_key, w_value, last_key, last_value, key_rows, value_rows,
    cosines, sines, out,
    keys, values, cos_rows, sin_rows, lengths, row_sem, table_sem, length_sem,
):
    fetch = pltpu.make_async_copy(lengths_hbm, lengths, length_sem)
    fetch.start()
    seqs, window = keys.shape[0] + 1, keys.shape[1]
    columns = keys.shape[2]
    queries = w_query.shape[1]
    kv_heads = columns // HEAD_SIZE
    group = queries // columns
    batch = normed.shape[1]
    first = own_seq() * seqs
    row_copies = (
        pltpu.make_async_copy(key_rows, keys, row_sem.at[0]),
        pltpu.make_async_copy(value_rows, values, row_sem.at[1]),
    )
    for copy in row_copies:
        copy.start()
    fetch.wait()
    table_copies = []
    for b in range(seqs):
        at = pl.ds(lengths[first + b], 1)
        table_copies.append(
            pltpu.make_async_copy(cosines.at[at], cos_rows.at[pl.ds(b, 1)], table_sem.at[0, b])
        )
        table_copies.append(
            pltpu.make_async_copy(sines.at[at], sin_rows.at[pl.ds(b, 1)], table_sem.at[1, b])
        )
    for copy in table_copies:
        copy.start()
    row = lax.broadcasted_iota(jnp.int32, (8, batch), 0)
    column = lax.broadcasted_iota(jnp.int32, (8, batch), 1)
    pick = jnp.where((column == first + row) & (row < seqs), 1.0, 0.0).astype(BF16)
    own = lax.dot_general(pick, normed[...], NT, preferred_element_type=F32).astype(BF16)
    query = dot(own, w_query[...])
    fresh_key = dot(own, w_key[...])
    fresh_value = dot(own, w_value[...]).astype(BF16).astype(F32)
    for copy in (*table_copies, *row_copies):
        copy.wait()
    scale = HEAD_SIZE ** (-0.5)
    blocks = [(b, g) for b in range(seqs) for g in range(kv_heads)]
    height = len(blocks) * 8
    spare = jnp.zeros((8 - group, HEAD_SIZE), F32)
    stacked, cos, sin, new_key, new_value = [], [], [], [], []
    for b, g in blocks:
        lanes = slice(g * HEAD_SIZE, (g + 1) * HEAD_SIZE)
        for i in range(group):
            head = g * group + i
            stacked.append(query[b : b + 1, head * HEAD_SIZE : (head + 1) * HEAD_SIZE])
        stacked.append(spare)
        cos.append(jnp.broadcast_to(cos_rows[b : b + 1, :], (8, HEAD_SIZE)))
        sin.append(jnp.broadcast_to(sin_rows[b : b + 1, :], (8, HEAD_SIZE)))
        new_key.append(jnp.broadcast_to(fresh_key[b : b + 1, lanes], (8, HEAD_SIZE)))
        new_value.append(jnp.broadcast_to(fresh_value[b : b + 1, lanes], (8, HEAD_SIZE)))
    cos = jnp.concatenate(cos, axis=0)
    sin = jnp.concatenate(sin, axis=0)

    def turned(part):
        return (part * cos + pltpu.roll(part, HEAD_SIZE // 2, 1) * sin).astype(BF16)

    q = turned(jnp.concatenate(stacked, axis=0))
    k_new = turned(jnp.concatenate(new_key, axis=0))

    def row_of(early, last, b):
        return early.at[b] if b < seqs - 1 else last.at[0]

    scores = jnp.concatenate(
        [
            lax.dot_general(
                q[n * 8 : n * 8 + 8],
                row_of(keys, last_key, b)[:, g * HEAD_SIZE : (g + 1) * HEAD_SIZE],
                NT,
                preferred_element_type=F32,
            )
            for n, (b, g) in enumerate(blocks)
        ],
        axis=0,
    ) * scale
    fresh = jnp.sum(q.astype(F32) * k_new.astype(F32), axis=1, keepdims=True) * scale
    slot_ids = lax.broadcasted_iota(jnp.int32, (height, window), 1)
    owner = lax.broadcasted_iota(jnp.int32, (height, window), 0) // (8 * kv_heads)
    length = jnp.where(
        owner == 0,
        lengths[first],
        jnp.where(owner == 1, lengths[first + 1], lengths[first + 2]),
    )
    valid = slot_ids < length
    scores = jnp.where(valid, scores, -1e30)
    top = jnp.maximum(jnp.max(scores, axis=1, keepdims=True), fresh)
    shares = jnp.where(valid, jnp.exp(scores - top), 0.0)
    share_new = jnp.exp(fresh - top)
    denominator = jnp.sum(shares, axis=1, keepdims=True) + share_new
    rounded = shares.astype(BF16)
    summed = jnp.concatenate(
        [
            dot(rounded[n * 8 : n * 8 + 8], row_of(values, last_value, b)[:, g * HEAD_SIZE : (g + 1) * HEAD_SIZE])
            for n, (b, g) in enumerate(blocks)
        ],
        axis=0,
    )
    result = (summed + share_new * jnp.concatenate(new_value, axis=0)) / denominator
    result = result.astype(BF16).astype(F32)
    out[...] = jnp.zeros((SLOT, HEAD_SIZE), F32)
    for n in range(len(blocks)):
        out[n * group : (n + 1) * group, :] = result[n * 8 : n * 8 + group, :]


def attended_rows(
    lengths, normed, w_query, w_key, w_value, keys, values, last_key, last_value, cosines, sines
):
    anywhere = pl.BlockSpec(memory_space=pl.ANY)
    vmem = pl.BlockSpec(memory_space=pltpu.VMEM)
    dma = pltpu.SemaphoreType.DMA
    return pl.pallas_call(
        attention_kernel,
        out_shape=pltpu.VMEM((SLOT, HEAD_SIZE), F32),
        in_specs=[anywhere] + [vmem] * 6 + [anywhere] * 4,
        out_specs=vmem,
        scratch_shapes=[
            pltpu.VMEM(keys.shape, BF16),
            pltpu.VMEM(values.shape, BF16),
            pltpu.VMEM((8, HEAD_SIZE), F32),
            pltpu.VMEM((8, HEAD_SIZE), F32),
            pltpu.SMEM(lengths.shape, jnp.int32),
            dma((2,)),
            dma((2, keys.shape[0] + 1)),
            dma,
        ],
        compiler_params=pltpu.CompilerParams(vmem_limit_bytes=12 << 20),
    )(
        in_hbm(lengths),
        *(in_vmem(v) for v in (normed, w_query, w_key, w_value, last_key, last_value)),
        *(in_hbm(v) for v in (keys, values, cosines, sines)),
    )


def pack_kernel(s0, s1, s2, s3, attended, out):
    low = (s0[...] + s1[...]) + (s2[...] + s3[...])
    tail = low[MAIN:, :]
    moved = [pltpu.roll(tail, 96 - TAIL * p, 1) for p in range(3)]
    moved.append(jnp.zeros((MAIN - 3 * TAIL, HEAD_SIZE), F32))
    lane = lax.broadcasted_iota(jnp.int32, (MAIN, HEAD_SIZE), 1)
    low = jnp.where(lane < 96, low[0:MAIN, :], jnp.concatenate(moved, axis=0)).astype(BF16)
    rows = attended[...].astype(BF16)
    for k in range(out.shape[0]):
        out[k, 0:MAIN, :] = low
        out[k, MAIN:, :] = rows


def combine_kernel(arrived, low_out, rows_out):
    total = arrived[0, 0:MAIN, :].astype(F32)
    rows_out[0:SLOT, :] = arrived[0, MAIN:, :]
    for k in range(1, arrived.shape[0]):
        total = total + arrived[k, 0:MAIN, :].astype(F32)
        rows_out[k * SLOT : (k + 1) * SLOT, :] = arrived[k, MAIN:, :]
    low_out[0:MAIN, :] = total
    lane = lax.broadcasted_iota(jnp.int32, (TAIL, HEAD_SIZE), 1)
    tail = jnp.zeros((TAIL, HEAD_SIZE), F32)
    for p in range(3):
        back = pltpu.roll(total[TAIL * p : TAIL * (p + 1), :], HEAD_SIZE - 96 + TAIL * p, 1)
        tail = jnp.where(lane // TAIL == p, back, tail)
    low_out[MAIN:, :] = tail


def outer_kernel(
    near, far, near_rows, far_rows, w_step, log_decay, step_bias, skip, conv, gate, state, w_out, term, w_attn,
    state_hbm, keep_out, send_out, total, state_out, state_sem,
):
    c = lax.axis_index("seq_2").astype(jnp.int32)
    seq = own_seq()
    batch = conv.shape[1]
    mine = c == 0
    near_low = near[:, 0:batch]
    far_low = far[:, 0:batch]
    low = jnp.concatenate(
        [jnp.where(mine, near_low, far_low), jnp.where(mine, far_low, near_low)], axis=0
    )
    rank = w_step.shape[1]
    states = state.shape[0]
    params = jnp.concatenate(
        [jnp.exp(log_decay[...]), step_bias[...], skip[...], jnp.zeros((6, conv.shape[0]), F32)],
        axis=0,
    ).T
    step = jax.nn.softplus(
        dot(w_step[...], low[0:rank].astype(BF16)) + params[:, states : states + 1]
    )
    conv_value = conv[...]
    driven = step * conv_value
    mixed = params[:, states + 1 : states + 2] * conv_value
    for n in range(states):
        decay = jnp.exp(-step * params[:, n : n + 1])
        fresh = decay * state[n] + driven * low[rank + n : rank + n + 1]
        state_out[n] = fresh
        mixed = mixed + fresh * low[rank + states + n : rank + states + n + 1]
    store = pltpu.make_async_copy(state_out, state_hbm, state_sem)
    store.start()
    gated = (mixed * gate[...]).astype(BF16)
    total[...] = term[...] + lax.dot_general(gated, w_out[...], TN, preferred_element_type=F32)

    slots = near_rows.shape[0]
    attended = jnp.concatenate([near_rows[...], far_rows[...]], axis=0)
    seqs = 3
    heads = w_attn.shape[0] // HEAD_SIZE
    token = lax.broadcasted_iota(jnp.int32, (batch, 2 * slots), 0)
    source = lax.broadcasted_iota(jnp.int32, (batch, 2 * slots), 1)
    owner = token // seqs
    other_core = jnp.where(owner % 2 == c, 0, 1)
    at = other_core * slots + (owner // 2) * SLOT + (token % seqs) * heads
    attn = jnp.zeros((batch, w_attn.shape[1]), F32)
    for h in range(heads):
        pick = jnp.where(source == at + h, 1.0, 0.0).astype(BF16)
        rows = dot(pick, attended).astype(BF16)
        attn = attn + dot(rows, w_attn[h * HEAD_SIZE : (h + 1) * HEAD_SIZE, :])
    start = pl.multiple_of(seq * HEAD_SIZE, HEAD_SIZE)
    total[:, pl.ds(start, HEAD_SIZE)] = total[:, pl.ds(start, HEAD_SIZE)] + attn

    rows = keep_out.shape[1]
    for i in range(total.shape[1] // HEAD_SIZE):
        block = total[:, i * HEAD_SIZE : (i + 1) * HEAD_SIZE].T.astype(BF16)
        for q in range(0, HEAD_SIZE // rows, 2):
            slot = (i * (HEAD_SIZE // rows) + q) // 2
            even = block[q * rows : (q + 1) * rows, :]
            odd = block[(q + 1) * rows : (q + 2) * rows, :]
            keep_out[slot] = jnp.where(mine, even, odd)
            send_out[slot] = jnp.where(mine, odd, even)
    store.wait()


def block(
    hidden_in,
    norm_gain,
    w_ssm_in,
    w_ssm_gate,
    conv_weight,
    conv_bias,
    conv_state,
    w_state_proj,
    w_step,
    step_bias,
    log_decay,
    skip_gain,
    ssm_state,
    w_ssm_out,
    w_query,
    key_projection,
    value_projection,
    w_attn_out,
    w_mlp_gate,
    w_mlp_up,
    w_mlp_down,
    cached_inputs,
    window_lengths,
):
    batch, features = hidden_in.shape
    width = norm_gain.shape[0]
    channels = w_ssm_in.shape[1]
    window = cached_inputs.shape[1]
    states = log_decay.shape[0]
    cosines, sines = (jnp.asarray(t) for t in rotary_tables(window + 8))

    hidden = hidden_in.T
    copies = jnp.broadcast_to(hidden[None], (64, features, batch))
    held = lax.all_to_all(copies, CHIPS, 0, 0, tiled=True)
    other = shifted(held, "seq_2", 1)

    window_parts = window_rows(
        window_lengths, cached_inputs, key_projection, value_projection, cosines, sines
    )

    normed, conv, low = vmem_call(
        inner_kernel,
        (
            ((width, batch), BF16, True),
            ((channels, batch), F32, True),
            ((2, ROWS, 128), F32, True),
        ),
        (
            held, other, norm_gain.reshape(-1, 128), w_ssm_in.T, w_state_proj,
            jnp.transpose(conv_state, (1, 2, 0)), conv_weight, conv_bias[None],
        ),
        fetched=(3,),
        scratch=(pltpu.VMEM((channels, width), BF16), pltpu.SemaphoreType.DMA),
        cost=pl.CostEstimate(flops=COST, bytes_accessed=0, transcendentals=0),
    )
    paired = shifted(low[1], "seq_2", 1)
    half = low[0] + paired
    arrived = from_ring(half, "grp")
    attended = attended_rows(
        window_lengths, normed, w_query, key_projection, value_projection, *window_parts,
        cosines, sines,
    )
    gate, act = vmem_call(
        gate_kernel,
        (((channels, batch), F32, True), ((w_mlp_up.shape[1], batch), BF16, True)),
        (normed, w_ssm_gate.T, w_mlp_gate.T, w_mlp_up.T),
    )
    (term,) = vmem_call(down_kernel, (((batch, width), F32, True),), (act, w_mlp_down))
    (packed,) = vmem_call(
        pack_kernel, (((16, MAIN + SLOT, HEAD_SIZE), BF16, True),), (*arrived, attended)
    )
    packed = lax.all_to_all(packed, PLANE, 0, 0, tiled=True)
    near_low, near_rows = vmem_call(
        combine_kernel,
        (((ROWS, HEAD_SIZE), F32, True), ((16 * SLOT, HEAD_SIZE), BF16, True)),
        (packed,),
    )
    far_low = shifted(near_low, "seq_2", 1)
    far_rows = shifted(near_rows, "seq_2", 1)

    piece = ((64, features, batch), BF16, True)
    state_new, keep, send = vmem_call(
        outer_kernel,
        (((states, channels, batch), F32, False), piece, piece),
        (
            near_low, far_low, near_rows, far_rows, w_step.T, log_decay, step_bias[None], skip_gain[None], conv, gate,
            jnp.transpose(ssm_state, (1, 2, 0)), w_ssm_out, term, w_attn_out,
        ),
        stored=(0,),
        scratch=(
            pltpu.VMEM((batch, width), F32),
            pltpu.VMEM((states, channels, batch), F32),
            pltpu.SemaphoreType.DMA,
        ),
    )
    came = shifted(send, "seq_2", 1)
    summed = (keep.astype(F32) + came.astype(F32)).astype(BF16)
    arrived = lax.all_to_all(summed, CHIPS, 0, 0, tiled=True)
    total = jnp.sum(arrived.astype(F32), axis=0)
    hidden_out = (hidden.astype(F32) + total).astype(BF16).T
    return (hidden_out, jnp.transpose(state_new, (2, 0, 1)))


def solution(mesh):
    torus = Mesh(
        mesh.devices.reshape(mesh.shape["grp"], 4, 4, 2), ("grp", "seq_0", "seq_1", "seq_2")
    )
    placed = (
        P(None, GRP_SEQ),
        P(),
        P(None, GRP_SEQ),
        P(None, GRP_SEQ),
        P(None, GRP_SEQ),
        P(GRP_SEQ),
        P(None, None, GRP_SEQ),
        P(GRP_SEQ, None),
        P(None, GRP_SEQ),
        P(GRP_SEQ),
        P(None, GRP_SEQ),
        P(GRP_SEQ),
        P(None, None, GRP_SEQ),
        P(GRP_SEQ, None),
        P(None, "grp"),
        P(None, "grp"),
        P(None, "grp"),
        P("grp", SEQ),
        P(None, GRP_SEQ),
        P(None, GRP_SEQ),
        P(GRP_SEQ, None),
        P(SEQ, None, None),
        P(),
    )
    return jax.shard_map(
        block,
        mesh=torus,
        in_specs=placed,
        out_specs=(P(None, GRP_SEQ), P(None, None, GRP_SEQ)),
        check_vma=False,
    )
```

```python
import functools

import jax
import jax.numpy as jnp
import numpy as np
from jax import lax
from jax.experimental import pallas as pl
from jax.experimental.pallas import tpu as pltpu
from jax.sharding import Mesh
from jax.sharding import PartitionSpec as P


HEAD_SIZE = 128
GRP_SEQ = ("grp", "seq_0", "seq_1", "seq_2")
SEQ = ("seq_0", "seq_1", "seq_2")
CHIPS = ("grp", "seq_0", "seq_1")
PLANE = ("seq_0", "seq_1")
EPSILON = 1e-05
ROPE_BASE = 10000.0
F32 = jnp.float32
BF16 = jnp.bfloat16
NT = (((1,), (1,)), ((), ()))
TN = (((0,), (0,)), ((), ()))
RING = 4
ROWS = 144
SLOT = 16
WEIGHT_PIECES = 4
WINDOW_SIZES = (256, 384, 512)
MAIN = 112
COST = 8_000_000_000
TAIL = 32


def rotary_tables(count):
    half = HEAD_SIZE // 2
    frequency = np.float32(ROPE_BASE) ** (
        -(np.arange(half, dtype=np.float32) * np.float32(2.0)) / np.float32(HEAD_SIZE)
    )
    angles = np.arange(count, dtype=np.float32)[:, None] * frequency.astype(np.float32)
    cosine = np.cos(angles.astype(np.float64)).astype(np.float32)
    sine = np.sin(angles.astype(np.float64)).astype(np.float32)
    return (
        np.concatenate([cosine, cosine], axis=1),
        np.concatenate([-sine, sine], axis=1),
    )


def shifted(value, axis, step):
    size = lax.axis_size(axis)
    return lax.ppermute(value, axis, [(i, (i + step) % size) for i in range(size)])


def from_ring(value, axis):
    arrived = [value]
    for step in (1, 3, 2):
        arrived.append(shifted(value, axis, step))
    return [arrived[0], arrived[1], arrived[3], arrived[2]]


def dot(a, b):
    return jnp.dot(a, b, preferred_element_type=F32)


def here():
    return tuple(lax.axis_index(a).astype(jnp.int32) for a in GRP_SEQ)


def own_seq():
    _, x, y, c = here()
    return (x * RING + y) * 2 + c


def in_hbm(value):
    return pltpu.with_memory_space_constraint(value, pltpu.HBM)


def in_vmem(value):
    return pltpu.with_memory_space_constraint(value, pltpu.VMEM)


def vmem_call(kernel, outs, operands, fetched=(), stored=(), scratch=(), limit=12 << 20, cost=None):
    vmem = pl.BlockSpec(memory_space=pltpu.VMEM)
    anywhere = pl.BlockSpec(memory_space=pl.ANY)
    return pl.pallas_call(
        kernel,
        out_shape=tuple(pltpu.VMEM(shape, dtype) if inner else jax.ShapeDtypeStruct(shape, dtype) for shape, dtype, inner in outs),
        in_specs=[anywhere if k in fetched else vmem for k in range(len(operands))],
        out_specs=tuple(anywhere if k in stored else vmem for k in range(len(outs))),
        scratch_shapes=list(scratch),
        compiler_params=pltpu.CompilerParams(vmem_limit_bytes=limit),
        cost_estimate=cost,
    )(*((in_hbm if k in fetched else in_vmem)(v) for k, v in enumerate(operands)))


def window_kernel(
    lengths_hbm, cached, w_key, w_value, cosines, sines, w_in_hbm, key_out, value_out, last_key,
    last_value, w_in,
    rows, weights, cos, sin, early_key, early_value, lengths,
    row_sem, first_sem, key_sem, value_sem, table_sem, out_sem, length_sem, w_in_sem,
):
    seqs, window, width = cached.shape
    columns = w_key.shape[1]
    first = own_seq() * seqs
    pieces = WEIGHT_PIECES
    step = width // pieces

    def piece_copies(p):
        span = pl.ds(p * step, step)
        return (
            pltpu.make_async_copy(
                w_key.at[span], weights.at[span, pl.ds(0, columns)], key_sem.at[p]
            ),
            pltpu.make_async_copy(
                w_value.at[span], weights.at[span, pl.ds(columns, columns)], value_sem.at[p]
            ),
            pltpu.make_async_copy(cached.at[0, :, span], rows.at[0, :, span], first_sem.at[p]),
        )

    tables = (
        pltpu.make_async_copy(cosines.at[pl.ds(0, window)], cos, table_sem.at[0]),
        pltpu.make_async_copy(sines.at[pl.ds(0, window)], sin, table_sem.at[1]),
    )
    later = [
        pltpu.make_async_copy(cached.at[b], rows.at[b], row_sem.at[b]) for b in range(1, seqs)
    ]
    fetch = pltpu.make_async_copy(lengths_hbm, lengths, length_sem)
    fetch.start()
    for p in range(pieces):
        for copy in piece_copies(p):
            copy.start()
    for copy in tables:
        copy.start()
    for copy in later:
        copy.start()
    ahead = pltpu.make_async_copy(w_in_hbm, w_in, w_in_sem)
    ahead.start()
    fetch.wait()

    def finish(b, both):
        live = both.shape[0]
        at = b if b < seqs - 1 else 0
        turned, plain = (early_key, early_value) if b < seqs - 1 else (last_key, last_value)
        for head in range(columns // HEAD_SIZE):
            lanes = slice(head * HEAD_SIZE, (head + 1) * HEAD_SIZE)
            part = both[:, lanes]
            turned[at, 0:live, lanes] = (
                part * cos[0:live, :] + pltpu.roll(part, HEAD_SIZE // 2, 1) * sin[0:live, :]
            ).astype(BF16)
        plain[at, 0:live, :] = both[:, columns:].astype(BF16)
        if live < window:
            turned[at, live:, :] = jnp.zeros((window - live, columns), BF16)
            plain[at, live:, :] = jnp.zeros((window - live, columns), BF16)

    def by_length(b, work):
        length = lengths[first + b]
        low = 0
        for size in WINDOW_SIZES:
            if size == WINDOW_SIZES[0]:
                chosen = length <= size
            elif size == WINDOW_SIZES[-1]:
                chosen = length > low
            else:
                chosen = (length > low) & (length <= size)
            pl.when(chosen)(functools.partial(work, size))
            low = size

    def out_copies(b):
        return (
            pltpu.make_async_copy(early_key.at[b], key_out.at[b], out_sem.at[0, b]),
            pltpu.make_async_copy(early_value.at[b], value_out.at[b], out_sem.at[1, b]),
        )

    def first_rows(size):
        total = None
        for p in range(pieces):
            for copy in piece_copies(p):
                copy.wait()
            span = slice(p * step, (p + 1) * step)
            part = dot(rows[0, 0:size, span], weights[span, :])
            total = part if total is None else total + part
        for copy in tables:
            copy.wait()
        finish(0, total)

    by_length(0, first_rows)
    for copy in out_copies(0):
        copy.start()
    for b in range(1, seqs):
        later[b - 1].wait()
        by_length(b, lambda size, b=b: finish(b, dot(rows[b, 0:size, :], weights[...])))
        if b < seqs - 1:
            for copy in out_copies(b):
                copy.start()
    ahead.wait()
    for b in range(seqs - 1):
        for copy in out_copies(b):
            copy.wait()


def window_rows(lengths, cached, w_key, w_value, cosines, sines, w_in):
    seqs, window, width = cached.shape
    columns = w_key.shape[1]
    anywhere = pl.BlockSpec(memory_space=pl.ANY)
    early = (seqs - 1, window, columns)
    last = (1, window, columns)
    vmem = pl.BlockSpec(memory_space=pltpu.VMEM)
    dma = pltpu.SemaphoreType.DMA
    return pl.pallas_call(
        window_kernel,
        out_shape=(
            pltpu.HBM(early, BF16),
            pltpu.HBM(early, BF16),
            pltpu.VMEM(last, BF16),
            pltpu.VMEM(last, BF16),
            pltpu.VMEM(w_in.shape, BF16),
        ),
        in_specs=[anywhere] * 7,
        out_specs=(anywhere, anywhere, vmem, vmem, vmem),
        scratch_shapes=[
            pltpu.VMEM((seqs, window, width), BF16),
            pltpu.VMEM((width, 2 * columns), BF16),
            pltpu.VMEM((window, HEAD_SIZE), F32),
            pltpu.VMEM((window, HEAD_SIZE), F32),
            pltpu.VMEM(early, BF16),
            pltpu.VMEM(early, BF16),
            pltpu.SMEM(lengths.shape, jnp.int32),
            dma((seqs,)),
            dma((WEIGHT_PIECES,)),
            dma((WEIGHT_PIECES,)),
            dma((WEIGHT_PIECES,)),
            dma((2,)),
            dma((2, seqs - 1)),
            dma,
            dma,
        ],
        compiler_params=pltpu.CompilerParams(vmem_limit_bytes=40 << 20),
    )(*(in_hbm(v) for v in (lengths, cached, w_key, w_value, cosines, sines, w_in)))


def inner_kernel(
    near, far, gain, w_in, w_proj, past, taps, bias, normed_out, conv_out, low_out,
):
    c = lax.axis_index("seq_2").astype(jnp.int32)
    rows, batch = near.shape[1], near.shape[2]
    total = jnp.zeros((rows, batch), F32)
    for slot in range(near.shape[0]):
        a = near[slot].astype(F32)
        b = far[slot].astype(F32)
        total = total + a * a + b * b
    width = gain.shape[0] * gain.shape[1]
    mean = jnp.sum(total, axis=0, keepdims=True) * (1.0 / width)
    scale = lax.rsqrt(mean + EPSILON)
    gains = gain[...].T
    mine = c == 0
    per_gain = gain.shape[1] // rows
    for slot in range(near.shape[0]):
        a = near[slot].astype(F32)
        b = far[slot].astype(F32)
        pair = (jnp.where(mine, a, b), jnp.where(mine, b, a))
        for k in range(2):
            j = 2 * slot + k
            at = (j % per_gain) * rows
            column = gains[at : at + rows, j // per_gain : j // per_gain + 1]
            normed_out[j * rows : (j + 1) * rows, :] = (pair[k] * scale * column).astype(BF16)
    fresh = dot(w_in[...], normed_out[...]).astype(BF16).astype(F32)
    params = jnp.concatenate([taps[...], bias[...], jnp.zeros((3, taps.shape[1]), F32)], axis=0).T
    mixed = params[:, 4:5] + params[:, 3:4] * fresh
    for k in range(past.shape[0]):
        mixed = mixed + past[k].astype(F32) * params[:, k : k + 1]
    conv = jax.nn.silu(mixed)
    conv_out[...] = conv
    low = lax.dot_general(w_proj[...], conv.astype(BF16), TN, preferred_element_type=F32)
    low = jnp.concatenate([low, jnp.zeros((low.shape[0], 128 - batch), F32)], axis=1)
    low_out[c] = low[0:ROWS]
    low_out[1 - c] = low[ROWS:]


def gate_kernel(normed, w_gate, w_mlp_gate, w_mlp_up, gate_out, act_out):
    gate_out[...] = jax.nn.silu(dot(w_gate[...], normed[...]))
    act = jax.nn.silu(dot(w_mlp_gate[...], normed[...])) * dot(w_mlp_up[...], normed[...])
    act_out[...] = act.astype(BF16)


def down_kernel(act, w_mlp_down, term_out):
    term_out[...] = lax.dot_general(act[...], w_mlp_down[...], TN, preferred_element_type=F32)


def attention_kernel(
    lengths_hbm, normed, w_query, w_key, w_value, last_key, last_value, key_rows, value_rows,
    cosines, sines, out,
    keys, values, cos_rows, sin_rows, lengths, row_sem, table_sem, length_sem,
):
    fetch = pltpu.make_async_copy(lengths_hbm, lengths, length_sem)
    fetch.start()
    seqs, window = keys.shape[0] + 1, keys.shape[1]
    columns = keys.shape[2]
    queries = w_query.shape[1]
    kv_heads = columns // HEAD_SIZE
    group = queries // columns
    batch = normed.shape[1]
    first = own_seq() * seqs
    row_copies = (
        pltpu.make_async_copy(key_rows, keys, row_sem.at[0]),
        pltpu.make_async_copy(value_rows, values, row_sem.at[1]),
    )
    for copy in row_copies:
        copy.start()
    fetch.wait()
    table_copies = []
    for b in range(seqs):
        at = pl.ds(lengths[first + b], 1)
        table_copies.append(
            pltpu.make_async_copy(cosines.at[at], cos_rows.at[pl.ds(b, 1)], table_sem.at[0, b])
        )
        table_copies.append(
            pltpu.make_async_copy(sines.at[at], sin_rows.at[pl.ds(b, 1)], table_sem.at[1, b])
        )
    for copy in table_copies:
        copy.start()
    row = lax.broadcasted_iota(jnp.int32, (8, batch), 0)
    column = lax.broadcasted_iota(jnp.int32, (8, batch), 1)
    pick = jnp.where((column == first + row) & (row < seqs), 1.0, 0.0).astype(BF16)
    own = lax.dot_general(pick, normed[...], NT, preferred_element_type=F32).astype(BF16)
    query = dot(own, w_query[...])
    fresh_key = dot(own, w_key[...])
    fresh_value = dot(own, w_value[...]).astype(BF16).astype(F32)
    for copy in (*table_copies, *row_copies):
        copy.wait()
    scale = HEAD_SIZE ** (-0.5)
    blocks = [(b, g) for b in range(seqs) for g in range(kv_heads)]
    height = len(blocks) * 8
    spare = jnp.zeros((8 - group, HEAD_SIZE), F32)
    stacked, cos, sin, new_key, new_value = [], [], [], [], []
    for b, g in blocks:
        lanes = slice(g * HEAD_SIZE, (g + 1) * HEAD_SIZE)
        for i in range(group):
            head = g * group + i
            stacked.append(query[b : b + 1, head * HEAD_SIZE : (head + 1) * HEAD_SIZE])
        stacked.append(spare)
        cos.append(jnp.broadcast_to(cos_rows[b : b + 1, :], (8, HEAD_SIZE)))
        sin.append(jnp.broadcast_to(sin_rows[b : b + 1, :], (8, HEAD_SIZE)))
        new_key.append(jnp.broadcast_to(fresh_key[b : b + 1, lanes], (8, HEAD_SIZE)))
        new_value.append(jnp.broadcast_to(fresh_value[b : b + 1, lanes], (8, HEAD_SIZE)))
    cos = jnp.concatenate(cos, axis=0)
    sin = jnp.concatenate(sin, axis=0)

    def turned(part):
        return (part * cos + pltpu.roll(part, HEAD_SIZE // 2, 1) * sin).astype(BF16)

    q = turned(jnp.concatenate(stacked, axis=0))
    k_new = turned(jnp.concatenate(new_key, axis=0))

    def row_of(early, last, b):
        return early.at[b] if b < seqs - 1 else last.at[0]

    scores = jnp.concatenate(
        [
            lax.dot_general(
                q[n * 8 : n * 8 + 8],
                row_of(keys, last_key, b)[:, g * HEAD_SIZE : (g + 1) * HEAD_SIZE],
                NT,
                preferred_element_type=F32,
            )
            for n, (b, g) in enumerate(blocks)
        ],
        axis=0,
    ) * scale
    fresh = jnp.sum(q.astype(F32) * k_new.astype(F32), axis=1, keepdims=True) * scale
    slot_ids = lax.broadcasted_iota(jnp.int32, (height, window), 1)
    owner = lax.broadcasted_iota(jnp.int32, (height, window), 0) // (8 * kv_heads)
    length = jnp.where(
        owner == 0,
        lengths[first],
        jnp.where(owner == 1, lengths[first + 1], lengths[first + 2]),
    )
    valid = slot_ids < length
    scores = jnp.where(valid, scores, -1e30)
    top = jnp.maximum(jnp.max(scores, axis=1, keepdims=True), fresh)
    shares = jnp.where(valid, jnp.exp(scores - top), 0.0)
    share_new = jnp.exp(fresh - top)
    denominator = jnp.sum(shares, axis=1, keepdims=True) + share_new
    rounded = shares.astype(BF16)
    summed = jnp.concatenate(
        [
            dot(rounded[n * 8 : n * 8 + 8], row_of(values, last_value, b)[:, g * HEAD_SIZE : (g + 1) * HEAD_SIZE])
            for n, (b, g) in enumerate(blocks)
        ],
        axis=0,
    )
    result = (summed + share_new * jnp.concatenate(new_value, axis=0)) / denominator
    result = result.astype(BF16).astype(F32)
    out[...] = jnp.zeros((SLOT, HEAD_SIZE), F32)
    for n in range(len(blocks)):
        out[n * group : (n + 1) * group, :] = result[n * 8 : n * 8 + group, :]


def attended_rows(
    lengths, normed, w_query, w_key, w_value, keys, values, last_key, last_value, cosines, sines
):
    anywhere = pl.BlockSpec(memory_space=pl.ANY)
    vmem = pl.BlockSpec(memory_space=pltpu.VMEM)
    dma = pltpu.SemaphoreType.DMA
    return pl.pallas_call(
        attention_kernel,
        out_shape=pltpu.VMEM((SLOT, HEAD_SIZE), F32),
        in_specs=[anywhere] + [vmem] * 6 + [anywhere] * 4,
        out_specs=vmem,
        scratch_shapes=[
            pltpu.VMEM(keys.shape, BF16),
            pltpu.VMEM(values.shape, BF16),
            pltpu.VMEM((8, HEAD_SIZE), F32),
            pltpu.VMEM((8, HEAD_SIZE), F32),
            pltpu.SMEM(lengths.shape, jnp.int32),
            dma((2,)),
            dma((2, keys.shape[0] + 1)),
            dma,
        ],
        compiler_params=pltpu.CompilerParams(vmem_limit_bytes=12 << 20),
    )(
        in_hbm(lengths),
        *(in_vmem(v) for v in (normed, w_query, w_key, w_value, last_key, last_value)),
        *(in_hbm(v) for v in (keys, values, cosines, sines)),
    )


def pack_kernel(s0, s1, s2, s3, attended, out):
    parts = [s[...].astype(F32) for s in (s0, s1, s2, s3)]
    low = (parts[0] + parts[1]) + (parts[2] + parts[3])
    tail = low[MAIN:, :]
    moved = [pltpu.roll(tail, 96 - TAIL * p, 1) for p in range(3)]
    moved.append(jnp.zeros((MAIN - 3 * TAIL, HEAD_SIZE), F32))
    lane = lax.broadcasted_iota(jnp.int32, (MAIN, HEAD_SIZE), 1)
    low = jnp.where(lane < 96, low[0:MAIN, :], jnp.concatenate(moved, axis=0)).astype(BF16)
    rows = attended[...].astype(BF16)
    for k in range(out.shape[0]):
        out[k, 0:MAIN, :] = low
        out[k, MAIN:, :] = rows


def combine_kernel(arrived, low_out, rows_out):
    total = arrived[0, 0:MAIN, :].astype(F32)
    rows_out[0:SLOT, :] = arrived[0, MAIN:, :]
    for k in range(1, arrived.shape[0]):
        total = total + arrived[k, 0:MAIN, :].astype(F32)
        rows_out[k * SLOT : (k + 1) * SLOT, :] = arrived[k, MAIN:, :]
    low_out[0:MAIN, :] = total
    lane = lax.broadcasted_iota(jnp.int32, (TAIL, HEAD_SIZE), 1)
    tail = jnp.zeros((TAIL, HEAD_SIZE), F32)
    for p in range(3):
        back = pltpu.roll(total[TAIL * p : TAIL * (p + 1), :], HEAD_SIZE - 96 + TAIL * p, 1)
        tail = jnp.where(lane // TAIL == p, back, tail)
    low_out[MAIN:, :] = tail


def outer_kernel(
    near, far, near_rows, far_rows, w_step, log_decay, step_bias, skip, conv, gate, state, w_out, term, w_attn,
    state_hbm, keep_out, send_out, total, state_out, state_sem,
):
    c = lax.axis_index("seq_2").astype(jnp.int32)
    seq = own_seq()
    batch = conv.shape[1]
    mine = c == 0
    near_low = near[:, 0:batch]
    far_low = far[:, 0:batch]
    low = jnp.concatenate(
        [jnp.where(mine, near_low, far_low), jnp.where(mine, far_low, near_low)], axis=0
    )
    rank = w_step.shape[1]
    states = state.shape[0]
    params = jnp.concatenate(
        [jnp.exp(log_decay[...]), step_bias[...], skip[...], jnp.zeros((6, conv.shape[0]), F32)],
        axis=0,
    ).T
    step = jax.nn.softplus(
        dot(w_step[...], low[0:rank].astype(BF16)) + params[:, states : states + 1]
    )
    conv_value = conv[...]
    driven = step * conv_value
    mixed = params[:, states + 1 : states + 2] * conv_value
    for n in range(states):
        decay = jnp.exp(-step * params[:, n : n + 1])
        fresh = decay * state[n] + driven * low[rank + n : rank + n + 1]
        state_out[n] = fresh
        mixed = mixed + fresh * low[rank + states + n : rank + states + n + 1]
    store = pltpu.make_async_copy(state_out, state_hbm, state_sem)
    store.start()
    gated = (mixed * gate[...]).astype(BF16)
    total[...] = term[...] + lax.dot_general(gated, w_out[...], TN, preferred_element_type=F32)

    slots = near_rows.shape[0]
    attended = jnp.concatenate([near_rows[...], far_rows[...]], axis=0)
    seqs = 3
    heads = w_attn.shape[0] // HEAD_SIZE
    token = lax.broadcasted_iota(jnp.int32, (batch, 2 * slots), 0)
    source = lax.broadcasted_iota(jnp.int32, (batch, 2 * slots), 1)
    owner = token // seqs
    other_core = jnp.where(owner % 2 == c, 0, 1)
    at = other_core * slots + (owner // 2) * SLOT + (token % seqs) * heads
    attn = jnp.zeros((batch, w_attn.shape[1]), F32)
    for h in range(heads):
        pick = jnp.where(source == at + h, 1.0, 0.0).astype(BF16)
        rows = dot(pick, attended).astype(BF16)
        attn = attn + dot(rows, w_attn[h * HEAD_SIZE : (h + 1) * HEAD_SIZE, :])
    start = pl.multiple_of(seq * HEAD_SIZE, HEAD_SIZE)
    total[:, pl.ds(start, HEAD_SIZE)] = total[:, pl.ds(start, HEAD_SIZE)] + attn

    rows = keep_out.shape[1]
    for i in range(total.shape[1] // HEAD_SIZE):
        block = total[:, i * HEAD_SIZE : (i + 1) * HEAD_SIZE].T.astype(BF16)
        for q in range(0, HEAD_SIZE // rows, 2):
            slot = (i * (HEAD_SIZE // rows) + q) // 2
            even = block[q * rows : (q + 1) * rows, :]
            odd = block[(q + 1) * rows : (q + 2) * rows, :]
            keep_out[slot] = jnp.where(mine, even, odd)
            send_out[slot] = jnp.where(mine, odd, even)
    store.wait()


def block(
    hidden_in,
    norm_gain,
    w_ssm_in,
    w_ssm_gate,
    conv_weight,
    conv_bias,
    conv_state,
    w_state_proj,
    w_step,
    step_bias,
    log_decay,
    skip_gain,
    ssm_state,
    w_ssm_out,
    w_query,
    key_projection,
    value_projection,
    w_attn_out,
    w_mlp_gate,
    w_mlp_up,
    w_mlp_down,
    cached_inputs,
    window_lengths,
):
    batch, features = hidden_in.shape
    width = norm_gain.shape[0]
    channels = w_ssm_in.shape[1]
    window = cached_inputs.shape[1]
    states = log_decay.shape[0]
    cosines, sines = (jnp.asarray(t) for t in rotary_tables(window + 8))

    hidden = hidden_in.T
    copies = jnp.broadcast_to(hidden[None], (64, features, batch))
    held = lax.all_to_all(copies, CHIPS, 0, 0, tiled=True)
    other = shifted(held, "seq_2", 1)

    *window_parts, w_in = window_rows(
        window_lengths, cached_inputs, key_projection, value_projection, cosines, sines,
        w_ssm_in.T,
    )

    normed, conv, low = vmem_call(
        inner_kernel,
        (
            ((width, batch), BF16, True),
            ((channels, batch), F32, True),
            ((2, ROWS, 128), F32, True),
        ),
        (
            held, other, norm_gain.reshape(-1, 128), w_in, w_state_proj,
            jnp.transpose(conv_state, (1, 2, 0)), conv_weight, conv_bias[None],
        ),
        cost=pl.CostEstimate(flops=COST, bytes_accessed=0, transcendentals=0),
    )
    paired = shifted(low[1], "seq_2", 1)
    half = (low[0] + paired).astype(BF16)
    arrived = from_ring(half, "grp")
    attended = attended_rows(
        window_lengths, normed, w_query, key_projection, value_projection, *window_parts,
        cosines, sines,
    )
    gate, act = vmem_call(
        gate_kernel,
        (((channels, batch), F32, True), ((w_mlp_up.shape[1], batch), BF16, True)),
        (normed, w_ssm_gate.T, w_mlp_gate.T, w_mlp_up.T),
    )
    (term,) = vmem_call(down_kernel, (((batch, width), F32, True),), (act, w_mlp_down))
    (packed,) = vmem_call(
        pack_kernel, (((16, MAIN + SLOT, HEAD_SIZE), BF16, True),), (*arrived, attended)
    )
    packed = lax.all_to_all(packed, PLANE, 0, 0, tiled=True)
    near_low, near_rows = vmem_call(
        combine_kernel,
        (((ROWS, HEAD_SIZE), F32, True), ((16 * SLOT, HEAD_SIZE), BF16, True)),
        (packed,),
    )
    far_low = shifted(near_low, "seq_2", 1)
    far_rows = shifted(near_rows, "seq_2", 1)

    piece = ((64, features, batch), BF16, True)
    state_new, keep, send = vmem_call(
        outer_kernel,
        (((states, channels, batch), F32, False), piece, piece),
        (
            near_low, far_low, near_rows, far_rows, w_step.T, log_decay, step_bias[None], skip_gain[None], conv, gate,
            jnp.transpose(ssm_state, (1, 2, 0)), w_ssm_out, term, w_attn_out,
        ),
        stored=(0,),
        scratch=(
            pltpu.VMEM((batch, width), F32),
            pltpu.VMEM((states, channels, batch), F32),
            pltpu.SemaphoreType.DMA,
        ),
    )
    came = shifted(send, "seq_2", 1)
    summed = (keep.astype(F32) + came.astype(F32)).astype(BF16)
    arrived = lax.all_to_all(summed, CHIPS, 0, 0, tiled=True)
    total = jnp.sum(arrived.astype(F32), axis=0)
    hidden_out = (hidden.astype(F32) + total).astype(BF16).T
    return (hidden_out, jnp.transpose(state_new, (2, 0, 1)))


def solution(mesh):
    torus = Mesh(
        mesh.devices.reshape(mesh.shape["grp"], 4, 4, 2), ("grp", "seq_0", "seq_1", "seq_2")
    )
    placed = (
        P(None, GRP_SEQ),
        P(),
        P(None, GRP_SEQ),
        P(None, GRP_SEQ),
        P(None, GRP_SEQ),
        P(GRP_SEQ),
        P(None, None, GRP_SEQ),
        P(GRP_SEQ, None),
        P(None, GRP_SEQ),
        P(GRP_SEQ),
        P(None, GRP_SEQ),
        P(GRP_SEQ),
        P(None, None, GRP_SEQ),
        P(GRP_SEQ, None),
        P(None, "grp"),
        P(None, "grp"),
        P(None, "grp"),
        P("grp", SEQ),
        P(None, GRP_SEQ),
        P(None, GRP_SEQ),
        P(GRP_SEQ, None),
        P(SEQ, None, None),
        P(),
    )
    return jax.shard_map(
        block,
        mesh=torus,
        in_specs=placed,
        out_specs=(P(None, GRP_SEQ), P(None, None, GRP_SEQ)),
        check_vma=False,
    )
```

```python
import functools

import jax
import jax.numpy as jnp
import numpy as np
from jax import lax
from jax.experimental import pallas as pl
from jax.experimental.pallas import tpu as pltpu
from jax.sharding import Mesh
from jax.sharding import PartitionSpec as P


HEAD_SIZE = 128
GRP_SEQ = ("grp", "seq_0", "seq_1", "seq_2")
SEQ = ("seq_0", "seq_1", "seq_2")
CHIPS = ("grp", "seq_0", "seq_1")
PLANE = ("seq_0", "seq_1")
EPSILON = 1e-05
ROPE_BASE = 10000.0
F32 = jnp.float32
BF16 = jnp.bfloat16
NT = (((1,), (1,)), ((), ()))
TN = (((0,), (0,)), ((), ()))
RING = 4
ROWS = 144
SLOT = 16
WEIGHT_PIECES = 4
WINDOW_SIZES = (128, 256, 384, 512)
MAIN = 112
COST = 8_000_000_000
TAIL = 32


def rotary_tables(count):
    half = HEAD_SIZE // 2
    frequency = np.float32(ROPE_BASE) ** (
        -(np.arange(half, dtype=np.float32) * np.float32(2.0)) / np.float32(HEAD_SIZE)
    )
    angles = np.arange(count, dtype=np.float32)[:, None] * frequency.astype(np.float32)
    cosine = np.cos(angles.astype(np.float64)).astype(np.float32)
    sine = np.sin(angles.astype(np.float64)).astype(np.float32)
    return (
        np.concatenate([cosine, cosine], axis=1),
        np.concatenate([-sine, sine], axis=1),
    )


def shifted(value, axis, step):
    size = lax.axis_size(axis)
    return lax.ppermute(value, axis, [(i, (i + step) % size) for i in range(size)])


def from_ring(value, axis):
    arrived = [value]
    for step in (1, 3, 2):
        arrived.append(shifted(value, axis, step))
    return [arrived[0], arrived[1], arrived[3], arrived[2]]


def dot(a, b):
    return jnp.dot(a, b, preferred_element_type=F32)


def here():
    return tuple(lax.axis_index(a).astype(jnp.int32) for a in GRP_SEQ)


def own_seq():
    _, x, y, c = here()
    return (x * RING + y) * 2 + c


def in_hbm(value):
    return pltpu.with_memory_space_constraint(value, pltpu.HBM)


def in_vmem(value):
    return pltpu.with_memory_space_constraint(value, pltpu.VMEM)


def vmem_call(kernel, outs, operands, fetched=(), stored=(), scratch=(), limit=12 << 20, cost=None):
    vmem = pl.BlockSpec(memory_space=pltpu.VMEM)
    anywhere = pl.BlockSpec(memory_space=pl.ANY)
    return pl.pallas_call(
        kernel,
        out_shape=tuple(pltpu.VMEM(shape, dtype) if inner else jax.ShapeDtypeStruct(shape, dtype) for shape, dtype, inner in outs),
        in_specs=[anywhere if k in fetched else vmem for k in range(len(operands))],
        out_specs=tuple(anywhere if k in stored else vmem for k in range(len(outs))),
        scratch_shapes=list(scratch),
        compiler_params=pltpu.CompilerParams(vmem_limit_bytes=limit),
        cost_estimate=cost,
    )(*((in_hbm if k in fetched else in_vmem)(v) for k, v in enumerate(operands)))


def window_kernel(
    lengths_hbm, cached, w_key, w_value, cosines, sines, w_in_hbm, key_out, value_out, cos_rows,
    sin_rows, w_in,
    rows, weights, cos, sin, lengths,
    row_sem, first_sem, key_sem, value_sem, table_sem, length_sem, w_in_sem,
):
    seqs, window, width = cached.shape
    columns = w_key.shape[1]
    first = own_seq() * seqs
    pieces = WEIGHT_PIECES
    step = width // pieces

    def piece_copies(p):
        span = pl.ds(p * step, step)
        return (
            pltpu.make_async_copy(
                w_key.at[span], weights.at[span, pl.ds(0, columns)], key_sem.at[p]
            ),
            pltpu.make_async_copy(
                w_value.at[span], weights.at[span, pl.ds(columns, columns)], value_sem.at[p]
            ),
            pltpu.make_async_copy(cached.at[0, :, span], rows.at[0, :, span], first_sem.at[p]),
        )

    tables = (
        pltpu.make_async_copy(cosines, cos, table_sem.at[0]),
        pltpu.make_async_copy(sines, sin, table_sem.at[1]),
    )
    later = [
        pltpu.make_async_copy(cached.at[b], rows.at[b], row_sem.at[b]) for b in range(1, seqs)
    ]
    fetch = pltpu.make_async_copy(lengths_hbm, lengths, length_sem)
    fetch.start()
    for p in range(pieces):
        for copy in piece_copies(p):
            copy.start()
    for copy in tables:
        copy.start()
    for copy in later:
        copy.start()
    ahead = pltpu.make_async_copy(w_in_hbm, w_in, w_in_sem)
    ahead.start()
    fetch.wait()

    def finish(b, both):
        live = both.shape[0]
        for head in range(columns // HEAD_SIZE):
            lanes = slice(head * HEAD_SIZE, (head + 1) * HEAD_SIZE)
            part = both[:, lanes]
            key_out[b, 0:live, lanes] = (
                part * cos[0:live, :] + pltpu.roll(part, HEAD_SIZE // 2, 1) * sin[0:live, :]
            ).astype(BF16)
        value_out[b, 0:live, :] = both[:, columns:].astype(BF16)
        if live < window:
            key_out[b, live:, :] = jnp.zeros((window - live, columns), BF16)
            value_out[b, live:, :] = jnp.zeros((window - live, columns), BF16)

    def by_length(b, work):
        length = lengths[first + b]
        low = 0
        for size in WINDOW_SIZES:
            if size == WINDOW_SIZES[0]:
                chosen = length <= size
            elif size == WINDOW_SIZES[-1]:
                chosen = length > low
            else:
                chosen = (length > low) & (length <= size)
            pl.when(chosen)(functools.partial(work, size))
            low = size

    def first_rows(size):
        total = None
        for p in range(pieces):
            for copy in piece_copies(p):
                copy.wait()
            span = slice(p * step, (p + 1) * step)
            part = dot(rows[0, 0:size, span], weights[span, :])
            total = part if total is None else total + part
        for copy in tables:
            copy.wait()
        finish(0, total)

    by_length(0, first_rows)
    for b in range(1, seqs):
        later[b - 1].wait()
        by_length(b, lambda size, b=b: finish(b, dot(rows[b, 0:size, :], weights[...])))
    for b in range(seqs):
        at = pl.ds(lengths[first + b], 1)
        cos_rows[b : b + 1, :] = cos[at, :]
        sin_rows[b : b + 1, :] = sin[at, :]
    ahead.wait()


def window_rows(lengths, cached, w_key, w_value, cosines, sines, w_in):
    seqs, window, width = cached.shape
    columns = w_key.shape[1]
    anywhere = pl.BlockSpec(memory_space=pl.ANY)
    projected = pltpu.VMEM((seqs, window, columns), BF16)
    angles = pltpu.VMEM((8, HEAD_SIZE), F32)
    vmem = pl.BlockSpec(memory_space=pltpu.VMEM)
    dma = pltpu.SemaphoreType.DMA
    return pl.pallas_call(
        window_kernel,
        out_shape=(
            projected, projected, angles, angles, pltpu.VMEM(w_in.shape, BF16)
        ),
        in_specs=[anywhere] * 7,
        out_specs=(vmem,) * 5,
        scratch_shapes=[
            pltpu.VMEM((seqs, window, width), BF16),
            pltpu.VMEM((width, 2 * columns), BF16),
            pltpu.VMEM(cosines.shape, F32),
            pltpu.VMEM(sines.shape, F32),
            pltpu.SMEM(lengths.shape, jnp.int32),
            dma((seqs,)),
            dma((WEIGHT_PIECES,)),
            dma((WEIGHT_PIECES,)),
            dma((WEIGHT_PIECES,)),
            dma((2,)),
            dma,
            dma,
        ],
        compiler_params=pltpu.CompilerParams(vmem_limit_bytes=40 << 20),
    )(*(in_hbm(v) for v in (lengths, cached, w_key, w_value, cosines, sines, w_in)))


def inner_kernel(
    near, far, gain, w_in, w_proj, past, taps, bias, normed_out, conv_out, low_out,
):
    c = lax.axis_index("seq_2").astype(jnp.int32)
    rows, batch = near.shape[1], near.shape[2]
    total = jnp.zeros((rows, batch), F32)
    for slot in range(near.shape[0]):
        a = near[slot].astype(F32)
        b = far[slot].astype(F32)
        total = total + a * a + b * b
    width = gain.shape[0] * gain.shape[1]
    mean = jnp.sum(total, axis=0, keepdims=True) * (1.0 / width)
    scale = lax.rsqrt(mean + EPSILON)
    gains = gain[...].T
    mine = c == 0
    per_gain = gain.shape[1] // rows
    for slot in range(near.shape[0]):
        a = near[slot].astype(F32)
        b = far[slot].astype(F32)
        pair = (jnp.where(mine, a, b), jnp.where(mine, b, a))
        for k in range(2):
            j = 2 * slot + k
            at = (j % per_gain) * rows
            column = gains[at : at + rows, j // per_gain : j // per_gain + 1]
            normed_out[j * rows : (j + 1) * rows, :] = (pair[k] * scale * column).astype(BF16)
    fresh = dot(w_in[...], normed_out[...]).astype(BF16).astype(F32)
    params = jnp.concatenate([taps[...], bias[...], jnp.zeros((3, taps.shape[1]), F32)], axis=0).T
    mixed = params[:, 4:5] + params[:, 3:4] * fresh
    for k in range(past.shape[0]):
        mixed = mixed + past[k].astype(F32) * params[:, k : k + 1]
    conv = jax.nn.silu(mixed)
    conv_out[...] = conv
    low = lax.dot_general(w_proj[...], conv.astype(BF16), TN, preferred_element_type=F32)
    low = jnp.concatenate([low, jnp.zeros((low.shape[0], 128 - batch), F32)], axis=1)
    low_out[c] = low[0:ROWS]
    low_out[1 - c] = low[ROWS:]


def gate_kernel(normed, w_gate, w_mlp_gate, w_mlp_up, gate_out, act_out):
    gate_out[...] = jax.nn.silu(dot(w_gate[...], normed[...]))
    act = jax.nn.silu(dot(w_mlp_gate[...], normed[...])) * dot(w_mlp_up[...], normed[...])
    act_out[...] = act.astype(BF16)


def down_kernel(act, w_mlp_down, term_out):
    term_out[...] = lax.dot_general(act[...], w_mlp_down[...], TN, preferred_element_type=F32)


def attention_kernel(
    lengths_hbm, normed, w_query, w_key, w_value, keys, values, cos_rows, sin_rows, out,
    lengths, length_sem,
):
    fetch = pltpu.make_async_copy(lengths_hbm, lengths, length_sem)
    fetch.start()
    seqs, window, columns = keys.shape
    queries = w_query.shape[1]
    kv_heads = columns // HEAD_SIZE
    group = queries // columns
    batch = normed.shape[1]
    first = own_seq() * seqs
    row = lax.broadcasted_iota(jnp.int32, (8, batch), 0)
    column = lax.broadcasted_iota(jnp.int32, (8, batch), 1)
    pick = jnp.where((column == first + row) & (row < seqs), 1.0, 0.0).astype(BF16)
    own = lax.dot_general(pick, normed[...], NT, preferred_element_type=F32).astype(BF16)
    query = dot(own, w_query[...])
    fresh_key = dot(own, w_key[...])
    fresh_value = dot(own, w_value[...]).astype(BF16).astype(F32)
    scale = HEAD_SIZE ** (-0.5)
    blocks = [(b, g) for b in range(seqs) for g in range(kv_heads)]
    height = len(blocks) * 8
    spare = jnp.zeros((8 - group, HEAD_SIZE), F32)
    stacked, cos, sin, new_key, new_value = [], [], [], [], []
    for b, g in blocks:
        lanes = slice(g * HEAD_SIZE, (g + 1) * HEAD_SIZE)
        for i in range(group):
            head = g * group + i
            stacked.append(query[b : b + 1, head * HEAD_SIZE : (head + 1) * HEAD_SIZE])
        stacked.append(spare)
        cos.append(jnp.broadcast_to(cos_rows[b : b + 1, :], (8, HEAD_SIZE)))
        sin.append(jnp.broadcast_to(sin_rows[b : b + 1, :], (8, HEAD_SIZE)))
        new_key.append(jnp.broadcast_to(fresh_key[b : b + 1, lanes], (8, HEAD_SIZE)))
        new_value.append(jnp.broadcast_to(fresh_value[b : b + 1, lanes], (8, HEAD_SIZE)))
    cos = jnp.concatenate(cos, axis=0)
    sin = jnp.concatenate(sin, axis=0)

    def turned(part):
        return (part * cos + pltpu.roll(part, HEAD_SIZE // 2, 1) * sin).astype(BF16)

    q = turned(jnp.concatenate(stacked, axis=0))
    k_new = turned(jnp.concatenate(new_key, axis=0))
    scores = jnp.concatenate(
        [
            lax.dot_general(
                q[n * 8 : n * 8 + 8],
                keys[b, :, g * HEAD_SIZE : (g + 1) * HEAD_SIZE],
                NT,
                preferred_element_type=F32,
            )
            for n, (b, g) in enumerate(blocks)
        ],
        axis=0,
    ) * scale
    fresh = jnp.sum(q.astype(F32) * k_new.astype(F32), axis=1, keepdims=True) * scale
    fetch.wait()
    slot_ids = lax.broadcasted_iota(jnp.int32, (height, window), 1)
    owner = lax.broadcasted_iota(jnp.int32, (height, window), 0) // (8 * kv_heads)
    length = jnp.where(
        owner == 0,
        lengths[first],
        jnp.where(owner == 1, lengths[first + 1], lengths[first + 2]),
    )
    valid = slot_ids < length
    scores = jnp.where(valid, scores, -1e30)
    top = jnp.maximum(jnp.max(scores, axis=1, keepdims=True), fresh)
    shares = jnp.where(valid, jnp.exp(scores - top), 0.0)
    share_new = jnp.exp(fresh - top)
    denominator = jnp.sum(shares, axis=1, keepdims=True) + share_new
    rounded = shares.astype(BF16)
    summed = jnp.concatenate(
        [
            dot(rounded[n * 8 : n * 8 + 8], values[b, :, g * HEAD_SIZE : (g + 1) * HEAD_SIZE])
            for n, (b, g) in enumerate(blocks)
        ],
        axis=0,
    )
    result = (summed + share_new * jnp.concatenate(new_value, axis=0)) / denominator
    result = result.astype(BF16).astype(F32)
    out[...] = jnp.zeros((SLOT, HEAD_SIZE), F32)
    for n in range(len(blocks)):
        out[n * group : (n + 1) * group, :] = result[n * 8 : n * 8 + group, :]


def attended_rows(lengths, *operands):
    vmem = pl.BlockSpec(memory_space=pltpu.VMEM)
    return pl.pallas_call(
        attention_kernel,
        out_shape=pltpu.VMEM((SLOT, HEAD_SIZE), F32),
        in_specs=[pl.BlockSpec(memory_space=pl.ANY)] + [vmem] * len(operands),
        out_specs=vmem,
        scratch_shapes=[pltpu.SMEM(lengths.shape, jnp.int32), pltpu.SemaphoreType.DMA],
        compiler_params=pltpu.CompilerParams(vmem_limit_bytes=12 << 20),
    )(in_hbm(lengths), *(in_vmem(v) for v in operands))


def pack_kernel(s0, s1, s2, s3, attended, out):
    parts = [s[...].astype(F32) for s in (s0, s1, s2, s3)]
    low = (parts[0] + parts[1]) + (parts[2] + parts[3])
    tail = low[MAIN:, :]
    moved = [pltpu.roll(tail, 96 - TAIL * p, 1) for p in range(3)]
    moved.append(jnp.zeros((MAIN - 3 * TAIL, HEAD_SIZE), F32))
    lane = lax.broadcasted_iota(jnp.int32, (MAIN, HEAD_SIZE), 1)
    low = jnp.where(lane < 96, low[0:MAIN, :], jnp.concatenate(moved, axis=0)).astype(BF16)
    rows = attended[...].astype(BF16)
    for k in range(out.shape[0]):
        out[k, 0:MAIN, :] = low
        out[k, MAIN:, :] = rows


def combine_kernel(arrived, low_out, rows_out):
    total = arrived[0, 0:MAIN, :].astype(F32)
    rows_out[0:SLOT, :] = arrived[0, MAIN:, :]
    for k in range(1, arrived.shape[0]):
        total = total + arrived[k, 0:MAIN, :].astype(F32)
        rows_out[k * SLOT : (k + 1) * SLOT, :] = arrived[k, MAIN:, :]
    low_out[0:MAIN, :] = total
    lane = lax.broadcasted_iota(jnp.int32, (TAIL, HEAD_SIZE), 1)
    tail = jnp.zeros((TAIL, HEAD_SIZE), F32)
    for p in range(3):
        back = pltpu.roll(total[TAIL * p : TAIL * (p + 1), :], HEAD_SIZE - 96 + TAIL * p, 1)
        tail = jnp.where(lane // TAIL == p, back, tail)
    low_out[MAIN:, :] = tail


def outer_kernel(
    near, far, near_rows, far_rows, w_step, log_decay, step_bias, skip, conv, gate, state, w_out, term, w_attn,
    state_hbm, keep_out, send_out, total, state_out, state_sem,
):
    c = lax.axis_index("seq_2").astype(jnp.int32)
    seq = own_seq()
    batch = conv.shape[1]
    mine = c == 0
    near_low = near[:, 0:batch]
    far_low = far[:, 0:batch]
    low = jnp.concatenate(
        [jnp.where(mine, near_low, far_low), jnp.where(mine, far_low, near_low)], axis=0
    )
    rank = w_step.shape[1]
    states = state.shape[0]
    params = jnp.concatenate(
        [jnp.exp(log_decay[...]), step_bias[...], skip[...], jnp.zeros((6, conv.shape[0]), F32)],
        axis=0,
    ).T
    step = jax.nn.softplus(
        dot(w_step[...], low[0:rank].astype(BF16)) + params[:, states : states + 1]
    )
    conv_value = conv[...]
    driven = step * conv_value
    mixed = params[:, states + 1 : states + 2] * conv_value
    for n in range(states):
        decay = jnp.exp(-step * params[:, n : n + 1])
        fresh = decay * state[n] + driven * low[rank + n : rank + n + 1]
        state_out[n] = fresh
        mixed = mixed + fresh * low[rank + states + n : rank + states + n + 1]
    store = pltpu.make_async_copy(state_out, state_hbm, state_sem)
    store.start()
    gated = (mixed * gate[...]).astype(BF16)
    total[...] = term[...] + lax.dot_general(gated, w_out[...], TN, preferred_element_type=F32)

    slots = near_rows.shape[0]
    attended = jnp.concatenate([near_rows[...], far_rows[...]], axis=0)
    seqs = 3
    heads = w_attn.shape[0] // HEAD_SIZE
    token = lax.broadcasted_iota(jnp.int32, (batch, 2 * slots), 0)
    source = lax.broadcasted_iota(jnp.int32, (batch, 2 * slots), 1)
    owner = token // seqs
    other_core = jnp.where(owner % 2 == c, 0, 1)
    at = other_core * slots + (owner // 2) * SLOT + (token % seqs) * heads
    attn = jnp.zeros((batch, w_attn.shape[1]), F32)
    for h in range(heads):
        pick = jnp.where(source == at + h, 1.0, 0.0).astype(BF16)
        rows = dot(pick, attended).astype(BF16)
        attn = attn + dot(rows, w_attn[h * HEAD_SIZE : (h + 1) * HEAD_SIZE, :])
    start = pl.multiple_of(seq * HEAD_SIZE, HEAD_SIZE)
    total[:, pl.ds(start, HEAD_SIZE)] = total[:, pl.ds(start, HEAD_SIZE)] + attn

    rows = keep_out.shape[1]
    for i in range(total.shape[1] // HEAD_SIZE):
        block = total[:, i * HEAD_SIZE : (i + 1) * HEAD_SIZE].T.astype(BF16)
        for q in range(0, HEAD_SIZE // rows, 2):
            slot = (i * (HEAD_SIZE // rows) + q) // 2
            even = block[q * rows : (q + 1) * rows, :]
            odd = block[(q + 1) * rows : (q + 2) * rows, :]
            keep_out[slot] = jnp.where(mine, even, odd)
            send_out[slot] = jnp.where(mine, odd, even)
    store.wait()


def block(
    hidden_in,
    norm_gain,
    w_ssm_in,
    w_ssm_gate,
    conv_weight,
    conv_bias,
    conv_state,
    w_state_proj,
    w_step,
    step_bias,
    log_decay,
    skip_gain,
    ssm_state,
    w_ssm_out,
    w_query,
    key_projection,
    value_projection,
    w_attn_out,
    w_mlp_gate,
    w_mlp_up,
    w_mlp_down,
    cached_inputs,
    window_lengths,
):
    batch, features = hidden_in.shape
    width = norm_gain.shape[0]
    channels = w_ssm_in.shape[1]
    window = cached_inputs.shape[1]
    states = log_decay.shape[0]
    cosines, sines = (jnp.asarray(t) for t in rotary_tables(window + 8))

    hidden = hidden_in.T
    copies = jnp.broadcast_to(hidden[None], (64, features, batch))
    held = lax.all_to_all(copies, CHIPS, 0, 0, tiled=True)
    other = shifted(held, "seq_2", 1)

    *window_parts, w_in = window_rows(
        window_lengths, cached_inputs, key_projection, value_projection, cosines, sines,
        w_ssm_in.T,
    )

    normed, conv, low = vmem_call(
        inner_kernel,
        (
            ((width, batch), BF16, True),
            ((channels, batch), F32, True),
            ((2, ROWS, 128), F32, True),
        ),
        (
            held, other, norm_gain.reshape(-1, 128), w_in, w_state_proj,
            jnp.transpose(conv_state, (1, 2, 0)), conv_weight, conv_bias[None],
        ),
        cost=pl.CostEstimate(flops=COST, bytes_accessed=0, transcendentals=0),
    )
    paired = shifted(low[1], "seq_2", 1)
    half = (low[0] + paired).astype(BF16)
    arrived = from_ring(half, "grp")
    attended = attended_rows(
        window_lengths, normed, w_query, key_projection, value_projection, *window_parts,
    )
    gate, act = vmem_call(
        gate_kernel,
        (((channels, batch), F32, True), ((w_mlp_up.shape[1], batch), BF16, True)),
        (normed, w_ssm_gate.T, w_mlp_gate.T, w_mlp_up.T),
    )
    (term,) = vmem_call(down_kernel, (((batch, width), F32, True),), (act, w_mlp_down))
    (packed,) = vmem_call(
        pack_kernel, (((16, MAIN + SLOT, HEAD_SIZE), BF16, True),), (*arrived, attended)
    )
    packed = lax.all_to_all(packed, PLANE, 0, 0, tiled=True)
    near_low, near_rows = vmem_call(
        combine_kernel,
        (((ROWS, HEAD_SIZE), F32, True), ((16 * SLOT, HEAD_SIZE), BF16, True)),
        (packed,),
    )
    far_low = shifted(near_low, "seq_2", 1)
    far_rows = shifted(near_rows, "seq_2", 1)

    piece = ((64, features, batch), BF16, True)
    state_new, keep, send = vmem_call(
        outer_kernel,
        (((states, channels, batch), F32, False), piece, piece),
        (
            near_low, far_low, near_rows, far_rows, w_step.T, log_decay, step_bias[None], skip_gain[None], conv, gate,
            jnp.transpose(ssm_state, (1, 2, 0)), w_ssm_out, term, w_attn_out,
        ),
        stored=(0,),
        scratch=(
            pltpu.VMEM((batch, width), F32),
            pltpu.VMEM((states, channels, batch), F32),
            pltpu.SemaphoreType.DMA,
        ),
    )
    came = shifted(send, "seq_2", 1)
    summed = (keep.astype(F32) + came.astype(F32)).astype(BF16)
    arrived = lax.all_to_all(summed, CHIPS, 0, 0, tiled=True)
    total = jnp.sum(arrived.astype(F32), axis=0)
    hidden_out = (hidden.astype(F32) + total).astype(BF16).T
    return (hidden_out, jnp.transpose(state_new, (2, 0, 1)))


def solution(mesh):
    torus = Mesh(
        mesh.devices.reshape(mesh.shape["grp"], 4, 4, 2), ("grp", "seq_0", "seq_1", "seq_2")
    )
    placed = (
        P(None, GRP_SEQ),
        P(),
        P(None, GRP_SEQ),
        P(None, GRP_SEQ),
        P(None, GRP_SEQ),
        P(GRP_SEQ),
        P(None, None, GRP_SEQ),
        P(GRP_SEQ, None),
        P(None, GRP_SEQ),
        P(GRP_SEQ),
        P(None, GRP_SEQ),
        P(GRP_SEQ),
        P(None, None, GRP_SEQ),
        P(GRP_SEQ, None),
        P(None, "grp"),
        P(None, "grp"),
        P(None, "grp"),
        P("grp", SEQ),
        P(None, GRP_SEQ),
        P(None, GRP_SEQ),
        P(GRP_SEQ, None),
        P(SEQ, None, None),
        P(),
    )
    return jax.shard_map(
        block,
        mesh=torus,
        in_specs=placed,
        out_specs=(P(None, GRP_SEQ), P(None, None, GRP_SEQ)),
        check_vma=False,
    )
```
